128 devices in a mesh: table: 4 (over x), row: 32 (over z, y, core).
Axes of the slice: x: 4, y: 4, z: 4, core: 2. Of those that a mesh axis runs over, the one named last changes fastest.
Arguments:
- table: float32 [12288, 128, 128], P(('table', 'row')), may hold values from -2 to 2
- accumulator: float32 [12288, 128], P(('table', 'row')), may hold values from 0.05 to 2
- grads_one: float32 [131072, 128], P(('table', 'row')), may hold values from -6 to 6
- ids_one: int32 [131072], P(('table', 'row')), may hold values from 0 to 1572863, as said below
- grads_two: float32 [131072, 128], P(('table', 'row')), may hold values from -6 to 6
- ids_two: int32 [131072], P(('table', 'row')), may hold values from 0 to 1572863, as said below
- new_slot: int32 [12288], replicated, may hold values from 0 to 12287, as said below
Outputs:
- table_out: float32 [12288, 128, 128], P(('table', 'row'))
- accum_out: float32 [12288, 128], P(('table', 'row'))
The draws below stay inside these ranges and needn't reach their ends.
Inputs may be any that keep to these rules, and one draw needn't show every extreme that they name: `ids_one`: the ids of one device are distinct. The owner of row r is device r // 12288; at most 16 of one device's ids fall on one owner, and on every device exactly 16 fall on some owner. `ids_two`: the ids of one device are distinct. After the move the owner of row r is device new_slot[r // 128] // 96; at most 16 of one device's ids fall on one such owner, and on every device exactly 16 fall on some owner. `new_slot`: A permutation. Each device keeps all but exactly 12 of its blocks in their slots; its leaving blocks go to 12 different other devices of its table group, one each, into slots freed there, so each device also receives exactly 12 blocks from different devices of its group.
All inputs are finite; a program needn't handle non-finite values.
Results may differ from the reference program's by a relative error of at most 0.00002.
Values sent between devices are 32-bit elements; how exact they have to be, the bound alone decides.
No kernel may reach another device: no remote copies, remote signals or barrier semaphores. Data moves between devices by JAX's collectives and lax.ppermute only.
A program may use at most 64 MiB of HBM per device.

```python
import math
import jax
import jax.numpy as jnp
from jax import lax

DIM = 128
BLOCK = 128
BLOCKS_DEV = 96
GRAD_DEV = 1024
ROWS_DEV = 12288
NBLOCKS = 12288
GRADS = 131072
CAP = 16
MOVES_DEV = 12
N_TABLE = 4
N_ROW = 32
DEVICES = 128


def make_plan(key):
    base = jax.random.fold_in(key, 7)
    key_order, key_shift, key_leave = jax.random.split(base, 3)
    order_rows = jax.vmap(lambda subkey: jax.random.permutation(subkey, N_ROW))(jax.random.split(key_order, N_TABLE)).astype(jnp.int32)
    shifts = jax.vmap(lambda subkey: 1 + jax.random.permutation(subkey, N_ROW - 1)[:MOVES_DEV])(jax.random.split(key_shift, N_TABLE)).astype(jnp.int32)
    leaving = jax.vmap(lambda subkey: jax.random.permutation(subkey, BLOCKS_DEV)[:MOVES_DEV])(jax.random.split(key_leave, DEVICES)).astype(jnp.int32).reshape(N_TABLE, N_ROW, MOVES_DEV)
    position = jnp.argsort(order_rows, axis=1).astype(jnp.int32)
    ahead = (position[:, :, None] + shifts[:, None, :]) % N_ROW
    target = jnp.take_along_axis(order_rows, ahead.reshape(N_TABLE, N_ROW * MOVES_DEV), axis=1).reshape(N_TABLE, N_ROW, MOVES_DEV)
    groups = jnp.arange(N_TABLE, dtype=jnp.int32)[:, None, None]
    rows_here = jnp.arange(N_ROW, dtype=jnp.int32)[None, :, None]
    moves = jnp.arange(MOVES_DEV, dtype=jnp.int32)[None, None, :]
    source = (groups * N_ROW + rows_here) * BLOCKS_DEV + leaving
    freed = leaving[groups, target, moves]
    arrival = (groups * N_ROW + target) * BLOCKS_DEV + freed
    return jnp.arange(NBLOCKS, dtype=jnp.int32).at[source.reshape(-1)].set(arrival.reshape(-1))


def make_ids(key, holder):
    pool_size = DEVICES * CAP
    spacing = ROWS_DEV // CAP
    slot_all = jnp.arange(pool_size, dtype=jnp.int32)

    def one_device(subkey):
        key_full, key_order, key_offset, key_jitter = jax.random.split(subkey, 4)
        crowded = jax.random.randint(key_full, (), 0, DEVICES, dtype=jnp.int32)
        shuffled = jax.random.permutation(key_order, pool_size).astype(jnp.int32)
        standing = jnp.argsort(shuffled).astype(jnp.int32)
        priority = jnp.where(slot_all // CAP == crowded, slot_all % CAP, CAP + standing)
        chosen = jnp.argsort(priority)[:GRAD_DEV].astype(jnp.int32)
        owners = chosen // CAP
        within = chosen % CAP
        offsets = jax.random.randint(key_offset, (DEVICES,), 0, ROWS_DEV, dtype=jnp.int32)
        jitter = jax.random.randint(key_jitter, (GRAD_DEV,), 0, spacing, dtype=jnp.int32)
        local_row = (offsets[owners] + within * spacing + jitter) % ROWS_DEV
        block_slot = owners * BLOCKS_DEV + local_row // BLOCK
        return holder[block_slot] * BLOCK + local_row % BLOCK
    return jax.vmap(one_device)(jax.random.split(key, DEVICES)).reshape(-1).astype(jnp.int32)


def draw_ids_one(key, part):
    return make_ids(jax.random.fold_in(key, 1), jnp.arange(NBLOCKS, dtype=jnp.int32))


def draw_ids_two(key, part):
    placing = make_plan(key)
    holder = jnp.zeros((NBLOCKS,), jnp.int32).at[placing].set(jnp.arange(NBLOCKS, dtype=jnp.int32))
    return make_ids(jax.random.fold_in(key, 2), holder)


def draw_new_slot(key, part):
    return make_plan(key)


def levels(rng, extent, shards, least, high):
    def one(dim, blocks):
        steps = jax.random.uniform(jax.random.fold_in(jax.random.fold_in(rng, 6), dim), (blocks,), jnp.float32, least / len(shards), high / len(shards))
        return jnp.repeat(jnp.exp(steps), extent[dim] // blocks).reshape((-1,) + (1,) * (len(extent) - dim - 1))

    gain = one(*shards[0])
    for cut in shards[1:]:
        gain = gain * one(*cut)
    return gain


def noise(key, extent, scale, most, cuts=(), kind=jnp.bfloat16):
    drawn = scale * jax.random.normal(key, extent, jnp.float32)
    if cuts:
        drawn = drawn * levels(key, extent, cuts, -0.22, 0.18)
    return jnp.clip(drawn, -most, most).astype(kind)


def setup_inputs(seed: int = 0) -> dict:
    keys = jax.random.split(jax.random.key(seed), 8)
    table = noise(keys[0], (NBLOCKS, BLOCK, DIM), 0.3, 2.0, ((0, 128),), jnp.float32)
    accumulator = jnp.clip(jnp.exp(math.log(2.0) - 3.6888794 * jax.random.uniform(keys[1], (NBLOCKS, BLOCK), jnp.float32) ** levels(keys[1], (NBLOCKS, BLOCK), ((0, 128),), -0.2, 0.2)), 0.05, 2.0)
    grads_one = noise(keys[2], (GRADS, DIM), 1.0, 6.0, ((0, 128),), jnp.float32)
    ids_one = draw_ids_one(jax.random.fold_in(keys[7], 71), 0)
    grads_two = noise(keys[4], (GRADS, DIM), 1.0, 6.0, ((0, 128),), jnp.float32)
    ids_two = draw_ids_two(jax.random.fold_in(keys[7], 71), 0)
    new_slot = draw_new_slot(jax.random.fold_in(keys[7], 71), 0)
    return dict(table=table, accumulator=accumulator, grads_one=grads_one, ids_one=ids_one, grads_two=grads_two, ids_two=ids_two, new_slot=new_slot)


LEARN = 0.5
EPSILON = 1e-08

def adagrad(weights, accums, gradient):
    fresh = accums + lax.optimization_barrier(jnp.mean(gradient * gradient, axis=-1))
    return (weights - LEARN * gradient / (jnp.sqrt(fresh)[:, None] + EPSILON), fresh)

def reference(table, accumulator, grads_one, ids_one, grads_two, ids_two, new_slot):
    row_count = NBLOCKS * BLOCK
    weights = table.reshape(row_count, DIM)
    accums = accumulator.reshape(row_count)
    first = jnp.zeros((row_count, DIM), jnp.float32).at[ids_one].add(grads_one)
    weights, accums = adagrad(weights, accums, first)
    holder = jnp.zeros((NBLOCKS,), jnp.int32).at[new_slot].set(jnp.arange(NBLOCKS, dtype=jnp.int32))
    weights = weights.reshape(NBLOCKS, BLOCK, DIM)[holder].reshape(row_count, DIM)
    accums = accums.reshape(NBLOCKS, BLOCK)[holder].reshape(row_count)
    landing = new_slot[ids_two // BLOCK] * BLOCK + ids_two % BLOCK
    second = jnp.zeros((row_count, DIM), jnp.float32).at[landing].add(grads_two)
    weights, accums = adagrad(weights, accums, second)
    return (weights.reshape(NBLOCKS, BLOCK, DIM), accums.reshape(NBLOCKS, BLOCK))
```

```python
import jax
import jax.numpy as jnp
from jax import lax
from jax.experimental import pallas as pl
from jax.experimental.pallas import tpu as pltpu
from jax.sharding import PartitionSpec as P

LEARN = 0.5
EPSILON = 1e-08


def ranks(owners, total):
    onehot = (owners[:, None] == jnp.arange(total, dtype=jnp.int32)[None, :]).astype(jnp.int32)
    return jnp.sum((jnp.cumsum(onehot, axis=0) - onehot) * onehot, axis=1)


def id_table(owners, within, local_row, total, capacity):
    to = (owners[:, None] == jnp.arange(total, dtype=jnp.int32)[None, :])
    at = (within[:, None] == jnp.arange(capacity, dtype=jnp.int32)[None, :]).astype(jnp.bfloat16)
    named = local_row + 1
    halves = []
    for part in (named // 128, named % 128):
        left = jnp.where(to, part[:, None], 0).astype(jnp.bfloat16)
        halves.append(lax.dot_general(left, at, (((0,), (0,)), ((), ())), preferred_element_type=jnp.float32))
    return halves[0] * 128.0 + halves[1]


def pack_kernel(place_ref, one_ref, two_ref, ids_ref, out_ref, *, rows, stride):
    def step(i, _):
        base = i * 8
        for src, off in ((one_ref, 0), (two_ref, rows)):
            tile = src[pl.ds(base, 8), :]
            for j in range(8):
                out_ref[place_ref[off + base + j]] = tile[j : j + 1, :]
        return 0

    out_ref[...] = jnp.zeros_like(out_ref)
    lax.fori_loop(0, rows // 8, step, 0)

    def names(d, _):
        out_ref[d * stride + stride - 1] = ids_ref[pl.ds(d, 1), :]
        return 0

    lax.fori_loop(0, ids_ref.shape[0], names, 0, unroll=8)


def pack(places, one, two, ids, total, stride):
    rows, feature = one.shape
    return pl.pallas_call(
        lambda *refs: pack_kernel(*refs, rows=rows, stride=stride),
        out_shape=jax.ShapeDtypeStruct((total * stride, 1, feature), jnp.float32),
        grid_spec=pltpu.PrefetchScalarGridSpec(
            num_scalar_prefetch=1,
            grid=(1,),
            in_specs=[
                pl.BlockSpec((rows, feature), lambda i, s: (0, 0)),
                pl.BlockSpec((rows, feature), lambda i, s: (0, 0)),
                pl.BlockSpec((total, feature), lambda i, s: (0, 0)),
            ],
            out_specs=pl.BlockSpec((total * stride, 1, feature), lambda i, s: (0, 0, 0)),
        ),
        name="pack",
    )(places, one, two, ids)


def scatter_rows(names_ref, got_ref, sums_ref, *, sources, stride, offset, cap, width):
    def step(s, _):
        rows = [names_ref[s * width + offset + j] for j in range(cap)]
        new = [sums_ref[pl.ds(r, 1), :] + got_ref[s * stride + offset + j] for j, r in enumerate(rows)]
        for r, value in zip(rows, new):
            sums_ref[pl.ds(r, 1), :] = value
        return 0

    lax.fori_loop(0, sources, step, 0)


def eye(size):
    return lax.broadcasted_iota(jnp.int32, (size, size), 0) == lax.broadcasted_iota(jnp.int32, (size, size), 1)


def column(diagonal, row):
    return jnp.sum(jnp.where(diagonal, row, 0.0), axis=1, keepdims=True)


def as_row(diagonal, col):
    return jnp.sum(jnp.where(diagonal, col, 0.0), axis=0, keepdims=True)


def adagrad(weights, accums, gradient):
    fresh = accums + jnp.sum(gradient * gradient, axis=1, keepdims=True) * (1.0 / gradient.shape[1])
    return weights - LEARN * gradient / (jnp.sqrt(fresh) + EPSILON), fresh


def leave_kernel(names_ref, send_ref, table_ref, acc_ref, got_ref, sums_ref, out_ref, sem, *, sources, stride, cap, peers, width):
    block = table_ref.shape[1]
    for p in range(peers):
        slot = send_ref[p]

        @pl.when(slot >= 0)
        def _():
            pltpu.make_async_copy(table_ref.at[slot], out_ref.at[p, pl.ds(0, block)], sem.at[p]).start()

    sums_ref[...] = jnp.zeros_like(sums_ref)
    scatter_rows(names_ref, got_ref, sums_ref, sources=sources, stride=stride, offset=0, cap=cap, width=width)
    diagonal = eye(block)

    def step(p, _):
        slot = send_ref[p]

        @pl.when(slot >= 0)
        def _():
            pltpu.make_async_copy(table_ref.at[slot], out_ref.at[p, pl.ds(0, block)], sem.at[p]).wait()
            old = column(diagonal, acc_ref[pl.ds(slot, 1), :])
            gradient = sums_ref[pl.ds(pl.multiple_of(slot * block, block), block), :]
            weights, fresh = adagrad(out_ref[p, pl.ds(0, block), :], old, gradient)
            out_ref[p, pl.ds(0, block), :] = weights
            out_ref[p, pl.ds(block, 8), :] = jnp.broadcast_to(as_row(diagonal, fresh), (8, block))

        return 0

    lax.fori_loop(0, peers, step, 0)


def leave(names, send, table, acc, got, sources, stride, cap, peers, width):
    blocks, block, feature = table.shape
    vm = pl.BlockSpec(memory_space=pltpu.VMEM)
    sm = pl.BlockSpec(memory_space=pltpu.SMEM)
    return pl.pallas_call(
        lambda *refs: leave_kernel(*refs, sources=sources, stride=stride, cap=cap, peers=peers, width=width),
        out_shape=(
            jax.ShapeDtypeStruct((blocks * block + 8, feature), jnp.float32),
            jax.ShapeDtypeStruct((peers, block + 8, feature), jnp.float32),
        ),
        in_specs=[sm, sm, pl.BlockSpec(memory_space=pl.ANY), vm, vm],
        out_specs=(vm, vm),
        scratch_shapes=[pltpu.SemaphoreType.DMA((peers,))],
        name="leave",
    )(names, send, table, acc, got)


def stay_kernel(names_ref, table_ref, acc_ref, got_ref, first_ref, out_ref, accout_ref, sums_ref, *, sources, stride, cap, width):
    b = pl.program_id(0)
    block = table_ref.shape[1]

    @pl.when(b == 0)
    def _():
        sums_ref[...] = jnp.zeros_like(sums_ref)
        scatter_rows(names_ref, got_ref, sums_ref, sources=sources, stride=stride, offset=cap, cap=cap, width=width)

    diagonal = eye(block)
    old = column(diagonal, acc_ref[pl.ds(b, 1), :])
    at = pl.ds(pl.multiple_of(b * block, block), block)
    weights, fresh = adagrad(table_ref[0], old, first_ref[at, :])
    weights, fresh = adagrad(weights, fresh, sums_ref[at, :])
    out_ref[0] = weights
    accout_ref[pl.ds(b, 1), :] = as_row(diagonal, fresh)


def stay(names, table, acc, got, first, sources, stride, cap, width):
    blocks, block, feature = table.shape
    vm = pl.BlockSpec(memory_space=pltpu.VMEM)
    sm = pl.BlockSpec(memory_space=pltpu.SMEM)
    return pl.pallas_call(
        lambda *refs: stay_kernel(*refs, sources=sources, stride=stride, cap=cap, width=width),
        grid=(blocks,),
        out_shape=(
            jax.ShapeDtypeStruct(table.shape, jnp.float32),
            jax.ShapeDtypeStruct(acc.shape, jnp.float32),
            jax.ShapeDtypeStruct(first.shape, jnp.float32),
        ),
        in_specs=[sm, pl.BlockSpec((1, block, feature), lambda b: (b, 0, 0)), vm, vm, vm],
        out_specs=(pl.BlockSpec((1, block, feature), lambda b: (b, 0, 0)), vm, vm),
        name="stay",
    )(names, table, acc, got, first)


def arrive_kernel(slots_ref, got_ref, second_ref, stayed_ref, accstay_ref, out_ref, acc_ref, buf_ref, sem, *, peers):
    block = stayed_ref.shape[1]
    acc_ref[...] = accstay_ref[...]
    diagonal = eye(block)

    def store(p, slot):
        return pltpu.make_async_copy(buf_ref.at[p], out_ref.at[slot], sem.at[p])

    def step(p, _):
        slot = slots_ref[p]

        @pl.when(slot >= 0)
        def _():
            old = column(diagonal, got_ref[p, pl.ds(block, 1), :])
            gradient = second_ref[pl.ds(pl.multiple_of(slot * block, block), block), :]
            weights, fresh = adagrad(got_ref[p, pl.ds(0, block), :], old, gradient)
            buf_ref[p] = weights
            acc_ref[pl.ds(slot, 1), :] = as_row(diagonal, fresh)
            store(p, slot).start()

        return 0

    lax.fori_loop(0, peers, step, 0)

    def finish(p, _):
        slot = slots_ref[p]

        @pl.when(slot >= 0)
        def _():
            store(p, slot).wait()

        return 0

    lax.fori_loop(0, peers, finish, 0)


def arrive(slots, got, second, stayed, accstay, peers):
    blocks, block, feature = stayed.shape
    vm = pl.BlockSpec(memory_space=pltpu.VMEM)
    sm = pl.BlockSpec(memory_space=pltpu.SMEM)
    hbm = pl.BlockSpec(memory_space=pl.ANY)
    return pl.pallas_call(
        lambda *refs: arrive_kernel(*refs, peers=peers),
        out_shape=(
            jax.ShapeDtypeStruct(stayed.shape, jnp.float32),
            jax.ShapeDtypeStruct(accstay.shape, jnp.float32),
        ),
        in_specs=[sm, vm, vm, hbm, vm],
        out_specs=(hbm, vm),
        scratch_shapes=[pltpu.VMEM((peers, block, feature), jnp.float32), pltpu.SemaphoreType.DMA((peers,))],
        input_output_aliases={3: 0},
        name="arrive",
    )(slots, got, second, stayed, accstay)


def on_device(table, accumulator, grads_one, ids_one, grads_two, ids_two, new_slot):
    blocks, block, feature = table.shape
    rows_here = blocks * block
    peers = lax.axis_size("row")
    total = lax.axis_size("table") * peers
    group = lax.axis_index("table")
    device = group * peers + lax.axis_index("row")
    cap = 2 * grads_one.shape[0] // total
    stride = 2 * cap + 1
    width = 2 * cap

    owner_one = ids_one // rows_here
    within_one = ranks(owner_one, total)
    slot_two = new_slot[ids_two // block]
    owner_two = slot_two // blocks
    within_two = ranks(owner_two, total)
    local_two = slot_two % blocks * block + ids_two % block
    places = jnp.concatenate([owner_one * stride + within_one, owner_two * stride + cap + within_two])
    names = jnp.concatenate(
        [
            id_table(owner_one, within_one, ids_one % rows_here, total, cap),
            id_table(owner_two, within_two, local_two, total, cap),
        ],
        axis=1,
    )
    names = jnp.pad(names, ((0, 0), (0, feature - width)))
    outgoing = pack(places, grads_one, grads_two, names, total, stride)
    got = lax.all_to_all(outgoing, ("table", "row"), split_axis=0, concat_axis=0, tiled=True)
    named = got.reshape(total, stride, feature)[:, stride - 1, :width].astype(jnp.int32)
    named = jnp.where(named > 0, named - 1, rows_here).reshape(-1)

    here = lax.dynamic_slice_in_dim(new_slot, group * peers * blocks, peers * blocks).reshape(peers, blocks)
    peer = jnp.arange(peers, dtype=jnp.int32)
    mine = lax.axis_index("row")
    leaving = lax.dynamic_slice_in_dim(here, mine, 1)
    to_peer = (leaving // blocks % peers == peer[:, None]) & (peer != mine)[:, None]
    send = jnp.sum(jnp.where(to_peer, jnp.arange(1, blocks + 1, dtype=jnp.int32)[None, :], 0), axis=1) - 1
    to_me = (here // blocks == device) & (peer != mine)[:, None]
    slots = jnp.sum(jnp.where(to_me, here - device * blocks + 1, 0), axis=1) - 1

    first, moving = leave(named, send, table, accumulator, got, total, stride, cap, peers, width)
    moved = lax.all_to_all(moving, "row", split_axis=0, concat_axis=0, tiled=True)
    stayed, accstay, second = stay(named, table, accumulator, got, first, total, stride, cap, width)
    return arrive(slots, moved, second, stayed, accstay, peers)


def solution(mesh):
    in_specs = (
        P(("table", "row"), None, None),
        P(("table", "row"), None),
        P(("table", "row"), None),
        P(("table", "row")),
        P(("table", "row"), None),
        P(("table", "row")),
        P(),
    )
    out_specs = (P(("table", "row"), None, None), P(("table", "row"), None))
    return jax.shard_map(
        on_device, mesh=mesh, in_specs=in_specs, out_specs=out_specs, check_vma=False
    )
```

```python
import jax
import jax.numpy as jnp
from jax import lax
from jax.experimental import pallas as pl
from jax.experimental.pallas import tpu as pltpu
from jax.sharding import PartitionSpec as P

LEARN = 0.5
EPSILON = 1e-08
LANES = 128
MOVES = 12
VM = pltpu.VMEM
SM = pltpu.SMEM
MIB = 1024 * 1024


def iota(shape, dim):
    return lax.broadcasted_iota(jnp.int32, shape, dim)


def dot(a, b, contract):
    return lax.dot_general(a, b, ((contract[:1], contract[1:]), ((), ())), preferred_element_type=jnp.float32)


def lookup(which_ref, indices):
    low, high = which_ref.shape
    pick = (iota((high, indices.shape[1]), 0) == (indices >> 7)).astype(jnp.bfloat16)
    found = jnp.zeros((low, indices.shape[1]), jnp.float32)
    table = which_ref[...]
    for part, scale in ((table >> 7, 128.0), (table & 127, 1.0)):
        found += dot(part.astype(jnp.float32).astype(jnp.bfloat16), pick, (1, 0)) * scale
    here = iota(found.shape, 0) == (indices & 127)
    return jnp.sum(jnp.where(here, found, 0.0), axis=0, keepdims=True).astype(jnp.int32)


def pack_kernel(one_ids, two_ids, slot_ref, one_hbm, two_hbm, out_ref, one_ref, two_ref, place_v, place_s, names_v, sems, *, total, blocks, cap):
    stride = 2 * cap + 1
    rows = one_ref.shape[0]
    chunks = rows // LANES
    copies = [
        pltpu.make_async_copy(one_hbm, one_ref, sems.at[0]),
        pltpu.make_async_copy(two_hbm, two_ref, sems.at[1]),
    ]
    for copy in copies:
        copy.start()
    ids = one_ids[...]
    ids2 = two_ids[...]
    block_slots = (ids >> 7, lookup(slot_ref, ids2 >> 7))
    inner = (ids & 127, ids2 & 127)
    upper = jnp.where(iota((LANES, 2 * LANES), 0) < iota((LANES, 2 * LANES), 1), 1.0, 0.0).astype(jnp.bfloat16)
    lane_slot = iota((LANES, LANES), 0) & (2 * cap - 1)
    high = jnp.zeros((total, LANES), jnp.float32)
    low = jnp.zeros((total, LANES), jnp.float32)
    for step in range(2):
        slot = block_slots[step]
        owner = (slot * 43691) >> 22
        named = (slot - owner * blocks) * LANES + inner[step] + 1
        carry = jnp.zeros((total, LANES), jnp.float32)
        for c in range(chunks):
            at = slice(c * LANES, (c + 1) * LANES)
            own = owner[:, at]
            name = named[:, at]
            mine = iota((total, LANES), 0) == own
            counted = dot(jnp.where(mine, 1.0, 0.0).astype(jnp.bfloat16), upper, (1, 0))
            before = counted[:, :LANES] + carry
            carry = carry + counted[:, LANES:]
            within = jnp.sum(jnp.where(mine, before, 0.0), axis=0, keepdims=True).astype(jnp.int32) + step * cap
            place_v[pl.ds(step * chunks + c, 1), :] = own * stride + within
            where = jnp.where(lane_slot == within, 1.0, 0.0).astype(jnp.bfloat16)
            high += dot(jnp.where(mine, (name >> 7).astype(jnp.float32), 0.0).astype(jnp.bfloat16), where, (1, 1))
            low += dot(jnp.where(mine, (name & 127).astype(jnp.float32), 0.0).astype(jnp.bfloat16), where, (1, 1))
    to_scalar = pltpu.make_async_copy(place_v, place_s, sems.at[2])
    to_scalar.start()
    names_v[...] = high * 128.0 + low

    def names(d, _):
        base = d * 8
        tile = names_v[pl.ds(base, 8), :]
        for j in range(8):
            out_ref[(base + j) * stride + stride - 1] = tile[j : j + 1, :]
        return 0

    lax.fori_loop(0, total // 8, names, 0, unroll=2)
    to_scalar.wait()
    for copy in copies:
        copy.wait()

    def move(i, _):
        base = i * 8
        for step, src in enumerate((one_ref, two_ref)):
            tile = src[pl.ds(base, 8), :]
            for j in range(8):
                out_ref[place_s[step * chunks + (i >> 4), ((i & 15) * 8) + j]] = tile[j : j + 1, :]
        return 0

    lax.fori_loop(0, rows // 8, move, 0, unroll=2)


def pack(one_ids, two_ids, slots, one, two, total, blocks, cap):
    rows, feature = one.shape
    vm = pl.BlockSpec(memory_space=VM)
    hbm = pl.BlockSpec(memory_space=pl.ANY)
    stride = 2 * cap + 1
    return pl.pallas_call(
        lambda *refs: pack_kernel(*refs, total=total, blocks=blocks, cap=cap),
        out_shape=jax.ShapeDtypeStruct((total * stride, 1, feature), jnp.float32),
        in_specs=[vm, vm, vm, hbm, hbm],
        out_specs=vm,
        scratch_shapes=[
            VM((rows, feature), jnp.float32),
            VM((rows, feature), jnp.float32),
            VM((2 * rows // LANES, LANES), jnp.int32),
            SM((2 * rows // LANES, LANES), jnp.int32),
            VM((total, LANES), jnp.float32),
            pltpu.SemaphoreType.DMA((3,)),
        ],
        compiler_params=pltpu.CompilerParams(vmem_limit_bytes=16 * MIB),
        name="pack",
    )(one_ids, two_ids, slots, one, two)


def read_names(got_ref, names_v, names_s, sem, *, total, cap, dump):
    width = 2 * cap
    stride = width + 1
    per = LANES // width
    group = iota((1, LANES), 1) // width
    for a in range(total // per):
        row = got_ref[a * per * stride + stride - 1]
        for k in range(1, per):
            row = jnp.where(group == k, got_ref[(a * per + k) * stride + stride - 1], row)
        names_v[pl.ds(a, 1), :] = row.astype(jnp.int32)
    named = names_v[...]
    names_v[...] = jnp.where(named > 0, named - 1, dump)
    copy = pltpu.make_async_copy(names_v, names_s, sem)
    copy.start()
    copy.wait()


def add_rows(names_s, got_ref, sums_ref, *, total, cap, offset):
    width = 2 * cap
    stride = width + 1
    per = LANES // width

    def step(a, _):
        for k in range(per):
            base = (a * per + k) * stride + offset
            rows = [names_s[a, k * width + offset + j] for j in range(cap)]
            new = [sums_ref[pl.ds(r, 1), :] + got_ref[base + j] for j, r in enumerate(rows)]
            for r, value in zip(rows, new):
                sums_ref[pl.ds(r, 1), :] = value
        return 0

    lax.fori_loop(0, total // per, step, 0)


def square_sums(block):
    return jnp.sum(block * block, axis=1, keepdims=True)


def rate(accums):
    return LEARN / (jnp.sqrt(accums) + EPSILON)


def lane_of(columns, k):
    return columns[:, k : k + 1]


def leave_kernel(from_ref, to_ref, table_ref, acc_ref, got_ref, names_out, out_ref, sums_ref, old_ref, names_v, names_s, sems, *, total, cap):
    block, feature = table_ref.shape[1:]
    rows = table_ref.shape[0] * block

    def fetch(k):
        return pltpu.make_async_copy(table_ref.at[from_ref[k]], out_ref.at[to_ref[k], pl.ds(0, block)], sems.at[k])

    for k in range(MOVES):
        fetch(k).start()
    spans = [pl.ds(pl.multiple_of(from_ref[k] * block, block), block) for k in range(MOVES)]
    for k in range(MOVES):
        sums_ref[spans[k], :] = jnp.zeros((block, feature), jnp.float32)
        old_ref[pl.ds(k, 1), :] = acc_ref[pl.ds(from_ref[k], 1), :]
    read_names(got_ref, names_v, names_s, sems.at[MOVES], total=total, cap=cap, dump=rows)
    names_out[...] = names_v[...]
    add_rows(names_s, got_ref, sums_ref, total=total, cap=cap, offset=0)
    lane = iota((block, LANES), 1)
    squares = jnp.zeros((block, LANES), jnp.float32)
    for k in range(MOVES):
        squares = jnp.where(lane == k, square_sums(sums_ref[spans[k], :]), squares)
    fresh = jnp.transpose(old_ref[...]) + squares * (1.0 / feature)
    rates = rate(jnp.where(lane < MOVES, fresh, 1.0))
    old_ref[...] = jnp.transpose(fresh)
    for k in range(MOVES):
        fetch(k).wait()
    for k in range(MOVES):
        weights = out_ref[to_ref[k], pl.ds(0, block), :]
        out_ref[to_ref[k], pl.ds(0, block), :] = weights - lane_of(rates, k) * sums_ref[spans[k], :]
        out_ref[to_ref[k], pl.ds(block, 1), :] = old_ref[pl.ds(k, 1), :]


def leave(came_from, go_to, table, acc, got, peers, total, cap):
    blocks, block, feature = table.shape
    vm = pl.BlockSpec(memory_space=VM)
    sm = pl.BlockSpec(memory_space=SM)
    names = (total * 2 * cap // LANES, LANES)
    return pl.pallas_call(
        lambda *refs: leave_kernel(*refs, total=total, cap=cap),
        out_shape=(
            jax.ShapeDtypeStruct(names, jnp.int32),
            jax.ShapeDtypeStruct((peers, block + 8, feature), jnp.float32),
        ),
        in_specs=[sm, sm, pl.BlockSpec(memory_space=pl.ANY), vm, vm],
        out_specs=(vm, vm),
        scratch_shapes=[
            VM((blocks * block + 8, feature), jnp.float32),
            VM((LANES, LANES), jnp.float32),
            VM(names, jnp.int32),
            SM(names, jnp.int32),
            pltpu.SemaphoreType.DMA((MOVES + 1,)),
        ],
        compiler_params=pltpu.CompilerParams(vmem_limit_bytes=20 * MIB),
        name="leave",
    )(came_from, go_to, table, acc, got)


def stay_kernel(names_ref, slots_ref, table_ref, acc_ref, got_ref, out_ref, accout_ref, arrive_ref, one_ref, two_ref, rates_ref, *, total, cap, blocks):
    i = pl.program_id(0)
    each, block, feature = table_ref.shape

    @pl.when(i == 0)
    def _():
        def clear(b, _):
            at = pl.ds(pl.multiple_of(b * block, block), block)
            one_ref[at, :] = jnp.zeros((block, feature), jnp.float32)
            two_ref[at, :] = jnp.zeros((block, feature), jnp.float32)
            return 0

        lax.fori_loop(0, blocks, clear, 0)
        add_rows(names_ref, got_ref, one_ref, total=total, cap=cap, offset=0)
        add_rows(names_ref, got_ref, two_ref, total=total, cap=cap, offset=cap)
        lane = iota((block, LANES), 1)

        def squares(g, sums):
            sums = list(sums)
            for k in range(4):
                b = g * 4 + k
                at = pl.ds(pl.multiple_of(b * block, block), block)
                for n, ref in enumerate((one_ref, two_ref)):
                    sums[n] = jnp.where(lane == b, square_sums(ref[at, :]), sums[n])
            return tuple(sums)

        zero = jnp.zeros((block, LANES), jnp.float32)
        first, second = lax.fori_loop(0, blocks // 4, squares, (zero, zero))
        old = jnp.concatenate([acc_ref[...], jnp.ones((LANES - blocks, LANES), jnp.float32)], axis=0)
        fresh = jnp.transpose(old) + first * (1.0 / feature)
        rates_ref[0] = rate(fresh)
        fresh = fresh + second * (1.0 / feature)
        rates_ref[1] = rate(fresh)
        accout_ref[...] = jnp.transpose(fresh)[:blocks, :]
        for k in range(MOVES):
            at = pl.ds(pl.multiple_of(slots_ref[k] * block, block), block)
            arrive_ref[k] = two_ref[at, :]

    turn = (LANES - each * i) % LANES
    one_rate = pltpu.roll(rates_ref[0], turn, 1)
    two_rate = pltpu.roll(rates_ref[1], turn, 1)
    for k in range(each):
        at = pl.ds(pl.multiple_of((i * each + k) * block, block), block)
        weights = table_ref[k] - lane_of(one_rate, k) * one_ref[at, :]
        out_ref[k] = weights - lane_of(two_rate, k) * two_ref[at, :]


def stay(names, slots, table, acc, got, total, cap, each=8):
    blocks, block, feature = table.shape
    vm = pl.BlockSpec(memory_space=VM)
    sm = pl.BlockSpec(memory_space=SM)
    piece = pl.BlockSpec((each, block, feature), lambda i: (i, 0, 0))
    return pl.pallas_call(
        lambda *refs: stay_kernel(*refs, total=total, cap=cap, blocks=blocks),
        grid=(blocks // each,),
        out_shape=(
            jax.ShapeDtypeStruct(table.shape, jnp.float32),
            jax.ShapeDtypeStruct(acc.shape, jnp.float32),
            jax.ShapeDtypeStruct((MOVES, block, feature), jnp.float32),
        ),
        in_specs=[sm, sm, piece, vm, vm],
        out_specs=(piece, vm, vm),
        scratch_shapes=[
            VM((blocks * block + 8, feature), jnp.float32),
            VM((blocks * block + 8, feature), jnp.float32),
            VM((2, LANES, LANES), jnp.float32),
        ],
        compiler_params=pltpu.CompilerParams(vmem_limit_bytes=28 * MIB),
        name="stay",
    )(names, slots, table, acc, got)


def arrive_kernel(peers_ref, slots_ref, got_ref, second_ref, stayed_ref, accstay_ref, out_ref, acc_ref, buf_ref, old_ref, sems):
    block, feature = stayed_ref.shape[1:]
    lane = iota((block, LANES), 1)
    for k in range(MOVES):
        old_ref[pl.ds(k, 1), :] = got_ref[peers_ref[k], pl.ds(block, 1), :]
    squares = jnp.zeros((block, LANES), jnp.float32)
    for k in range(MOVES):
        squares = jnp.where(lane == k, square_sums(second_ref[k]), squares)
    fresh = jnp.transpose(old_ref[...]) + squares * (1.0 / feature)
    rates = rate(jnp.where(lane < MOVES, fresh, 1.0))
    copies = []
    for k in range(MOVES):
        buf_ref[k] = got_ref[peers_ref[k], pl.ds(0, block), :] - lane_of(rates, k) * second_ref[k]
        copies.append(pltpu.make_async_copy(buf_ref.at[k], out_ref.at[slots_ref[k]], sems.at[k]))
        copies[-1].start()
    old_ref[...] = jnp.transpose(fresh)
    acc_ref[...] = accstay_ref[...]
    for k in range(MOVES):
        acc_ref[pl.ds(slots_ref[k], 1), :] = old_ref[pl.ds(k, 1), :]
    for copy in copies:
        copy.wait()


def arrive(peers, slots, got, second, stayed, accstay):
    blocks, block, feature = stayed.shape
    vm = pl.BlockSpec(memory_space=VM)
    sm = pl.BlockSpec(memory_space=SM)
    hbm = pl.BlockSpec(memory_space=pl.ANY)
    return pl.pallas_call(
        arrive_kernel,
        out_shape=(
            jax.ShapeDtypeStruct(stayed.shape, jnp.float32),
            jax.ShapeDtypeStruct(accstay.shape, jnp.float32),
        ),
        in_specs=[sm, sm, vm, vm, hbm, vm],
        out_specs=(hbm, vm),
        scratch_shapes=[
            VM((MOVES, block, feature), jnp.float32),
            VM((LANES, LANES), jnp.float32),
            pltpu.SemaphoreType.DMA((MOVES,)),
        ],
        input_output_aliases={4: 0},
        compiler_params=pltpu.CompilerParams(vmem_limit_bytes=12 * MIB),
        name="arrive",
    )(peers, slots, got, second, stayed, accstay)


def listed(mask, values):
    position = jnp.cumsum(mask.astype(jnp.int32)) - 1
    hit = mask[None, :] & (position[None, :] == jnp.arange(MOVES, dtype=jnp.int32)[:, None])
    return [jnp.sum(jnp.where(hit, v[None, :], 0), axis=1) for v in values]


def on_device(table, accumulator, grads_one, ids_one, grads_two, ids_two, new_slot):
    blocks, block, feature = table.shape
    peers = lax.axis_size("row")
    total = lax.axis_size("table") * peers
    group = lax.axis_index("table")
    mine = lax.axis_index("row")
    device = group * peers + mine
    rows = grads_one.shape[0]
    cap = 2 * rows // total

    slot_table = new_slot.reshape(-1, LANES).T
    outgoing = pack(ids_one.reshape(1, rows), ids_two.reshape(1, rows), slot_table, grads_one, grads_two, total, blocks, cap)
    got = lax.all_to_all(outgoing, ("table", "row"), split_axis=0, concat_axis=0, tiled=True)

    here = lax.dynamic_slice_in_dim(new_slot, group * peers * blocks, peers * blocks).reshape(peers, blocks)
    own = lax.dynamic_slice_in_dim(new_slot, device * blocks, blocks)
    came_from, go_to = listed(own // blocks != device, (jnp.arange(blocks, dtype=jnp.int32), own // blocks % peers))
    peer = jnp.arange(peers, dtype=jnp.int32)
    to_me = (here // blocks == device) & (peer != mine)[:, None]
    slots = jnp.sum(jnp.where(to_me, here - device * blocks + 1, 0), axis=1)
    from_peer, slots = listed(slots > 0, (peer, slots - 1))

    names, moving = leave(came_from, go_to, table, accumulator, got, peers, total, cap)
    moved = lax.all_to_all(moving, "row", split_axis=0, concat_axis=0, tiled=True)
    stayed, accstay, second = stay(names, slots, table, accumulator, got, total, cap)
    return arrive(from_peer, slots, moved, second, stayed, accstay)


def solution(mesh):
    in_specs = (
        P(("table", "row"), None, None),
        P(("table", "row"), None),
        P(("table", "row"), None),
        P(("table", "row")),
        P(("table", "row"), None),
        P(("table", "row")),
        P(),
    )
    out_specs = (P(("table", "row"), None, None), P(("table", "row"), None))
    return jax.shard_map(
        on_device, mesh=mesh, in_specs=in_specs, out_specs=out_specs, check_vma=False
    )
```

```python
import jax
import jax.numpy as jnp
from jax import lax
from jax.experimental import pallas as pl
from jax.experimental.pallas import tpu as pltpu
from jax.sharding import PartitionSpec as P

LEARN = 0.5
EPSILON = 1e-08
LANES = 128
MOVES = 12
VM = pltpu.VMEM
SM = pltpu.SMEM
ALL_VMEM = 67043328
LEAVE_ROOM = 14000000
MIB = 1024 * 1024


def iota(shape, dim):
    return lax.broadcasted_iota(jnp.int32, shape, dim)


def dot(a, b, contract):
    return lax.dot_general(a, b, ((contract[:1], contract[1:]), ((), ())), preferred_element_type=jnp.float32)


def lookup(which_ref, indices):
    high, low = which_ref.shape
    pick = (iota((high, indices.shape[1]), 0) == (indices >> 7)).astype(jnp.bfloat16)
    found = jnp.zeros((low, indices.shape[1]), jnp.float32)
    table = jnp.concatenate([which_ref[...].astype(jnp.float32), jnp.zeros((low - high, low), jnp.float32)], axis=0)
    table = jnp.transpose(table)[:, :high].astype(jnp.int32)
    for part, scale in ((table >> 7, 128.0), (table & 127, 1.0)):
        found += dot(part.astype(jnp.float32).astype(jnp.bfloat16), pick, (1, 0)) * scale
    here = iota(found.shape, 0) == (indices & 127)
    return jnp.sum(jnp.where(here, found, 0.0), axis=0, keepdims=True).astype(jnp.int32)


def pack_kernel(one_ids, two_ids, slot_hbm, one_hbm, two_hbm, out_hbm, one_ref, two_ref, ids_ref, ids2_ref, slot_ref, place_v, place_s, names_v, out_ref, sems, *, total, blocks, cap):
    stride = 2 * cap + 1
    rows = one_ref.shape[0]
    chunks = rows // LANES
    pairs = ((one_ids, ids_ref), (two_ids, ids2_ref), (slot_hbm, slot_ref), (one_hbm, one_ref), (two_hbm, two_ref))
    copies = [pltpu.make_async_copy(src, dst, sems.at[n]) for n, (src, dst) in enumerate(pairs)]
    for copy in copies:
        copy.start()
    for copy in copies[:3]:
        copy.wait()
    ids = ids_ref[...]
    ids2 = ids2_ref[...]
    block_slots = (ids >> 7, lookup(slot_ref, ids2 >> 7))
    inner = (ids & 127, ids2 & 127)
    upper = jnp.where(iota((LANES, 2 * LANES), 0) < iota((LANES, 2 * LANES), 1), 1.0, 0.0).astype(jnp.bfloat16)
    lane_slot = iota((LANES, LANES), 0) & (2 * cap - 1)
    high = jnp.zeros((total, LANES), jnp.float32)
    low = jnp.zeros((total, LANES), jnp.float32)
    for step in range(2):
        slot = block_slots[step]
        owner = (slot * 43691) >> 22
        named = (slot - owner * blocks) * LANES + inner[step] + 1
        carry = jnp.zeros((total, LANES), jnp.float32)
        for c in range(chunks):
            at = slice(c * LANES, (c + 1) * LANES)
            own = owner[:, at]
            name = named[:, at]
            mine = iota((total, LANES), 0) == own
            counted = dot(jnp.where(mine, 1.0, 0.0).astype(jnp.bfloat16), upper, (1, 0))
            before = counted[:, :LANES] + carry
            carry = carry + counted[:, LANES:]
            within = jnp.sum(jnp.where(mine, before, 0.0), axis=0, keepdims=True).astype(jnp.int32) + step * cap
            place_v[pl.ds(step * chunks + c, 1), :] = own * stride + within
            where = jnp.where(lane_slot == within, 1.0, 0.0).astype(jnp.bfloat16)
            high += dot(jnp.where(mine, (name >> 7).astype(jnp.float32), 0.0).astype(jnp.bfloat16), where, (1, 1))
            low += dot(jnp.where(mine, (name & 127).astype(jnp.float32), 0.0).astype(jnp.bfloat16), where, (1, 1))
    to_scalar = pltpu.make_async_copy(place_v, place_s, sems.at[5])
    to_scalar.start()
    names_v[...] = high * 128.0 + low

    def names(d, _):
        base = d * 8
        tile = names_v[pl.ds(base, 8), :]
        for j in range(8):
            out_ref[(base + j) * stride + stride - 1] = tile[j : j + 1, :]
        return 0

    lax.fori_loop(0, total // 8, names, 0, unroll=2)
    to_scalar.wait()
    for copy in copies[3:]:
        copy.wait()
    for step, src in enumerate((one_ref, two_ref)):

        def move(c, _):
            for g in range(LANES // 8):
                tile = src[pl.ds(c * LANES + g * 8, 8), :]
                for j in range(8):
                    out_ref[place_s[step * chunks + c, g * 8 + j]] = tile[j : j + 1, :]
            return 0

        lax.fori_loop(0, chunks, move, 0)
    whole = pltpu.make_async_copy(out_ref, out_hbm, sems.at[6])
    whole.start()
    whole.wait()


def pack(one_ids, two_ids, slots, one, two, total, blocks, cap):
    rows, feature = one.shape
    hbm = pl.BlockSpec(memory_space=pltpu.HBM)
    stride = 2 * cap + 1
    return pl.pallas_call(
        lambda *refs: pack_kernel(*refs, total=total, blocks=blocks, cap=cap),
        out_shape=jax.ShapeDtypeStruct((total * stride, 1, feature), jnp.float32),
        in_specs=[hbm] * 5,
        out_specs=hbm,
        scratch_shapes=[
            VM((rows, feature), jnp.float32),
            VM((rows, feature), jnp.float32),
            VM((1, rows), jnp.int32),
            VM((1, rows), jnp.int32),
            VM(slots.shape, jnp.int32),
            VM((2 * rows // LANES, LANES), jnp.int32),
            SM((2 * rows // LANES, LANES), jnp.int32),
            VM((total, LANES), jnp.float32),
            VM((total * stride, 1, feature), jnp.float32),
            pltpu.SemaphoreType.DMA((7,)),
        ],
        compiler_params=pltpu.CompilerParams(vmem_limit_bytes=ALL_VMEM),
        name="pack",
    )(one_ids, two_ids, slots, one, two)


def read_names(got_ref, names_v, names_s, sem, *, total, cap, dump):
    width = 2 * cap
    stride = width + 1
    per = LANES // width
    group = iota((1, LANES), 1) // width
    for a in range(total // per):
        row = got_ref[a * per * stride + stride - 1]
        for k in range(1, per):
            row = jnp.where(group == k, got_ref[(a * per + k) * stride + stride - 1], row)
        names_v[pl.ds(a, 1), :] = row.astype(jnp.int32)
    named = names_v[...]
    names_v[...] = jnp.where(named > 0, named - 1, dump)
    copy = pltpu.make_async_copy(names_v, names_s, sem)
    copy.start()
    copy.wait()


def add_rows(names_s, got_ref, sums_ref, *, total, cap, offset):
    width = 2 * cap
    stride = width + 1
    per = LANES // width

    def step(a, _):
        for k in range(per):
            base = (a * per + k) * stride + offset
            rows = [names_s[a, k * width + offset + j] for j in range(cap)]
            new = [sums_ref[pl.ds(r, 1), :] + got_ref[base + j] for j, r in enumerate(rows)]
            for r, value in zip(rows, new):
                sums_ref[pl.ds(r, 1), :] = value
        return 0

    lax.fori_loop(0, total // per, step, 0)


def square_sums(block):
    return jnp.sum(block * block, axis=1, keepdims=True)


def rate(accums):
    return LEARN / (jnp.sqrt(accums) + EPSILON)


def lane_of(columns, k):
    return columns[:, k : k + 1]


def fetch_kernel(from_ref, table_ref, acc_ref, out_ref, old_ref, sems):
    copies = [pltpu.make_async_copy(table_ref.at[from_ref[k]], out_ref.at[k], sems.at[k]) for k in range(MOVES)]
    for copy in copies:
        copy.start()
    old_ref[...] = jnp.zeros_like(old_ref)
    for k in range(MOVES):
        old_ref[pl.ds(k, 1), :] = acc_ref[pl.ds(from_ref[k], 1), :]
    for copy in copies:
        copy.wait()


def fetch(came_from, table, acc):
    vm = pl.BlockSpec(memory_space=VM)
    hbm = pl.BlockSpec(memory_space=pltpu.HBM)
    return pl.pallas_call(
        fetch_kernel,
        out_shape=(
            jax.ShapeDtypeStruct((MOVES,) + table.shape[1:], jnp.float32),
            jax.ShapeDtypeStruct((LANES, LANES), jnp.float32),
        ),
        in_specs=[pl.BlockSpec(memory_space=SM), hbm, vm],
        out_specs=(vm, vm),
        scratch_shapes=[pltpu.SemaphoreType.DMA((MOVES,))],
        compiler_params=pltpu.CompilerParams(vmem_limit_bytes=ALL_VMEM - LEAVE_ROOM),
        name="fetch",
    )(came_from, table, acc)


def leave_kernel(from_ref, to_ref, table_ref, acc_ref, got_ref, names_out, out_hbm, out_ref, sums_ref, old_ref, names_v, names_s, sems, *, total, cap, rows):
    block, feature = table_ref.shape[1:]
    spans = [pl.ds(pl.multiple_of(from_ref[k] * block, block), block) for k in range(MOVES)]
    for k in range(MOVES):
        sums_ref[spans[k], :] = jnp.zeros((block, feature), jnp.float32)
    read_names(got_ref, names_v, names_s, sems.at[MOVES], total=total, cap=cap, dump=rows)
    names_out[...] = names_v[...]
    add_rows(names_s, got_ref, sums_ref, total=total, cap=cap, offset=0)
    lane = iota((block, LANES), 1)
    squares = jnp.zeros((block, LANES), jnp.float32)
    for k in range(MOVES):
        squares = jnp.where(lane == k, square_sums(sums_ref[spans[k], :]), squares)
    fresh = jnp.transpose(acc_ref[...]) + squares * (1.0 / feature)
    rates = rate(jnp.where(lane < MOVES, fresh, 1.0))
    old_ref[...] = jnp.transpose(fresh)
    sends = []
    for k in range(MOVES):
        out_ref[k, pl.ds(block, 1), :] = old_ref[pl.ds(k, 1), :]
        out_ref[k, pl.ds(0, block), :] = table_ref[k] - lane_of(rates, k) * sums_ref[spans[k], :]
        sends.append(pltpu.make_async_copy(out_ref.at[k], out_hbm.at[to_ref[k]], sems.at[k]))
        sends[-1].start()
    for send in sends:
        send.wait()


def leave(came_from, go_to, table, acc, got, peers, total, cap, rows):
    block, feature = table.shape[1:]
    vm = pl.BlockSpec(memory_space=VM)
    sm = pl.BlockSpec(memory_space=SM)
    names = (total * 2 * cap // LANES, LANES)
    return pl.pallas_call(
        lambda *refs: leave_kernel(*refs, total=total, cap=cap, rows=rows),
        out_shape=(
            jax.ShapeDtypeStruct(names, jnp.int32),
            jax.ShapeDtypeStruct((peers, block + 8, feature), jnp.float32),
        ),
        in_specs=[sm, sm, vm, vm, vm],
        out_specs=(vm, pl.BlockSpec(memory_space=pltpu.HBM)),
        scratch_shapes=[
            VM((MOVES, block + 8, feature), jnp.float32),
            VM((rows + 8, feature), jnp.float32),
            VM((LANES, LANES), jnp.float32),
            VM(names, jnp.int32),
            SM(names, jnp.int32),
            pltpu.SemaphoreType.DMA((MOVES + 1,)),
        ],
        compiler_params=pltpu.CompilerParams(vmem_limit_bytes=ALL_VMEM - LEAVE_ROOM),
        name="leave",
    )(came_from, go_to, table, acc, got)


def stay_kernel(names_ref, slots_ref, table_ref, acc_ref, got_ref, out_ref, accout_ref, arrive_ref, one_ref, two_ref, rates_ref, *, total, cap, blocks):
    i = pl.program_id(0)
    each, block, feature = table_ref.shape

    @pl.when(i == 0)
    def _():
        def clear(b, _):
            at = pl.ds(pl.multiple_of(b * block, block), block)
            one_ref[at, :] = jnp.zeros((block, feature), jnp.float32)
            two_ref[at, :] = jnp.zeros((block, feature), jnp.float32)
            return 0

        lax.fori_loop(0, blocks, clear, 0)
        add_rows(names_ref, got_ref, one_ref, total=total, cap=cap, offset=0)
        add_rows(names_ref, got_ref, two_ref, total=total, cap=cap, offset=cap)
        lane = iota((block, LANES), 1)

        def squares(g, sums):
            sums = list(sums)
            for k in range(4):
                b = g * 4 + k
                at = pl.ds(pl.multiple_of(b * block, block), block)
                for n, ref in enumerate((one_ref, two_ref)):
                    sums[n] = jnp.where(lane == b, square_sums(ref[at, :]), sums[n])
            return tuple(sums)

        zero = jnp.zeros((block, LANES), jnp.float32)
        first, second = lax.fori_loop(0, blocks // 4, squares, (zero, zero))
        old = jnp.concatenate([acc_ref[...], jnp.ones((LANES - blocks, LANES), jnp.float32)], axis=0)
        fresh = jnp.transpose(old) + first * (1.0 / feature)
        rates_ref[0] = rate(fresh)
        fresh = fresh + second * (1.0 / feature)
        rates_ref[1] = rate(fresh)
        accout_ref[...] = jnp.transpose(fresh)[:blocks, :]
        for k in range(MOVES):
            at = pl.ds(pl.multiple_of(slots_ref[k] * block, block), block)
            arrive_ref[k] = two_ref[at, :]

    turn = (LANES - each * i) % LANES
    one_rate = pltpu.roll(rates_ref[0], turn, 1)
    two_rate = pltpu.roll(rates_ref[1], turn, 1)
    for k in range(each):
        at = pl.ds(pl.multiple_of((i * each + k) * block, block), block)
        weights = table_ref[k] - lane_of(one_rate, k) * one_ref[at, :]
        out_ref[k] = weights - lane_of(two_rate, k) * two_ref[at, :]


def stay(names, slots, table, acc, got, total, cap, each=8):
    blocks, block, feature = table.shape
    vm = pl.BlockSpec(memory_space=VM)
    sm = pl.BlockSpec(memory_space=SM)
    piece = pl.BlockSpec((each, block, feature), lambda i: (i, 0, 0))
    return pl.pallas_call(
        lambda *refs: stay_kernel(*refs, total=total, cap=cap, blocks=blocks),
        grid=(blocks // each,),
        out_shape=(
            jax.ShapeDtypeStruct(table.shape, jnp.float32),
            jax.ShapeDtypeStruct(acc.shape, jnp.float32),
            jax.ShapeDtypeStruct((MOVES, block, feature), jnp.float32),
        ),
        in_specs=[sm, sm, piece, vm, vm],
        out_specs=(piece, vm, vm),
        scratch_shapes=[
            VM((blocks * block + 8, feature), jnp.float32),
            VM((blocks * block + 8, feature), jnp.float32),
            VM((2, LANES, LANES), jnp.float32),
        ],
        compiler_params=pltpu.CompilerParams(vmem_limit_bytes=28 * MIB),
        name="stay",
    )(names, slots, table, acc, got)


def arrive_kernel(peers_ref, slots_ref, got_hbm, second_ref, stayed_ref, accstay_ref, out_ref, acc_ref, got_ref, buf_ref, old_ref, sems):
    takes = [pltpu.make_async_copy(got_hbm.at[peers_ref[k]], got_ref.at[k], sems.at[k]) for k in range(MOVES)]
    for take in takes:
        take.start()
    block, feature = stayed_ref.shape[1:]
    lane = iota((block, LANES), 1)
    squares = jnp.zeros((block, LANES), jnp.float32)
    for k in range(MOVES):
        squares = jnp.where(lane == k, square_sums(second_ref[k]), squares)
    for k in range(MOVES):
        takes[k].wait()
        old_ref[pl.ds(k, 1), :] = got_ref[k, pl.ds(block, 1), :]
    fresh = jnp.transpose(old_ref[...]) + squares * (1.0 / feature)
    rates = rate(jnp.where(lane < MOVES, fresh, 1.0))
    copies = []
    for k in range(MOVES):
        buf_ref[k] = got_ref[k, pl.ds(0, block), :] - lane_of(rates, k) * second_ref[k]
        copies.append(pltpu.make_async_copy(buf_ref.at[k], out_ref.at[slots_ref[k]], sems.at[k]))
        copies[-1].start()
    old_ref[...] = jnp.transpose(fresh)
    acc_ref[...] = accstay_ref[...]
    for k in range(MOVES):
        acc_ref[pl.ds(slots_ref[k], 1), :] = old_ref[pl.ds(k, 1), :]
    for copy in copies:
        copy.wait()


def arrive(peers, slots, got, second, stayed, accstay):
    blocks, block, feature = stayed.shape
    vm = pl.BlockSpec(memory_space=VM)
    sm = pl.BlockSpec(memory_space=SM)
    hbm = pl.BlockSpec(memory_space=pltpu.HBM)
    return pl.pallas_call(
        arrive_kernel,
        out_shape=(
            jax.ShapeDtypeStruct(stayed.shape, jnp.float32),
            jax.ShapeDtypeStruct(accstay.shape, jnp.float32),
        ),
        in_specs=[sm, sm, hbm, vm, hbm, vm],
        out_specs=(hbm, vm),
        scratch_shapes=[
            VM((MOVES,) + got.shape[1:], jnp.float32),
            VM((MOVES, block, feature), jnp.float32),
            VM((LANES, LANES), jnp.float32),
            pltpu.SemaphoreType.DMA((MOVES,)),
        ],
        input_output_aliases={4: 0},
        compiler_params=pltpu.CompilerParams(vmem_limit_bytes=ALL_VMEM),
        name="arrive",
    )(peers, slots, got, second, stayed, accstay)


def listed(mask, values):
    position = jnp.cumsum(mask.astype(jnp.int32)) - 1
    hit = mask[None, :] & (position[None, :] == jnp.arange(MOVES, dtype=jnp.int32)[:, None])
    return [jnp.sum(jnp.where(hit, v[None, :], 0), axis=1) for v in values]


def on_device(table, accumulator, grads_one, ids_one, grads_two, ids_two, new_slot):
    blocks, block, feature = table.shape
    peers = lax.axis_size("row")
    total = lax.axis_size("table") * peers
    group = lax.axis_index("table")
    mine = lax.axis_index("row")
    device = group * peers + mine
    rows = grads_one.shape[0]
    cap = 2 * rows // total

    slot_table = new_slot.reshape(-1, LANES)
    outgoing = pack(ids_one.reshape(1, rows), ids_two.reshape(1, rows), slot_table, grads_one, grads_two, total, blocks, cap)
    got = lax.all_to_all(outgoing, ("table", "row"), split_axis=0, concat_axis=0, tiled=True)

    here = lax.dynamic_slice_in_dim(new_slot, group * peers * blocks, peers * blocks).reshape(peers, blocks)
    own = lax.dynamic_slice_in_dim(new_slot, device * blocks, blocks)
    came_from, go_to = listed(own // blocks != device, (jnp.arange(blocks, dtype=jnp.int32), own // blocks % peers))
    peer = jnp.arange(peers, dtype=jnp.int32)
    to_me = (here // blocks == device) & (peer != mine)[:, None]
    slots = jnp.sum(jnp.where(to_me, here - device * blocks + 1, 0), axis=1)
    from_peer, slots = listed(slots > 0, (peer, slots - 1))

    gone, old = fetch(came_from, table, accumulator)
    names, moving = leave(came_from, go_to, gone, old, got, peers, total, cap, blocks * block)
    moved = lax.all_to_all(moving, "row", split_axis=0, concat_axis=0, tiled=True)
    stayed, accstay, second = stay(names, slots, table, accumulator, got, total, cap)
    return arrive(from_peer, slots, moved, second, stayed, accstay)


def solution(mesh):
    in_specs = (
        P(("table", "row"), None, None),
        P(("table", "row"), None),
        P(("table", "row"), None),
        P(("table", "row")),
        P(("table", "row"), None),
        P(("table", "row")),
        P(),
    )
    out_specs = (P(("table", "row"), None, None), P(("table", "row"), None))
    return jax.shard_map(
        on_device, mesh=mesh, in_specs=in_specs, out_specs=out_specs, check_vma=False
    )
```

```python
import jax
import jax.numpy as jnp
from jax import lax
from jax.experimental import pallas as pl
from jax.experimental.pallas import tpu as pltpu
from jax.sharding import PartitionSpec as P

LEARN = 0.5
EPSILON = 1e-08
LANES = 128
MOVES = 12
VM = pltpu.VMEM
SM = pltpu.SMEM
ALL_VMEM = 67043328
ROOM = 14000000


def iota(shape, dim):
    return lax.broadcasted_iota(jnp.int32, shape, dim)


def dot(a, b, contract):
    return lax.dot_general(a, b, ((contract[:1], contract[1:]), ((), ())), preferred_element_type=jnp.float32)


def lookup(which_ref, indices):
    high, low = which_ref.shape
    pick = (iota((high, indices.shape[1]), 0) == (indices >> 7)).astype(jnp.bfloat16)
    found = jnp.zeros((low, indices.shape[1]), jnp.float32)
    table = jnp.concatenate([which_ref[...].astype(jnp.float32), jnp.zeros((low - high, low), jnp.float32)], axis=0)
    table = jnp.transpose(table)[:, :high].astype(jnp.int32)
    for part, scale in ((table >> 7, 128.0), (table & 127, 1.0)):
        found += dot(part.astype(jnp.float32).astype(jnp.bfloat16), pick, (1, 0)) * scale
    here = iota(found.shape, 0) == (indices & 127)
    return jnp.sum(jnp.where(here, found, 0.0), axis=0, keepdims=True).astype(jnp.int32)


def pack_kernel(one_ids, two_ids, slot_hbm, one_hbm, two_hbm, out_hbm, one_ref, two_ref, ids_ref, ids2_ref, slot_ref, place_v, place2_v, place_s, place2_s, names_v, out_ref, sems, *, blocks, cap):
    total, stride = out_ref.shape[:2]
    rows = one_ref.shape[0]
    chunks = rows // LANES
    pairs = ((one_ids, ids_ref), (two_ids, ids2_ref), (slot_hbm, slot_ref), (one_hbm, one_ref), (two_hbm, two_ref))
    copies = [pltpu.make_async_copy(src, dst, sems.at[n]) for n, (src, dst) in enumerate(pairs)]
    for copy in copies:
        copy.start()
    for copy in copies[:3]:
        copy.wait()
    ids = ids_ref[...]
    ids2 = ids2_ref[...]
    held = ids >> 7
    leaving = lookup(slot_ref, held) != held
    block_slots = (held, lookup(slot_ref, ids2 >> 7))
    inner = (ids & 127, ids2 & 127)
    upper = jnp.where(iota((LANES, 2 * LANES), 0) < iota((LANES, 2 * LANES), 1), 1.0, 0.0).astype(jnp.bfloat16)
    everywhere = jnp.ones((LANES, LANES), jnp.bfloat16)
    lane_slot = iota((LANES, LANES), 0) & (2 * cap - 1)
    high = jnp.zeros((total, LANES), jnp.float32)
    low = jnp.zeros((total, LANES), jnp.float32)
    places = ((place_v, place_s), (place2_v, place2_s))
    to_scalar = [pltpu.make_async_copy(v, s, sems.at[5 + n]) for n, (v, s) in enumerate(places)]
    for step in range(2):
        slot = block_slots[step]
        owner = (slot * 43691) >> 22
        named = (slot - owner * blocks) * LANES + inner[step] + 1
        carry = jnp.zeros((total, LANES), jnp.float32)
        carry_first = jnp.zeros((total, LANES), jnp.float32)
        spots = [slice(c * LANES, (c + 1) * LANES) for c in range(chunks)]
        if step == 0:
            firsts = jnp.zeros((total, LANES), jnp.float32)
            for at in spots:
                mine = (iota((total, LANES), 0) == owner[:, at]) & leaving[:, at]
                firsts += dot(jnp.where(mine, 1.0, 0.0).astype(jnp.bfloat16), everywhere, (1, 0))
        for c, at in enumerate(spots):
            own = owner[:, at]
            name = named[:, at]
            mine = iota((total, LANES), 0) == own
            counted = dot(jnp.where(mine, 1.0, 0.0).astype(jnp.bfloat16), upper, (1, 0))
            before = counted[:, :LANES] + carry
            carry = carry + counted[:, LANES:]
            if step == 0:
                early = leaving[:, at]
                counted = dot(jnp.where(mine & early, 1.0, 0.0).astype(jnp.bfloat16), upper, (1, 0))
                before_first = counted[:, :LANES] + carry_first
                carry_first = carry_first + counted[:, LANES:]
                before = jnp.where(early, before_first, firsts + before - before_first)
            within = jnp.sum(jnp.where(mine, before, 0.0), axis=0, keepdims=True).astype(jnp.int32) + step * cap
            places[step][0][pl.ds(c, 1), :] = own * stride + within
            where = jnp.where(lane_slot == within, 1.0, 0.0).astype(jnp.bfloat16)
            high += dot(jnp.where(mine, (name >> 7).astype(jnp.float32), 0.0).astype(jnp.bfloat16), where, (1, 1))
            low += dot(jnp.where(mine, (name & 127).astype(jnp.float32), 0.0).astype(jnp.bfloat16), where, (1, 1))
        to_scalar[step].start()
    names_v[...] = high * 128.0 + low
    flat = out_ref.reshape(total * stride, 1, LANES)

    def move(src, place):
        def chunk(c, _):
            for g in range(LANES // 8):
                tile = src[pl.ds(c * LANES + g * 8, 8), :]
                for j in range(8):
                    flat[place[c, g * 8 + j]] = tile[j : j + 1, :]
            return 0

        lax.fori_loop(0, chunks, chunk, 0)

    to_scalar[0].wait()
    copies[3].wait()
    move(one_ref, place_s)
    first = pltpu.make_async_copy(out_ref.at[:, pl.ds(0, cap)], out_hbm.at[:, pl.ds(0, cap)], sems.at[7])
    first.start()

    def names(d, _):
        base = d * 8
        tile = names_v[pl.ds(base, 8), :]
        for j in range(8):
            out_ref[base + j, stride - 1] = tile[j : j + 1, :]
        return 0

    lax.fori_loop(0, total // 8, names, 0, unroll=2)
    to_scalar[1].wait()
    copies[4].wait()
    move(two_ref, place2_s)
    second = pltpu.make_async_copy(out_ref.at[:, pl.ds(cap, cap + 1)], out_hbm.at[:, pl.ds(cap, cap + 1)], sems.at[8])
    second.start()
    first.wait()
    second.wait()


def pack(one_ids, two_ids, slots, one, two, total, blocks, cap):
    rows, feature = one.shape
    hbm = pl.BlockSpec(memory_space=pltpu.HBM)
    message = (total, 2 * cap + 1, 1, feature)
    place = (rows // LANES, LANES)
    return pl.pallas_call(
        lambda *refs: pack_kernel(*refs, blocks=blocks, cap=cap),
        out_shape=jax.ShapeDtypeStruct(message, jnp.float32),
        in_specs=[hbm] * 5,
        out_specs=hbm,
        scratch_shapes=[
            VM((rows, feature), jnp.float32),
            VM((rows, feature), jnp.float32),
            VM((1, rows), jnp.int32),
            VM((1, rows), jnp.int32),
            VM(slots.shape, jnp.int32),
            VM(place, jnp.int32),
            VM(place, jnp.int32),
            SM(place, jnp.int32),
            SM(place, jnp.int32),
            VM((total, LANES), jnp.float32),
            VM(message, jnp.float32),
            pltpu.SemaphoreType.DMA((9,)),
        ],
        compiler_params=pltpu.CompilerParams(vmem_limit_bytes=ALL_VMEM),
        name="pack",
    )(one_ids, two_ids, slots, one, two)


def read_names(got_ref, names_v, copy, *, dump):
    total, stride = got_ref.shape[:2]
    width = stride - 1
    per = LANES // width
    group = iota((1, LANES), 1) // width
    for a in range(total // per):
        row = got_ref[a * per, width]
        for k in range(1, per):
            row = jnp.where(group == k, got_ref[a * per + k, width], row)
        names_v[pl.ds(a, 1), :] = row.astype(jnp.int32)
    named = names_v[...]
    named = jnp.where(named > 0, named - 1, dump)
    names_v[...] = named
    copy.start()
    return named


def add_rows(names_s, got_ref, sums_refs, *, offset, count):
    total, stride = got_ref.shape[:2]
    width = stride - 1
    per = LANES // width

    def step(a, _):
        for k in range(per):
            sums_ref = sums_refs[k % len(sums_refs)]
            rows = [names_s[a, k * width + offset + j] for j in range(count)]
            new = [sums_ref[pl.ds(r, 1), :] + got_ref[a * per + k, offset + j] for j, r in enumerate(rows)]
            for r, value in zip(rows, new):
                sums_ref[pl.ds(r, 1), :] = value
        return 0

    lax.fori_loop(0, total // per, step, 0)


def square_sums(block):
    return jnp.sum(block * block, axis=1, keepdims=True)


def rate(accums):
    return LEARN / (jnp.sqrt(accums) + EPSILON)


def lane_of(columns, k):
    return columns[:, k : k + 1]


def fetch_kernel(from_ref, table_ref, acc_ref, out_ref, old_ref, sems):
    copies = [pltpu.make_async_copy(table_ref.at[from_ref[k]], out_ref.at[k], sems.at[k]) for k in range(MOVES)]
    for copy in copies:
        copy.start()
    old_ref[...] = jnp.zeros_like(old_ref)
    for k in range(MOVES):
        old_ref[pl.ds(k, 1), :] = acc_ref[pl.ds(from_ref[k], 1), :]
    for copy in copies:
        copy.wait()


def fetch(came_from, table, acc):
    vm = pl.BlockSpec(memory_space=VM)
    hbm = pl.BlockSpec(memory_space=pltpu.HBM)
    return pl.pallas_call(
        fetch_kernel,
        out_shape=(
            jax.ShapeDtypeStruct((MOVES,) + table.shape[1:], jnp.float32),
            jax.ShapeDtypeStruct((LANES, LANES), jnp.float32),
        ),
        in_specs=[pl.BlockSpec(memory_space=SM), hbm, vm],
        out_specs=(vm, vm),
        scratch_shapes=[pltpu.SemaphoreType.DMA((MOVES,))],
        compiler_params=pltpu.CompilerParams(vmem_limit_bytes=ALL_VMEM - ROOM),
        name="fetch",
    )(came_from, table, acc)


ROUND = 4


def leave_kernel(from_ref, to_ref, table_ref, acc_ref, got_ref, names_out, out_hbm, out_ref, even_ref, odd_ref, old_ref, names_v, names_s, sems, *, cap, rows):
    block, feature = table_ref.shape[1:]
    spans = [pl.ds(pl.multiple_of(from_ref[k] * block, block), block) for k in range(MOVES)]
    to_scalar = pltpu.make_async_copy(names_v, names_s, sems.at[MOVES])
    named = read_names(got_ref, names_v, to_scalar, dump=rows)
    names_out[...] = named
    at = iota(named.shape, 1) & (2 * cap - 1)
    goes = jnp.zeros(named.shape, jnp.bool_)
    for k in range(MOVES):
        goes = goes | ((named >> 7) == from_ref[k])
    needed = jnp.max(jnp.where(goes & (at < cap), at + 1, 0))
    for k in range(MOVES):
        even_ref[spans[k], :] = jnp.zeros((block, feature), jnp.float32)
        odd_ref[spans[k], :] = jnp.zeros((block, feature), jnp.float32)
    to_scalar.wait()

    def some(r, _):
        add_rows(names_s, got_ref, (even_ref, odd_ref), offset=r * ROUND, count=ROUND)
        return 0

    lax.fori_loop(0, (needed + ROUND - 1) // ROUND, some, 0)
    lane = iota((block, LANES), 1)
    squares = jnp.zeros((block, LANES), jnp.float32)
    for k in range(MOVES):
        gradient = even_ref[spans[k], :] + odd_ref[spans[k], :]
        even_ref[spans[k], :] = gradient
        squares = jnp.where(lane == k, square_sums(gradient), squares)
    fresh = jnp.transpose(acc_ref[...]) + squares * (1.0 / feature)
    rates = rate(jnp.where(lane < MOVES, fresh, 1.0))
    old_ref[...] = jnp.transpose(fresh)
    sends = []
    for k in range(MOVES):
        out_ref[k, pl.ds(block, 1), :] = old_ref[pl.ds(k, 1), :]
        out_ref[k, pl.ds(0, block), :] = table_ref[k] - lane_of(rates, k) * even_ref[spans[k], :]
        sends.append(pltpu.make_async_copy(out_ref.at[k], out_hbm.at[to_ref[k]], sems.at[k]))
        sends[-1].start()
    for send in sends:
        send.wait()


def leave(came_from, go_to, table, acc, got, peers, cap, rows):
    block, feature = table.shape[1:]
    vm = pl.BlockSpec(memory_space=VM)
    sm = pl.BlockSpec(memory_space=SM)
    names = (got.shape[0] * 2 * cap // LANES, LANES)
    return pl.pallas_call(
        lambda *refs: leave_kernel(*refs, cap=cap, rows=rows),
        out_shape=(
            jax.ShapeDtypeStruct(names, jnp.int32),
            jax.ShapeDtypeStruct((peers, block + 8, feature), jnp.float32),
        ),
        in_specs=[sm, sm, vm, vm, vm],
        out_specs=(vm, pl.BlockSpec(memory_space=pltpu.HBM)),
        scratch_shapes=[
            VM((MOVES, block + 8, feature), jnp.float32),
            VM((rows + 8, feature), jnp.float32),
            VM((rows + 8, feature), jnp.float32),
            VM((LANES, LANES), jnp.float32),
            VM(names, jnp.int32),
            SM(names, jnp.int32),
            pltpu.SemaphoreType.DMA((MOVES + 1,)),
        ],
        compiler_params=pltpu.CompilerParams(vmem_limit_bytes=ALL_VMEM - ROOM),
        name="leave",
    )(came_from, go_to, table, acc, got)


def stay_kernel(names_ref, slots_ref, table_ref, acc_ref, got_ref, out_ref, accout_ref, arrive_ref, squares_ref, one_ref, two_ref, rates_ref, *, cap, blocks):
    i = pl.program_id(0)
    each, block, feature = table_ref.shape

    @pl.when(i == 0)
    def _():
        def clear(b, _):
            at = pl.ds(pl.multiple_of(b * block, block), block)
            one_ref[at, :] = jnp.zeros((block, feature), jnp.float32)
            two_ref[at, :] = jnp.zeros((block, feature), jnp.float32)
            return 0

        lax.fori_loop(0, blocks, clear, 0)
        add_rows(names_ref, got_ref, (one_ref,), offset=0, count=cap)
        add_rows(names_ref, got_ref, (two_ref,), offset=cap, count=cap)
        lane = iota((block, LANES), 1)

        def squares(g, sums):
            sums = list(sums)
            for k in range(4):
                b = g * 4 + k
                at = pl.ds(pl.multiple_of(b * block, block), block)
                for n, ref in enumerate((one_ref, two_ref)):
                    sums[n] = jnp.where(lane == b, square_sums(ref[at, :]), sums[n])
            return tuple(sums)

        zero = jnp.zeros((block, LANES), jnp.float32)
        first, second = lax.fori_loop(0, blocks // 4, squares, (zero, zero))
        old = jnp.concatenate([acc_ref[...], jnp.ones((LANES - blocks, LANES), jnp.float32)], axis=0)
        fresh = jnp.transpose(old) + first * (1.0 / feature)
        rates_ref[0] = rate(fresh)
        fresh = fresh + second * (1.0 / feature)
        rates_ref[1] = rate(fresh)
        accout_ref[...] = jnp.transpose(fresh)[:blocks, :]
        arriving = zero
        for k in range(MOVES):
            at = pl.ds(pl.multiple_of(slots_ref[k] * block, block), block)
            arrive_ref[k] = two_ref[at, :]
            arriving = jnp.where(lane == k, square_sums(two_ref[at, :]), arriving)
        squares_ref[...] = arriving

    turn = (LANES - each * i) % LANES
    one_rate = pltpu.roll(rates_ref[0], turn, 1)
    two_rate = pltpu.roll(rates_ref[1], turn, 1)
    for k in range(each):
        at = pl.ds(pl.multiple_of((i * each + k) * block, block), block)
        weights = table_ref[k] - lane_of(one_rate, k) * one_ref[at, :]
        out_ref[k] = weights - lane_of(two_rate, k) * two_ref[at, :]


def stay(names, slots, table, acc, got, cap, each=8):
    blocks, block, feature = table.shape
    vm = pl.BlockSpec(memory_space=VM)
    sm = pl.BlockSpec(memory_space=SM)
    piece = pl.BlockSpec((each, block, feature), lambda i: (i, 0, 0))
    return pl.pallas_call(
        lambda *refs: stay_kernel(*refs, cap=cap, blocks=blocks),
        grid=(blocks // each,),
        out_shape=(
            jax.ShapeDtypeStruct(table.shape, jnp.float32),
            jax.ShapeDtypeStruct(acc.shape, jnp.float32),
            jax.ShapeDtypeStruct((MOVES, block, feature), jnp.float32),
            jax.ShapeDtypeStruct((LANES, LANES), jnp.float32),
        ),
        in_specs=[sm, sm, piece, vm, vm],
        out_specs=(piece, vm, vm, vm),
        scratch_shapes=[
            VM((blocks * block + 8, feature), jnp.float32),
            VM((blocks * block + 8, feature), jnp.float32),
            VM((2, LANES, LANES), jnp.float32),
        ],
        compiler_params=pltpu.CompilerParams(vmem_limit_bytes=ALL_VMEM - ROOM),
        name="stay",
    )(names, slots, table, acc, got)


def arrive_kernel(peers_ref, slots_ref, got_hbm, second_hbm, squares_hbm, stayed_ref, accstay_hbm, out_ref, acc_hbm, got_ref, second_ref, squares_ref, acc_ref, buf_ref, old_ref, sems):
    block, feature = stayed_ref.shape[1:]
    takes = [pltpu.make_async_copy(got_hbm.at[peers_ref[k]], got_ref.at[k], sems.at[k]) for k in range(MOVES)]
    pairs = ((squares_hbm, squares_ref), (accstay_hbm, acc_ref), (second_hbm, second_ref))
    rest = [pltpu.make_async_copy(src, dst, sems.at[MOVES + n]) for n, (src, dst) in enumerate(pairs)]
    for take in takes + rest:
        take.start()
    lane = iota((block, LANES), 1)
    for k in range(MOVES):
        takes[k].wait()
        old_ref[pl.ds(k, 1), :] = got_ref[k, pl.ds(block, 1), :]
    rest[0].wait()
    fresh = jnp.transpose(old_ref[...]) + squares_ref[...] * (1.0 / feature)
    rates = rate(jnp.where(lane < MOVES, fresh, 1.0))
    old_ref[...] = jnp.transpose(fresh)
    rest[1].wait()
    for k in range(MOVES):
        acc_ref[pl.ds(slots_ref[k], 1), :] = old_ref[pl.ds(k, 1), :]
    copies = [pltpu.make_async_copy(acc_ref, acc_hbm, sems.at[MOVES])]
    copies[0].start()
    rest[2].wait()
    for k in range(MOVES):
        buf_ref[k] = got_ref[k, pl.ds(0, block), :] - lane_of(rates, k) * second_ref[k]
        copies.append(pltpu.make_async_copy(buf_ref.at[k], out_ref.at[slots_ref[k]], sems.at[k]))
        copies[-1].start()
    for copy in copies:
        copy.wait()


def arrive(peers, slots, got, second, squares, stayed, accstay):
    blocks, block, feature = stayed.shape
    sm = pl.BlockSpec(memory_space=SM)
    hbm = pl.BlockSpec(memory_space=pltpu.HBM)
    return pl.pallas_call(
        arrive_kernel,
        out_shape=(
            jax.ShapeDtypeStruct(stayed.shape, jnp.float32),
            jax.ShapeDtypeStruct(accstay.shape, jnp.float32),
        ),
        in_specs=[sm, sm, hbm, hbm, hbm, hbm, hbm],
        out_specs=(hbm, hbm),
        scratch_shapes=[
            VM((MOVES,) + got.shape[1:], jnp.float32),
            VM(second.shape, jnp.float32),
            VM(squares.shape, jnp.float32),
            VM(accstay.shape, jnp.float32),
            VM((MOVES, block, feature), jnp.float32),
            VM((LANES, LANES), jnp.float32),
            pltpu.SemaphoreType.DMA((MOVES + 3,)),
        ],
        input_output_aliases={5: 0},
        compiler_params=pltpu.CompilerParams(vmem_limit_bytes=ALL_VMEM),
        name="arrive",
    )(peers, slots, got, second, squares, stayed, accstay)


def listed(mask, values):
    position = jnp.cumsum(mask.astype(jnp.int32)) - 1
    hit = mask[None, :] & (position[None, :] == jnp.arange(MOVES, dtype=jnp.int32)[:, None])
    return [jnp.sum(jnp.where(hit, v[None, :], 0), axis=1) for v in values]


def on_device(table, accumulator, grads_one, ids_one, grads_two, ids_two, new_slot):
    blocks, block, feature = table.shape
    peers = lax.axis_size("row")
    total = lax.axis_size("table") * peers
    group = lax.axis_index("table")
    mine = lax.axis_index("row")
    device = group * peers + mine
    rows = grads_one.shape[0]
    cap = 2 * rows // total

    slot_table = new_slot.reshape(-1, LANES)
    outgoing = pack(ids_one.reshape(1, rows), ids_two.reshape(1, rows), slot_table, grads_one, grads_two, total, blocks, cap)
    got = lax.all_to_all(outgoing, ("table", "row"), split_axis=0, concat_axis=0, tiled=True)

    here = lax.dynamic_slice_in_dim(new_slot, group * peers * blocks, peers * blocks).reshape(peers, blocks)
    own = lax.dynamic_slice_in_dim(new_slot, device * blocks, blocks)
    came_from, go_to = listed(own // blocks != device, (jnp.arange(blocks, dtype=jnp.int32), own // blocks % peers))
    peer = jnp.arange(peers, dtype=jnp.int32)
    to_me = (here // blocks == device) & (peer != mine)[:, None]
    slots = jnp.sum(jnp.where(to_me, here - device * blocks + 1, 0), axis=1)
    from_peer, slots = listed(slots > 0, (peer, slots - 1))

    gone, old = fetch(came_from, table, accumulator)
    names, moving = leave(came_from, go_to, gone, old, got, peers, cap, blocks * block)
    moved = lax.all_to_all(moving, "row", split_axis=0, concat_axis=0, tiled=True)
    stayed, accstay, second, squares = stay(names, slots, table, accumulator, got, cap)
    return arrive(from_peer, slots, moved, second, squares, stayed, accstay)


def solution(mesh):
    in_specs = (
        P(("table", "row"), None, None),
        P(("table", "row"), None),
        P(("table", "row"), None),
        P(("table", "row")),
        P(("table", "row"), None),
        P(("table", "row")),
        P(),
    )
    out_specs = (P(("table", "row"), None, None), P(("table", "row"), None))
    return jax.shard_map(
        on_device, mesh=mesh, in_specs=in_specs, out_specs=out_specs, check_vma=False
    )
```

```python
import jax
import jax.numpy as jnp
from jax import lax
from jax.experimental import pallas as pl
from jax.experimental.pallas import tpu as pltpu
from jax.sharding import PartitionSpec as P

LEARN = 0.5
EPSILON = 1e-08
LANES = 128
MOVES = 12
FROM, TO, SLOT, PEER = 0, MOVES, 2 * MOVES, 3 * MOVES
VM = pltpu.VMEM
SM = pltpu.SMEM
ALL_VMEM = 67043328
ROOM = 14000000
LAST_ROOM = 11500000


def iota(shape, dim):
    return lax.broadcasted_iota(jnp.int32, shape, dim)


def dot(a, b, contract):
    return lax.dot_general(a, b, ((contract[:1], contract[1:]), ((), ())), preferred_element_type=jnp.float32)


def lookup(which_ref, indices):
    high, low = which_ref.shape
    pick = (iota((high, indices.shape[1]), 0) == (indices >> 7)).astype(jnp.bfloat16)
    found = jnp.zeros((low, indices.shape[1]), jnp.float32)
    table = jnp.concatenate([which_ref[...].astype(jnp.float32), jnp.zeros((low - high, low), jnp.float32)], axis=0)
    table = jnp.transpose(table)[:, :high].astype(jnp.int32)
    for part, scale in ((table >> 7, 128.0), (table & 127, 1.0)):
        found += dot(part.astype(jnp.float32).astype(jnp.bfloat16), pick, (1, 0)) * scale
    here = iota(found.shape, 0) == (indices & 127)
    return jnp.sum(jnp.where(here, found, 0.0), axis=0, keepdims=True).astype(jnp.int32)


def pack_kernel(one_ids, two_ids, slot_hbm, one_hbm, two_hbm, out_hbm, one_ref, two_ref, ids_ref, ids2_ref, slot_ref, place_v, place2_v, place_s, place2_s, names_v, out_ref, sems, *, blocks, cap):
    total, stride = out_ref.shape[:2]
    rows = one_ref.shape[0]
    chunks = rows // LANES
    pairs = ((one_ids, ids_ref), (two_ids, ids2_ref), (slot_hbm, slot_ref), (one_hbm, one_ref), (two_hbm, two_ref))
    copies = [pltpu.make_async_copy(src, dst, sems.at[n]) for n, (src, dst) in enumerate(pairs)]
    for copy in copies:
        copy.start()
    for copy in copies[:3]:
        copy.wait()
    ids = ids_ref[...]
    ids2 = ids2_ref[...]
    held = ids >> 7
    leaving = lookup(slot_ref, held) != held
    block_slots = (held, lookup(slot_ref, ids2 >> 7))
    inner = (ids & 127, ids2 & 127)
    upper = jnp.where(iota((LANES, 2 * LANES), 0) < iota((LANES, 2 * LANES), 1), 1.0, 0.0).astype(jnp.bfloat16)
    everywhere = jnp.ones((LANES, LANES), jnp.bfloat16)
    lane_slot = iota((LANES, LANES), 0) & (2 * cap - 1)
    high = jnp.zeros((total, LANES), jnp.float32)
    low = jnp.zeros((total, LANES), jnp.float32)
    places = ((place_v, place_s), (place2_v, place2_s))
    to_scalar = [pltpu.make_async_copy(v, s, sems.at[5 + n]) for n, (v, s) in enumerate(places)]
    for step in range(2):
        slot = block_slots[step]
        owner = (slot * 43691) >> 22
        named = (slot - owner * blocks) * LANES + inner[step] + 1
        carry = jnp.zeros((total, LANES), jnp.float32)
        carry_first = jnp.zeros((total, LANES), jnp.float32)
        spots = [slice(c * LANES, (c + 1) * LANES) for c in range(chunks)]
        if step == 0:
            firsts = jnp.zeros((total, LANES), jnp.float32)
            for at in spots:
                mine = (iota((total, LANES), 0) == owner[:, at]) & leaving[:, at]
                firsts += dot(jnp.where(mine, 1.0, 0.0).astype(jnp.bfloat16), everywhere, (1, 0))
        for c, at in enumerate(spots):
            own = owner[:, at]
            name = named[:, at]
            mine = iota((total, LANES), 0) == own
            counted = dot(jnp.where(mine, 1.0, 0.0).astype(jnp.bfloat16), upper, (1, 0))
            before = counted[:, :LANES] + carry
            carry = carry + counted[:, LANES:]
            if step == 0:
                early = leaving[:, at]
                counted = dot(jnp.where(mine & early, 1.0, 0.0).astype(jnp.bfloat16), upper, (1, 0))
                before_first = counted[:, :LANES] + carry_first
                carry_first = carry_first + counted[:, LANES:]
                before = jnp.where(early, before_first, firsts + before - before_first)
            within = jnp.sum(jnp.where(mine, before, 0.0), axis=0, keepdims=True).astype(jnp.int32) + step * cap
            places[step][0][pl.ds(c, 1), :] = own * stride + within
            where = jnp.where(lane_slot == within, 1.0, 0.0).astype(jnp.bfloat16)
            high += dot(jnp.where(mine, (name >> 7).astype(jnp.float32), 0.0).astype(jnp.bfloat16), where, (1, 1))
            low += dot(jnp.where(mine, (name & 127).astype(jnp.float32), 0.0).astype(jnp.bfloat16), where, (1, 1))
        to_scalar[step].start()
    names_v[...] = high * 128.0 + low
    flat = out_ref.reshape(total * stride, 1, LANES)

    def move(src, place):
        def chunk(c, _):
            for g in range(LANES // 8):
                tile = src[pl.ds(c * LANES + g * 8, 8), :]
                for j in range(8):
                    flat[place[c, g * 8 + j]] = tile[j : j + 1, :]
            return 0

        lax.fori_loop(0, chunks, chunk, 0)

    to_scalar[0].wait()
    copies[3].wait()
    move(one_ref, place_s)
    first = pltpu.make_async_copy(out_ref.at[:, pl.ds(0, cap)], out_hbm.at[:, pl.ds(0, cap)], sems.at[7])
    first.start()

    def names(d, _):
        base = d * 8
        tile = names_v[pl.ds(base, 8), :]
        for j in range(8):
            out_ref[base + j, stride - 1] = tile[j : j + 1, :]
        return 0

    lax.fori_loop(0, total // 8, names, 0, unroll=2)
    to_scalar[1].wait()
    copies[4].wait()
    move(two_ref, place2_s)
    second = pltpu.make_async_copy(out_ref.at[:, pl.ds(cap, cap + 1)], out_hbm.at[:, pl.ds(cap, cap + 1)], sems.at[8])
    second.start()
    first.wait()
    second.wait()


def pack(one_ids, two_ids, slots, one, two, total, blocks, cap):
    rows, feature = one.shape
    hbm = pl.BlockSpec(memory_space=pltpu.HBM)
    message = (total, 2 * cap + 1, 1, feature)
    place = (rows // LANES, LANES)
    return pl.pallas_call(
        lambda *refs: pack_kernel(*refs, blocks=blocks, cap=cap),
        out_shape=jax.ShapeDtypeStruct(message, jnp.float32),
        in_specs=[hbm] * 5,
        out_specs=hbm,
        scratch_shapes=[
            VM((rows, feature), jnp.float32),
            VM((rows, feature), jnp.float32),
            VM((1, rows), jnp.int32),
            VM((1, rows), jnp.int32),
            VM(slots.shape, jnp.int32),
            VM(place, jnp.int32),
            VM(place, jnp.int32),
            SM(place, jnp.int32),
            SM(place, jnp.int32),
            VM((total, LANES), jnp.float32),
            VM(message, jnp.float32),
            pltpu.SemaphoreType.DMA((9,)),
        ],
        compiler_params=pltpu.CompilerParams(vmem_limit_bytes=ALL_VMEM),
        name="pack",
    )(one_ids, two_ids, slots, one, two)


def read_names(got_ref, names_v, copy, *, dump):
    total, stride = got_ref.shape[:2]
    width = stride - 1
    per = LANES // width
    group = iota((1, LANES), 1) // width
    for a in range(total // per):
        row = got_ref[a * per, width]
        for k in range(1, per):
            row = jnp.where(group == k, got_ref[a * per + k, width], row)
        names_v[pl.ds(a, 1), :] = row.astype(jnp.int32)
    named = names_v[...]
    named = jnp.where(named > 0, named - 1, dump)
    names_v[...] = named
    copy.start()
    return named


def add_rows(names_s, got_ref, sums_refs, *, offset, count):
    total, stride = got_ref.shape[:2]
    width = stride - 1
    per = LANES // width

    def step(a, _):
        for k in range(per):
            sums_ref = sums_refs[k % len(sums_refs)]
            rows = [names_s[a, k * width + offset + j] for j in range(count)]
            new = [sums_ref[pl.ds(r, 1), :] + got_ref[a * per + k, offset + j] for j, r in enumerate(rows)]
            for r, value in zip(rows, new):
                sums_ref[pl.ds(r, 1), :] = value
        return 0

    lax.fori_loop(0, total // per, step, 0)


def square_sums(block):
    return jnp.sum(block * block, axis=1, keepdims=True)


def rate(accums):
    return LEARN / (jnp.sqrt(accums) + EPSILON)


def lane_of(columns, k):
    return columns[:, k : k + 1]


def fetch_kernel(list_ref, table_ref, acc_ref, out_ref, old_ref, sems):
    copies = [pltpu.make_async_copy(table_ref.at[list_ref[FROM + k]], out_ref.at[k], sems.at[k]) for k in range(MOVES)]
    for copy in copies:
        copy.start()
    old_ref[...] = jnp.zeros_like(old_ref)
    for k in range(MOVES):
        old_ref[pl.ds(k, 1), :] = acc_ref[pl.ds(list_ref[FROM + k], 1), :]
    for copy in copies:
        copy.wait()


def fetch(lists, table, acc):
    vm = pl.BlockSpec(memory_space=VM)
    hbm = pl.BlockSpec(memory_space=pltpu.HBM)
    return pl.pallas_call(
        fetch_kernel,
        out_shape=(
            jax.ShapeDtypeStruct((MOVES,) + table.shape[1:], jnp.float32),
            jax.ShapeDtypeStruct((LANES, LANES), jnp.float32),
        ),
        in_specs=[pl.BlockSpec(memory_space=SM), hbm, vm],
        out_specs=(vm, vm),
        scratch_shapes=[pltpu.SemaphoreType.DMA((MOVES,))],
        compiler_params=pltpu.CompilerParams(vmem_limit_bytes=ALL_VMEM - ROOM),
        name="fetch",
    )(lists, table, acc)


ROUND = 4


def leave_kernel(list_ref, table_ref, acc_ref, got_ref, names_out, out_hbm, out_ref, even_ref, odd_ref, old_ref, names_v, names_s, sems, *, cap, rows):
    block, feature = table_ref.shape[1:]
    spans = [pl.ds(pl.multiple_of(list_ref[FROM + k] * block, block), block) for k in range(MOVES)]
    to_scalar = pltpu.make_async_copy(names_v, names_s, sems.at[MOVES])
    named = read_names(got_ref, names_v, to_scalar, dump=rows)
    names_out[...] = named
    at = iota(named.shape, 1) & (2 * cap - 1)
    goes = jnp.zeros(named.shape, jnp.bool_)
    for k in range(MOVES):
        goes = goes | ((named >> 7) == list_ref[FROM + k])
    needed = jnp.max(jnp.where(goes & (at < cap), at + 1, 0))
    for k in range(MOVES):
        even_ref[spans[k], :] = jnp.zeros((block, feature), jnp.float32)
        odd_ref[spans[k], :] = jnp.zeros((block, feature), jnp.float32)
    to_scalar.wait()

    def some(r, _):
        add_rows(names_s, got_ref, (even_ref, odd_ref), offset=r * ROUND, count=ROUND)
        return 0

    lax.fori_loop(0, (needed + ROUND - 1) // ROUND, some, 0)
    lane = iota((block, LANES), 1)
    squares = jnp.zeros((block, LANES), jnp.float32)
    for k in range(MOVES):
        gradient = even_ref[spans[k], :] + odd_ref[spans[k], :]
        even_ref[spans[k], :] = gradient
        squares = jnp.where(lane == k, square_sums(gradient), squares)
    fresh = jnp.transpose(acc_ref[...]) + squares * (1.0 / feature)
    rates = rate(jnp.where(lane < MOVES, fresh, 1.0))
    old_ref[...] = jnp.transpose(fresh)
    sends = []
    for k in range(MOVES):
        out_ref[k, pl.ds(block, 1), :] = old_ref[pl.ds(k, 1), :]
        out_ref[k, pl.ds(0, block), :] = table_ref[k] - lane_of(rates, k) * even_ref[spans[k], :]
        sends.append(pltpu.make_async_copy(out_ref.at[k], out_hbm.at[list_ref[TO + k]], sems.at[k]))
        sends[-1].start()
    for send in sends:
        send.wait()


def leave(lists, table, acc, got, peers, cap, rows):
    block, feature = table.shape[1:]
    vm = pl.BlockSpec(memory_space=VM)
    sm = pl.BlockSpec(memory_space=SM)
    names = (got.shape[0] * 2 * cap // LANES, LANES)
    return pl.pallas_call(
        lambda *refs: leave_kernel(*refs, cap=cap, rows=rows),
        out_shape=(
            jax.ShapeDtypeStruct(names, jnp.int32),
            jax.ShapeDtypeStruct((peers, block + 8, feature), jnp.float32),
        ),
        in_specs=[sm, vm, vm, vm],
        out_specs=(vm, pl.BlockSpec(memory_space=pltpu.HBM)),
        scratch_shapes=[
            VM((MOVES, block + 8, feature), jnp.float32),
            VM((rows + 8, feature), jnp.float32),
            VM((rows + 8, feature), jnp.float32),
            VM((LANES, LANES), jnp.float32),
            VM(names, jnp.int32),
            SM(names, jnp.int32),
            pltpu.SemaphoreType.DMA((MOVES + 1,)),
        ],
        compiler_params=pltpu.CompilerParams(vmem_limit_bytes=ALL_VMEM - ROOM),
        name="leave",
    )(lists, table, acc, got)


PIECE = 8


def stay_kernel(list_ref, names_ref, table_hbm, acc_ref, got_ref, out_hbm, accout_ref, arrive_ref, squares_ref, table_ref, one_ref, two_ref, rates_ref, sems):
    blocks, block, feature = table_ref.shape
    pieces = blocks // PIECE
    cap = (got_ref.shape[1] - 1) // 2

    def take(i):
        at = pl.ds(i * PIECE, PIECE)
        return pltpu.make_async_copy(table_hbm.at[at], table_ref.at[at], sems.at[i])

    def give(i):
        at = pl.ds(i * PIECE, PIECE)
        return pltpu.make_async_copy(table_ref.at[at], out_hbm.at[at], sems.at[i])

    for i in range(pieces):
        take(i).start()

    def span(b):
        return pl.ds(pl.multiple_of(b * block, block), block)

    def clear(b, _):
        one_ref[span(b), :] = jnp.zeros((block, feature), jnp.float32)
        two_ref[span(b), :] = jnp.zeros((block, feature), jnp.float32)
        return 0

    lax.fori_loop(0, blocks, clear, 0)
    add_rows(names_ref, got_ref, (one_ref,), offset=0, count=cap)
    add_rows(names_ref, got_ref, (two_ref,), offset=cap, count=cap)
    lane = iota((block, LANES), 1)

    def squares(g, sums):
        sums = list(sums)
        for k in range(4):
            b = g * 4 + k
            for n, ref in enumerate((one_ref, two_ref)):
                sums[n] = jnp.where(lane == b, square_sums(ref[span(b), :]), sums[n])
        return tuple(sums)

    zero = jnp.zeros((block, LANES), jnp.float32)
    first, second = lax.fori_loop(0, blocks // 4, squares, (zero, zero))
    old = jnp.concatenate([acc_ref[...], jnp.ones((LANES - blocks, LANES), jnp.float32)], axis=0)
    fresh = jnp.transpose(old) + first * (1.0 / feature)
    rates_ref[0] = rate(fresh)
    fresh = fresh + second * (1.0 / feature)
    rates_ref[1] = rate(fresh)
    accout_ref[...] = jnp.transpose(fresh)[:blocks, :]
    arriving = zero
    for k in range(MOVES):
        gradient = two_ref[span(list_ref[SLOT + k]), :]
        arrive_ref[k] = gradient
        arriving = jnp.where(lane == k, square_sums(gradient), arriving)
    squares_ref[...] = arriving

    def piece(i, _):
        turn = (LANES - PIECE * i) % LANES
        one_rate = pltpu.roll(rates_ref[0], turn, 1)
        two_rate = pltpu.roll(rates_ref[1], turn, 1)
        take(i).wait()
        for k in range(PIECE):
            b = i * PIECE + k
            weights = table_ref[b] - lane_of(one_rate, k) * one_ref[span(b), :]
            table_ref[b] = weights - lane_of(two_rate, k) * two_ref[span(b), :]
        give(i).start()
        return 0

    lax.fori_loop(0, pieces, piece, 0)
    for i in range(pieces):
        give(i).wait()


def stay(lists, names, table, acc, got):
    blocks, block, feature = table.shape
    vm = pl.BlockSpec(memory_space=VM)
    sm = pl.BlockSpec(memory_space=SM)
    hbm = pl.BlockSpec(memory_space=pltpu.HBM)
    return pl.pallas_call(
        stay_kernel,
        out_shape=(
            jax.ShapeDtypeStruct(table.shape, jnp.float32),
            jax.ShapeDtypeStruct(acc.shape, jnp.float32),
            jax.ShapeDtypeStruct((MOVES, block, feature), jnp.float32),
            jax.ShapeDtypeStruct((LANES, LANES), jnp.float32),
        ),
        in_specs=[sm, sm, hbm, vm, vm],
        out_specs=(hbm, vm, vm, vm),
        scratch_shapes=[
            VM(table.shape, jnp.float32),
            VM((blocks * block + 8, feature), jnp.float32),
            VM((blocks * block + 8, feature), jnp.float32),
            VM((2, LANES, LANES), jnp.float32),
            pltpu.SemaphoreType.DMA((blocks // PIECE,)),
        ],
        compiler_params=pltpu.CompilerParams(vmem_limit_bytes=ALL_VMEM - ROOM),
        name="stay",
    )(lists, names, table, acc, got)


def arrive_kernel(list_ref, got_hbm, second_ref, squares_ref, stayed_ref, accstay_ref, out_ref, acc_hbm, got_ref, acc_ref, buf_ref, old_ref, sems):
    block, feature = stayed_ref.shape[1:]
    takes = [pltpu.make_async_copy(got_hbm.at[list_ref[PEER + k]], got_ref.at[k], sems.at[k]) for k in range(MOVES)]
    for take in takes:
        take.start()
    acc_ref[...] = accstay_ref[...]
    lane = iota((block, LANES), 1)
    for k in range(MOVES):
        takes[k].wait()
        old_ref[pl.ds(k, 1), :] = got_ref[k, pl.ds(block, 1), :]
    fresh = jnp.transpose(old_ref[...]) + squares_ref[...] * (1.0 / feature)
    rates = rate(jnp.where(lane < MOVES, fresh, 1.0))
    copies = []
    for k in range(MOVES):
        buf_ref[k] = got_ref[k, pl.ds(0, block), :] - lane_of(rates, k) * second_ref[k]
        copies.append(pltpu.make_async_copy(buf_ref.at[k], out_ref.at[list_ref[SLOT + k]], sems.at[k]))
        copies[-1].start()
    old_ref[...] = jnp.transpose(fresh)
    for k in range(MOVES):
        acc_ref[pl.ds(list_ref[SLOT + k], 1), :] = old_ref[pl.ds(k, 1), :]
    copies.append(pltpu.make_async_copy(acc_ref, acc_hbm, sems.at[MOVES]))
    copies[-1].start()
    for copy in copies:
        copy.wait()


def arrive(lists, got, second, squares, stayed, accstay):
    blocks, block, feature = stayed.shape
    vm = pl.BlockSpec(memory_space=VM)
    sm = pl.BlockSpec(memory_space=SM)
    hbm = pl.BlockSpec(memory_space=pltpu.HBM)
    return pl.pallas_call(
        arrive_kernel,
        out_shape=(
            jax.ShapeDtypeStruct(stayed.shape, jnp.float32),
            jax.ShapeDtypeStruct(accstay.shape, jnp.float32),
        ),
        in_specs=[sm, hbm, vm, vm, hbm, vm],
        out_specs=(hbm, hbm),
        scratch_shapes=[
            VM((MOVES,) + got.shape[1:], jnp.float32),
            VM(accstay.shape, jnp.float32),
            VM((MOVES, block, feature), jnp.float32),
            VM((LANES, LANES), jnp.float32),
            pltpu.SemaphoreType.DMA((MOVES + 1,)),
        ],
        input_output_aliases={4: 0},
        compiler_params=pltpu.CompilerParams(vmem_limit_bytes=ALL_VMEM - LAST_ROOM),
        name="arrive",
    )(lists, got, second, squares, stayed, accstay)


def listed(mask, values):
    position = jnp.cumsum(mask.astype(jnp.int32)) - 1
    hit = mask[None, :] & (position[None, :] == jnp.arange(MOVES, dtype=jnp.int32)[:, None])
    return [jnp.sum(jnp.where(hit, v[None, :], 0), axis=1) for v in values]


def on_device(table, accumulator, grads_one, ids_one, grads_two, ids_two, new_slot):
    blocks, block, feature = table.shape
    peers = lax.axis_size("row")
    total = lax.axis_size("table") * peers
    group = lax.axis_index("table")
    mine = lax.axis_index("row")
    device = group * peers + mine
    rows = grads_one.shape[0]
    cap = 2 * rows // total

    slot_table = new_slot.reshape(-1, LANES)
    outgoing = pack(ids_one.reshape(1, rows), ids_two.reshape(1, rows), slot_table, grads_one, grads_two, total, blocks, cap)
    got = lax.all_to_all(outgoing, ("table", "row"), split_axis=0, concat_axis=0, tiled=True)

    here = lax.dynamic_slice_in_dim(new_slot, group * peers * blocks, peers * blocks).reshape(peers, blocks)
    own = lax.dynamic_slice_in_dim(new_slot, device * blocks, blocks)
    going = listed(own // blocks != device, (jnp.arange(blocks, dtype=jnp.int32), own // blocks % peers))
    peer = jnp.arange(peers, dtype=jnp.int32)
    to_me = (here // blocks == device) & (peer != mine)[:, None]
    slots = jnp.sum(jnp.where(to_me, here - device * blocks + 1, 0), axis=1)
    coming = listed(slots > 0, (slots - 1, peer))
    lists = jnp.concatenate(going + coming)

    gone, old = fetch(lists, table, accumulator)
    names, moving = leave(lists, gone, old, got, peers, cap, blocks * block)
    moved = lax.all_to_all(moving, "row", split_axis=0, concat_axis=0, tiled=True)
    stayed, accstay, second, squares = stay(lists, names, table, accumulator, got)
    return arrive(lists, moved, second, squares, stayed, accstay)


def solution(mesh):
    in_specs = (
        P(("table", "row"), None, None),
        P(("table", "row"), None),
        P(("table", "row"), None),
        P(("table", "row")),
        P(("table", "row"), None),
        P(("table", "row")),
        P(),
    )
    out_specs = (P(("table", "row"), None, None), P(("table", "row"), None))
    return jax.shard_map(
        on_device, mesh=mesh, in_specs=in_specs, out_specs=out_specs, check_vma=False
    )
```

```python
import jax
import jax.numpy as jnp
from jax import lax
from jax.experimental import pallas as pl
from jax.experimental.pallas import tpu as pltpu
from jax.sharding import PartitionSpec as P

LEARN = 0.5
EPSILON = 1e-08
LANES = 128
MOVES = 12
FROM, TO, SLOT, PEER = 0, MOVES, 2 * MOVES, 3 * MOVES
VM = pltpu.VMEM
SM = pltpu.SMEM
ALL_VMEM = 67043328
ROOM = 14000000
LAST_ROOM = 14000000


def iota(shape, dim):
    return lax.broadcasted_iota(jnp.int32, shape, dim)


def dot(a, b, contract):
    return lax.dot_general(a, b, ((contract[:1], contract[1:]), ((), ())), preferred_element_type=jnp.float32)


def lookup(which_ref, indices):
    high, low = which_ref.shape
    pick = (iota((high, indices.shape[1]), 0) == (indices >> 7)).astype(jnp.bfloat16)
    found = jnp.zeros((low, indices.shape[1]), jnp.float32)
    table = jnp.concatenate([which_ref[...].astype(jnp.float32), jnp.zeros((low - high, low), jnp.float32)], axis=0)
    table = jnp.transpose(table)[:, :high].astype(jnp.int32)
    for part, scale in ((table >> 7, 128.0), (table & 127, 1.0)):
        found += dot(part.astype(jnp.float32).astype(jnp.bfloat16), pick, (1, 0)) * scale
    here = iota(found.shape, 0) == (indices & 127)
    return jnp.sum(jnp.where(here, found, 0.0), axis=0, keepdims=True).astype(jnp.int32)


def leaves(which_ref, indices):
    high, low = which_ref.shape
    pick = (iota((high, indices.shape[1]), 0) == (indices >> 7)).astype(jnp.bfloat16)
    moves = jnp.where(which_ref[...] != iota((high, low), 0) * low + iota((high, low), 1), 1.0, 0.0)
    moves = jnp.concatenate([moves, jnp.zeros((low - high, low), jnp.float32)], axis=0)
    found = dot(jnp.transpose(moves)[:, :high].astype(jnp.bfloat16), pick, (1, 0))
    here = iota(found.shape, 0) == (indices & 127)
    return jnp.sum(jnp.where(here, found, 0.0), axis=0, keepdims=True) > 0.5


def pack_kernel(one_ids, two_ids, slot_hbm, one_hbm, two_hbm, out_hbm, one_ref, two_ref, ids_ref, ids2_ref, slot_ref, place_v, place2_v, place_s, place2_s, names_v, out_ref, sems, *, blocks, cap):
    total, stride = out_ref.shape[:2]
    rows = one_ref.shape[0]
    chunks = rows // LANES
    pairs = ((one_ids, ids_ref), (two_ids, ids2_ref), (slot_hbm, slot_ref), (one_hbm, one_ref), (two_hbm, two_ref))
    copies = [pltpu.make_async_copy(src, dst, sems.at[n]) for n, (src, dst) in enumerate(pairs)]
    for copy in copies:
        copy.start()
    for copy in copies[:3]:
        copy.wait()
    ids = ids_ref[...]
    ids2 = ids2_ref[...]
    held = ids >> 7
    leaving = leaves(slot_ref, held)
    block_slots = (held, lookup(slot_ref, ids2 >> 7))
    inner = (ids & 127, ids2 & 127)
    upper = jnp.where(iota((LANES, 2 * LANES), 0) < iota((LANES, 2 * LANES), 1), 1.0, 0.0).astype(jnp.bfloat16)
    everywhere = jnp.ones((LANES, LANES), jnp.bfloat16)
    lane_slot = iota((LANES, LANES), 0) & (2 * cap - 1)
    high = jnp.zeros((total, LANES), jnp.float32)
    low = jnp.zeros((total, LANES), jnp.float32)
    places = ((place_v, place_s), (place2_v, place2_s))
    to_scalar = [pltpu.make_async_copy(v, s, sems.at[5 + n]) for n, (v, s) in enumerate(places)]
    for step in range(2):
        slot = block_slots[step]
        owner = (slot * 43691) >> 22
        named = (slot - owner * blocks) * LANES + inner[step] + 1
        carry = jnp.zeros((total, LANES), jnp.float32)
        carry_first = jnp.zeros((total, LANES), jnp.float32)
        spots = [slice(c * LANES, (c + 1) * LANES) for c in range(chunks)]
        if step == 0:
            firsts = jnp.zeros((total, LANES), jnp.float32)
            for at in spots:
                mine = (iota((total, LANES), 0) == owner[:, at]) & leaving[:, at]
                firsts += dot(jnp.where(mine, 1.0, 0.0).astype(jnp.bfloat16), everywhere, (1, 0))
        for c, at in enumerate(spots):
            own = owner[:, at]
            name = named[:, at]
            mine = iota((total, LANES), 0) == own
            counted = dot(jnp.where(mine, 1.0, 0.0).astype(jnp.bfloat16), upper, (1, 0))
            before = counted[:, :LANES] + carry
            carry = carry + counted[:, LANES:]
            if step == 0:
                early = leaving[:, at]
                counted = dot(jnp.where(mine & early, 1.0, 0.0).astype(jnp.bfloat16), upper, (1, 0))
                before_first = counted[:, :LANES] + carry_first
                carry_first = carry_first + counted[:, LANES:]
                before = jnp.where(early, before_first, firsts + before - before_first)
            within = jnp.sum(jnp.where(mine, before, 0.0), axis=0, keepdims=True).astype(jnp.int32) + step * cap
            places[step][0][pl.ds(c, 1), :] = own * stride + within
            where = jnp.where(lane_slot == within, 1.0, 0.0).astype(jnp.bfloat16)
            high += dot(jnp.where(mine, (name >> 7).astype(jnp.float32), 0.0).astype(jnp.bfloat16), where, (1, 1))
            low += dot(jnp.where(mine, (name & 127).astype(jnp.float32), 0.0).astype(jnp.bfloat16), where, (1, 1))
        to_scalar[step].start()
    names_v[...] = high * 128.0 + low
    flat = out_ref.reshape(total * stride, 1, LANES)

    def move(src, place):
        def chunk(c, _):
            for g in range(LANES // 8):
                tile = src[pl.ds(c * LANES + g * 8, 8), :]
                for j in range(8):
                    flat[place[c, g * 8 + j]] = tile[j : j + 1, :]
            return 0

        lax.fori_loop(0, chunks, chunk, 0)

    to_scalar[0].wait()
    copies[3].wait()
    move(one_ref, place_s)
    first = pltpu.make_async_copy(out_ref.at[:, pl.ds(0, cap)], out_hbm.at[:, pl.ds(0, cap)], sems.at[7])
    first.start()

    def names(d, _):
        base = d * 8
        tile = names_v[pl.ds(base, 8), :]
        for j in range(8):
            out_ref[base + j, stride - 1] = tile[j : j + 1, :]
        return 0

    lax.fori_loop(0, total // 8, names, 0, unroll=2)
    to_scalar[1].wait()
    copies[4].wait()
    move(two_ref, place2_s)
    second = pltpu.make_async_copy(out_ref.at[:, pl.ds(cap, cap + 1)], out_hbm.at[:, pl.ds(cap, cap + 1)], sems.at[8])
    second.start()
    first.wait()
    second.wait()


def pack(one_ids, two_ids, slots, one, two, total, blocks, cap):
    rows, feature = one.shape
    hbm = pl.BlockSpec(memory_space=pltpu.HBM)
    message = (total, 2 * cap + 1, 1, feature)
    place = (rows // LANES, LANES)
    return pl.pallas_call(
        lambda *refs: pack_kernel(*refs, blocks=blocks, cap=cap),
        out_shape=jax.ShapeDtypeStruct(message, jnp.float32),
        in_specs=[hbm] * 5,
        out_specs=hbm,
        scratch_shapes=[
            VM((rows, feature), jnp.float32),
            VM((rows, feature), jnp.float32),
            VM((1, rows), jnp.int32),
            VM((1, rows), jnp.int32),
            VM(slots.shape, jnp.int32),
            VM(place, jnp.int32),
            VM(place, jnp.int32),
            SM(place, jnp.int32),
            SM(place, jnp.int32),
            VM((total, LANES), jnp.float32),
            VM(message, jnp.float32),
            pltpu.SemaphoreType.DMA((9,)),
        ],
        compiler_params=pltpu.CompilerParams(vmem_limit_bytes=ALL_VMEM),
        name="pack",
    )(one_ids, two_ids, slots, one, two)


def read_names(got_ref, names_v, copy, *, dump):
    total, stride = got_ref.shape[:2]
    width = stride - 1
    per = LANES // width
    group = iota((1, LANES), 1) // width
    for a in range(total // per):
        row = got_ref[a * per, width]
        for k in range(1, per):
            row = jnp.where(group == k, got_ref[a * per + k, width], row)
        names_v[pl.ds(a, 1), :] = row.astype(jnp.int32)
    named = names_v[...]
    named = jnp.where(named > 0, named - 1, dump)
    names_v[...] = named
    copy.start()
    return named


def add_rows(names_s, got_ref, sums_refs, *, offset, count):
    total, stride = got_ref.shape[:2]
    width = stride - 1
    per = LANES // width

    def step(a, _):
        for k in range(per):
            sums_ref = sums_refs[k % len(sums_refs)]
            rows = [names_s[a, k * width + offset + j] for j in range(count)]
            new = [sums_ref[pl.ds(r, 1), :] + got_ref[a * per + k, offset + j] for j, r in enumerate(rows)]
            for r, value in zip(rows, new):
                sums_ref[pl.ds(r, 1), :] = value
        return 0

    lax.fori_loop(0, total // per, step, 0)


def square_sums(block):
    return jnp.sum(block * block, axis=1, keepdims=True)


def rate(accums):
    return LEARN / (jnp.sqrt(accums) + EPSILON)


def lane_of(columns, k):
    return columns[:, k : k + 1]


def fetch_kernel(list_ref, table_ref, acc_ref, out_ref, old_ref, sems):
    copies = [pltpu.make_async_copy(table_ref.at[list_ref[FROM + k]], out_ref.at[k], sems.at[k]) for k in range(MOVES)]
    for copy in copies:
        copy.start()
    old_ref[...] = jnp.zeros_like(old_ref)
    for k in range(MOVES):
        old_ref[pl.ds(k, 1), :] = acc_ref[pl.ds(list_ref[FROM + k], 1), :]
    for copy in copies:
        copy.wait()


def fetch(lists, table, acc):
    vm = pl.BlockSpec(memory_space=VM)
    hbm = pl.BlockSpec(memory_space=pltpu.HBM)
    return pl.pallas_call(
        fetch_kernel,
        out_shape=(
            jax.ShapeDtypeStruct((MOVES,) + table.shape[1:], jnp.float32),
            jax.ShapeDtypeStruct((LANES, LANES), jnp.float32),
        ),
        in_specs=[pl.BlockSpec(memory_space=SM), hbm, vm],
        out_specs=(vm, vm),
        scratch_shapes=[pltpu.SemaphoreType.DMA((MOVES,))],
        compiler_params=pltpu.CompilerParams(vmem_limit_bytes=ALL_VMEM - ROOM),
        name="fetch",
    )(lists, table, acc)


ROUNDS = ((0, 6), (6, 5), (11, 5))


def message(ref, peer):
    peers, rows, _, feature = ref.shape
    return ref.reshape(peers * rows, feature).at[pl.ds(peer * rows, rows)]


def leave_kernel(list_ref, table_ref, acc_ref, got_ref, names_out, out_hbm, kept_hbm, out_ref, even_ref, odd_ref, old_ref, names_v, names_s, sems, *, cap, rows):
    block, feature = table_ref.shape[1:]
    spans = [pl.ds(pl.multiple_of(list_ref[FROM + k] * block, block), block) for k in range(MOVES)]
    to_scalar = pltpu.make_async_copy(names_v, names_s, sems.at[MOVES])
    keep = pltpu.make_async_copy(got_ref, kept_hbm, sems.at[MOVES + 1])
    keep.start()
    named = read_names(got_ref, names_v, to_scalar, dump=rows)
    names_out[...] = named
    at = iota(named.shape, 1) & (2 * cap - 1)
    goes = jnp.zeros(named.shape, jnp.bool_)
    for k in range(MOVES):
        goes = goes | ((named >> 7) == list_ref[FROM + k])
    needed = jnp.max(jnp.where(goes & (at < cap), at + 1, 0))
    for k in range(MOVES):
        even_ref[spans[k], :] = jnp.zeros((block, feature), jnp.float32)
        odd_ref[spans[k], :] = jnp.zeros((block, feature), jnp.float32)
    to_scalar.wait()

    for offset, count in ROUNDS:

        @pl.when(needed > offset)
        def _():
            add_rows(names_s, got_ref, (even_ref, odd_ref), offset=offset, count=count)

    lane = iota((block, LANES), 1)
    squares = jnp.zeros((block, LANES), jnp.float32)
    for k in range(MOVES):
        gradient = even_ref[spans[k], :] + odd_ref[spans[k], :]
        even_ref[spans[k], :] = gradient
        squares = jnp.where(lane == k, square_sums(gradient), squares)
    fresh = jnp.transpose(acc_ref[...]) + squares * (1.0 / feature)
    rates = rate(jnp.where(lane < MOVES, fresh, 1.0))
    old_ref[...] = jnp.transpose(fresh)
    sends = []
    for k in range(MOVES):
        out_ref[k, pl.ds(block, 1), :] = old_ref[pl.ds(k, 1), :]
        out_ref[k, pl.ds(0, block), :] = table_ref[k] - lane_of(rates, k) * even_ref[spans[k], :]
        sends.append(pltpu.make_async_copy(out_ref.at[k, pl.ds(0, block + 1)], message(out_hbm, list_ref[TO + k]), sems.at[k]))
        sends[-1].start()
    for send in sends:
        send.wait()
    keep.wait()


def leave(lists, table, acc, got, peers, cap, rows):
    block, feature = table.shape[1:]
    vm = pl.BlockSpec(memory_space=VM)
    sm = pl.BlockSpec(memory_space=SM)
    names = (got.shape[0] * 2 * cap // LANES, LANES)
    return pl.pallas_call(
        lambda *refs: leave_kernel(*refs, cap=cap, rows=rows),
        out_shape=(
            jax.ShapeDtypeStruct(names, jnp.int32),
            pltpu.HBM((peers, block + 1, 1, feature), jnp.float32),
            pltpu.HBM(got.shape, jnp.float32),
        ),
        in_specs=[sm, vm, vm, vm],
        out_specs=(vm, pl.BlockSpec(memory_space=pltpu.HBM), pl.BlockSpec(memory_space=pltpu.HBM)),
        scratch_shapes=[
            VM((MOVES, block + 8, feature), jnp.float32),
            VM((rows + 8, feature), jnp.float32),
            VM((rows + 8, feature), jnp.float32),
            VM((LANES, LANES), jnp.float32),
            VM(names, jnp.int32),
            SM(names, jnp.int32),
            pltpu.SemaphoreType.DMA((MOVES + 2,)),
        ],
        compiler_params=pltpu.CompilerParams(vmem_limit_bytes=ALL_VMEM - ROOM),
        name="leave",
    )(lists, table, acc, got)


PIECE = 8


def stay_kernel(list_ref, names_ref, table_hbm, acc_ref, got_ref, out_hbm, accout_ref, arrive_ref, squares_ref, table_ref, one_ref, two_ref, rates_ref, sems):
    blocks, block, feature = table_ref.shape
    pieces = blocks // PIECE
    cap = (got_ref.shape[1] - 1) // 2

    def take(i):
        at = pl.ds(i * PIECE, PIECE)
        return pltpu.make_async_copy(table_hbm.at[at], table_ref.at[at], sems.at[i])

    def give(i):
        at = pl.ds(i * PIECE, PIECE)
        return pltpu.make_async_copy(table_ref.at[at], out_hbm.at[at], sems.at[i])

    for i in range(pieces):
        take(i).start()

    def span(b):
        return pl.ds(pl.multiple_of(b * block, block), block)

    def clear(b, _):
        one_ref[span(b), :] = jnp.zeros((block, feature), jnp.float32)
        two_ref[span(b), :] = jnp.zeros((block, feature), jnp.float32)
        return 0

    lax.fori_loop(0, blocks, clear, 0)
    add_rows(names_ref, got_ref, (one_ref,), offset=0, count=cap)
    add_rows(names_ref, got_ref, (two_ref,), offset=cap, count=cap)
    lane = iota((block, LANES), 1)

    def squares(g, sums):
        sums = list(sums)
        for k in range(4):
            b = g * 4 + k
            for n, ref in enumerate((one_ref, two_ref)):
                sums[n] = jnp.where(lane == b, square_sums(ref[span(b), :]), sums[n])
        return tuple(sums)

    zero = jnp.zeros((block, LANES), jnp.float32)
    first, second = lax.fori_loop(0, blocks // 4, squares, (zero, zero))
    old = jnp.concatenate([acc_ref[...], jnp.ones((LANES - blocks, LANES), jnp.float32)], axis=0)
    fresh = jnp.transpose(old) + first * (1.0 / feature)
    rates_ref[0] = rate(fresh)
    fresh = fresh + second * (1.0 / feature)
    rates_ref[1] = rate(fresh)
    accout_ref[...] = jnp.transpose(fresh)[:blocks, :]
    arriving = zero
    for k in range(MOVES):
        gradient = two_ref[span(list_ref[SLOT + k]), :]
        arrive_ref[k] = gradient
        arriving = jnp.where(lane == k, square_sums(gradient), arriving)
    squares_ref[...] = arriving

    def piece(i, _):
        turn = (LANES - PIECE * i) % LANES
        one_rate = pltpu.roll(rates_ref[0], turn, 1)
        two_rate = pltpu.roll(rates_ref[1], turn, 1)
        take(i).wait()
        for k in range(PIECE):
            b = i * PIECE + k
            weights = table_ref[b] - lane_of(one_rate, k) * one_ref[span(b), :]
            table_ref[b] = weights - lane_of(two_rate, k) * two_ref[span(b), :]
        give(i).start()
        return 0

    lax.fori_loop(0, pieces, piece, 0)
    for i in range(pieces):
        give(i).wait()


def stay(lists, names, table, acc, got):
    blocks, block, feature = table.shape
    vm = pl.BlockSpec(memory_space=VM)
    sm = pl.BlockSpec(memory_space=SM)
    hbm = pl.BlockSpec(memory_space=pltpu.HBM)
    return pl.pallas_call(
        stay_kernel,
        out_shape=(
            jax.ShapeDtypeStruct(table.shape, jnp.float32),
            jax.ShapeDtypeStruct(acc.shape, jnp.float32),
            jax.ShapeDtypeStruct((MOVES, block, feature), jnp.float32),
            jax.ShapeDtypeStruct((LANES, LANES), jnp.float32),
        ),
        in_specs=[sm, sm, hbm, vm, vm],
        out_specs=(hbm, vm, vm, vm),
        scratch_shapes=[
            VM(table.shape, jnp.float32),
            VM((blocks * block + 8, feature), jnp.float32),
            VM((blocks * block + 8, feature), jnp.float32),
            VM((2, LANES, LANES), jnp.float32),
            pltpu.SemaphoreType.DMA((blocks // PIECE,)),
        ],
        compiler_params=pltpu.CompilerParams(vmem_limit_bytes=ALL_VMEM - ROOM),
        name="stay",
    )(lists, names, table, acc, got)


def arrive_kernel(list_ref, got_ref, second_ref, squares_ref, stayed_ref, accstay_ref, out_ref, acc_hbm, acc_ref, buf_ref, old_ref, sems):
    block, feature = stayed_ref.shape[1:]
    stride = got_ref.shape[1]
    rows_ref = got_ref.reshape(got_ref.shape[0] * stride, feature)
    acc_ref[...] = accstay_ref[...]
    lane = iota((block, LANES), 1)
    for k in range(MOVES):
        old_ref[pl.ds(k, 1), :] = got_ref[list_ref[PEER + k], block]
    fresh = jnp.transpose(old_ref[...]) + squares_ref[...] * (1.0 / feature)
    rates = rate(jnp.where(lane < MOVES, fresh, 1.0))
    copies = []
    for k in range(MOVES):
        buf_ref[k] = rows_ref[pl.ds(list_ref[PEER + k] * stride, block), :] - lane_of(rates, k) * second_ref[k]
        copies.append(pltpu.make_async_copy(buf_ref.at[k], out_ref.at[list_ref[SLOT + k]], sems.at[k]))
        copies[-1].start()
    old_ref[...] = jnp.transpose(fresh)
    for k in range(MOVES):
        acc_ref[pl.ds(list_ref[SLOT + k], 1), :] = old_ref[pl.ds(k, 1), :]
    copies.append(pltpu.make_async_copy(acc_ref, acc_hbm, sems.at[MOVES]))
    copies[-1].start()
    for copy in copies:
        copy.wait()


def arrive(lists, got, second, squares, stayed, accstay):
    blocks, block, feature = stayed.shape
    vm = pl.BlockSpec(memory_space=VM)
    sm = pl.BlockSpec(memory_space=SM)
    hbm = pl.BlockSpec(memory_space=pltpu.HBM)
    return pl.pallas_call(
        arrive_kernel,
        out_shape=(
            jax.ShapeDtypeStruct(stayed.shape, jnp.float32),
            jax.ShapeDtypeStruct(accstay.shape, jnp.float32),
        ),
        in_specs=[sm, vm, vm, vm, hbm, vm],
        out_specs=(hbm, hbm),
        scratch_shapes=[
            VM(accstay.shape, jnp.float32),
            VM((MOVES, block, feature), jnp.float32),
            VM((LANES, LANES), jnp.float32),
            pltpu.SemaphoreType.DMA((MOVES + 1,)),
        ],
        input_output_aliases={4: 0},
        compiler_params=pltpu.CompilerParams(vmem_limit_bytes=ALL_VMEM - LAST_ROOM),
        name="arrive",
    )(lists, got, second, squares, stayed, accstay)


def listed(mask, values):
    position = jnp.cumsum(mask.astype(jnp.int32)) - 1
    hit = mask[None, :] & (position[None, :] == jnp.arange(MOVES, dtype=jnp.int32)[:, None])
    return [jnp.sum(jnp.where(hit, v[None, :], 0), axis=1) for v in values]


def on_device(table, accumulator, grads_one, ids_one, grads_two, ids_two, new_slot):
    blocks, block, feature = table.shape
    peers = lax.axis_size("row")
    total = lax.axis_size("table") * peers
    group = lax.axis_index("table")
    mine = lax.axis_index("row")
    device = group * peers + mine
    rows = grads_one.shape[0]
    cap = 2 * rows // total

    slot_table = new_slot.reshape(-1, LANES)
    outgoing = pack(ids_one.reshape(1, rows), ids_two.reshape(1, rows), slot_table, grads_one, grads_two, total, blocks, cap)
    got = lax.all_to_all(outgoing, ("table", "row"), split_axis=0, concat_axis=0, tiled=True)

    here = lax.dynamic_slice_in_dim(new_slot, group * peers * blocks, peers * blocks).reshape(peers, blocks)
    own = lax.dynamic_slice_in_dim(new_slot, device * blocks, blocks)
    going = listed(own // blocks != device, (jnp.arange(blocks, dtype=jnp.int32), own // blocks % peers))
    peer = jnp.arange(peers, dtype=jnp.int32)
    to_me = (here // blocks == device) & (peer != mine)[:, None]
    slots = jnp.sum(jnp.where(to_me, here - device * blocks + 1, 0), axis=1)
    coming = listed(slots > 0, (slots - 1, peer))
    lists = jnp.concatenate(going + coming)

    gone, old = fetch(lists, table, accumulator)
    names, moving, kept = leave(lists, gone, old, got, peers, cap, blocks * block)
    moved = lax.all_to_all(moving, "row", split_axis=0, concat_axis=0, tiled=True)
    stayed, accstay, second, squares = stay(lists, names, table, accumulator, kept)
    return arrive(lists, moved, second, squares, stayed, accstay)


def solution(mesh):
    in_specs = (
        P(("table", "row"), None, None),
        P(("table", "row"), None),
        P(("table", "row"), None),
        P(("table", "row")),
        P(("table", "row"), None),
        P(("table", "row")),
        P(),
    )
    out_specs = (P(("table", "row"), None, None), P(("table", "row"), None))
    return jax.shard_map(
        on_device, mesh=mesh, in_specs=in_specs, out_specs=out_specs, check_vma=False
    )
```

```python
import jax
import jax.numpy as jnp
from jax import lax
from jax.experimental import pallas as pl
from jax.experimental.pallas import tpu as pltpu
from jax.sharding import PartitionSpec as P

LEARN = 0.5
EPSILON = 1e-08
LANES = 128
MOVES = 12
FROM, TO, SLOT, PEER = 0, MOVES, 2 * MOVES, 3 * MOVES
VM = pltpu.VMEM
SM = pltpu.SMEM
ALL_VMEM = 67043328
ROOM = 14000000
LAST_ROOM = 14000000


def iota(shape, dim):
    return lax.broadcasted_iota(jnp.int32, shape, dim)


def dot(a, b, contract):
    return lax.dot_general(a, b, ((contract[:1], contract[1:]), ((), ())), preferred_element_type=jnp.float32)


def lookup(which_ref, indices):
    high, low = which_ref.shape
    pick = (iota((high, indices.shape[1]), 0) == (indices >> 7)).astype(jnp.bfloat16)
    found = jnp.zeros((low, indices.shape[1]), jnp.float32)
    table = jnp.concatenate([which_ref[...].astype(jnp.float32), jnp.zeros((low - high, low), jnp.float32)], axis=0)
    table = jnp.transpose(table)[:, :high].astype(jnp.int32)
    for part, scale in ((table >> 7, 128.0), (table & 127, 1.0)):
        found += dot(part.astype(jnp.float32).astype(jnp.bfloat16), pick, (1, 0)) * scale
    here = iota(found.shape, 0) == (indices & 127)
    return jnp.sum(jnp.where(here, found, 0.0), axis=0, keepdims=True).astype(jnp.int32)


def leaves(which_ref, indices):
    high, low = which_ref.shape
    pick = (iota((high, indices.shape[1]), 0) == (indices >> 7)).astype(jnp.bfloat16)
    moves = jnp.where(which_ref[...] != iota((high, low), 0) * low + iota((high, low), 1), 1.0, 0.0)
    moves = jnp.concatenate([moves, jnp.zeros((low - high, low), jnp.float32)], axis=0)
    found = dot(jnp.transpose(moves)[:, :high].astype(jnp.bfloat16), pick, (1, 0))
    here = iota(found.shape, 0) == (indices & 127)
    return jnp.sum(jnp.where(here, found, 0.0), axis=0, keepdims=True) > 0.5


def pack_kernel(one_ids, two_ids, slot_hbm, one_hbm, two_hbm, out_hbm, one_ref, two_ref, ids_ref, ids2_ref, slot_ref, place_v, place2_v, place_s, place2_s, names_v, halves_ref, spots_ref, out_ref, sems, *, blocks, cap):
    total, stride = out_ref.shape[:2]
    rows = one_ref.shape[0]
    chunks = rows // LANES
    pairs = ((one_ids, ids_ref), (two_ids, ids2_ref), (slot_hbm, slot_ref), (one_hbm, one_ref), (two_hbm, two_ref))
    copies = [pltpu.make_async_copy(src, dst, sems.at[n]) for n, (src, dst) in enumerate(pairs)]
    for copy in copies:
        copy.start()
    for copy in copies[:3]:
        copy.wait()
    ids = ids_ref[...]
    ids2 = ids2_ref[...]
    held = ids >> 7
    leaving = leaves(slot_ref, held)
    block_slots = (held, lookup(slot_ref, ids2 >> 7))
    inner = (ids & 127, ids2 & 127)
    upper = jnp.where(iota((LANES, 2 * LANES), 0) < iota((LANES, 2 * LANES), 1), 1.0, 0.0).astype(jnp.bfloat16)
    everywhere = jnp.ones((LANES, LANES), jnp.bfloat16)
    lane_slot = iota((LANES, LANES), 0) & (2 * cap - 1)
    places = ((place_v, place_s), (place2_v, place2_s))
    to_scalar = [pltpu.make_async_copy(v, s, sems.at[5 + n]) for n, (v, s) in enumerate(places)]
    for step in range(2):
        slot = block_slots[step]
        owner = (slot * 43691) >> 22
        named = (slot - owner * blocks) * LANES + inner[step] + 1
        carry = jnp.zeros((total, LANES), jnp.float32)
        carry_first = jnp.zeros((total, LANES), jnp.float32)
        spots = [slice(c * LANES, (c + 1) * LANES) for c in range(chunks)]
        if step == 0:
            firsts = jnp.zeros((total, LANES), jnp.float32)
            for at in spots:
                mine = (iota((total, LANES), 0) == owner[:, at]) & leaving[:, at]
                firsts += dot(jnp.where(mine, 1.0, 0.0).astype(jnp.bfloat16), everywhere, (1, 0))
        for c, at in enumerate(spots):
            own = owner[:, at]
            name = named[:, at]
            mine = iota((total, LANES), 0) == own
            counted = dot(jnp.where(mine, 1.0, 0.0).astype(jnp.bfloat16), upper, (1, 0))
            before = counted[:, :LANES] + carry
            carry = carry + counted[:, LANES:]
            if step == 0:
                early = leaving[:, at]
                counted = dot(jnp.where(mine & early, 1.0, 0.0).astype(jnp.bfloat16), upper, (1, 0))
                before_first = counted[:, :LANES] + carry_first
                carry_first = carry_first + counted[:, LANES:]
                before = jnp.where(early, before_first, firsts + before - before_first)
            within = jnp.sum(jnp.where(mine, before, 0.0), axis=0, keepdims=True).astype(jnp.int32) + step * cap
            places[step][0][pl.ds(c, 1), :] = own * stride + within
            here = slice(step * rows + c * LANES, step * rows + (c + 1) * LANES)
            spots_ref[:, here] = jnp.where(lane_slot == within, 1.0, 0.0).astype(jnp.bfloat16)
            halves_ref[:total, here] = jnp.where(mine, (name >> 7).astype(jnp.float32), 0.0).astype(jnp.bfloat16)
            halves_ref[total:, here] = jnp.where(mine, (name & 127).astype(jnp.float32), 0.0).astype(jnp.bfloat16)
        to_scalar[step].start()
    halves = dot(halves_ref[...], spots_ref[...], (1, 1))
    names_v[...] = halves[:total] * 128.0 + halves[total:]
    flat = out_ref.reshape(total * stride, 1, LANES)

    def move(src, place):
        def chunk(c, _):
            for g in range(LANES // 8):
                tile = src[pl.ds(c * LANES + g * 8, 8), :]
                for j in range(8):
                    flat[place[c, g * 8 + j]] = tile[j : j + 1, :]
            return 0

        lax.fori_loop(0, chunks, chunk, 0)

    to_scalar[0].wait()
    copies[3].wait()
    move(one_ref, place_s)
    first = pltpu.make_async_copy(out_ref.at[:, pl.ds(0, cap)], out_hbm.at[:, pl.ds(0, cap)], sems.at[7])
    first.start()

    def names(d, _):
        base = d * 8
        tile = names_v[pl.ds(base, 8), :]
        for j in range(8):
            out_ref[base + j, stride - 1] = tile[j : j + 1, :]
        return 0

    lax.fori_loop(0, total // 8, names, 0, unroll=2)
    to_scalar[1].wait()
    copies[4].wait()
    move(two_ref, place2_s)
    second = pltpu.make_async_copy(out_ref.at[:, pl.ds(cap, cap + 1)], out_hbm.at[:, pl.ds(cap, cap + 1)], sems.at[8])
    second.start()
    first.wait()
    second.wait()


def pack(one_ids, two_ids, slots, one, two, total, blocks, cap):
    rows, feature = one.shape
    hbm = pl.BlockSpec(memory_space=pltpu.HBM)
    message = (total, 2 * cap + 1, 1, feature)
    place = (rows // LANES, LANES)
    return pl.pallas_call(
        lambda *refs: pack_kernel(*refs, blocks=blocks, cap=cap),
        out_shape=jax.ShapeDtypeStruct(message, jnp.float32),
        in_specs=[hbm] * 5,
        out_specs=hbm,
        scratch_shapes=[
            VM((rows, feature), jnp.float32),
            VM((rows, feature), jnp.float32),
            VM((1, rows), jnp.int32),
            VM((1, rows), jnp.int32),
            VM(slots.shape, jnp.int32),
            VM(place, jnp.int32),
            VM(place, jnp.int32),
            SM(place, jnp.int32),
            SM(place, jnp.int32),
            VM((total, LANES), jnp.float32),
            VM((2 * total, 2 * rows), jnp.bfloat16),
            VM((LANES, 2 * rows), jnp.bfloat16),
            VM(message, jnp.float32),
            pltpu.SemaphoreType.DMA((9,)),
        ],
        compiler_params=pltpu.CompilerParams(vmem_limit_bytes=ALL_VMEM),
        name="pack",
    )(one_ids, two_ids, slots, one, two)


def read_names(got_ref, names_v, copy, *, dump):
    total, stride = got_ref.shape[:2]
    width = stride - 1
    per = LANES // width
    group = iota((1, LANES), 1) // width
    for a in range(total // per):
        row = got_ref[a * per, width]
        for k in range(1, per):
            row = jnp.where(group == k, got_ref[a * per + k, width], row)
        names_v[pl.ds(a, 1), :] = row.astype(jnp.int32)
    named = names_v[...]
    named = jnp.where(named > 0, named - 1, dump)
    names_v[...] = named
    copy.start()
    return named


def add_rows(names_s, got_ref, sums_refs, *, offset, count):
    total, stride = got_ref.shape[:2]
    width = stride - 1
    per = LANES // width

    def step(a, _):
        for k in range(per):
            sums_ref = sums_refs[k % len(sums_refs)]
            rows = [names_s[a, k * width + offset + j] for j in range(count)]
            new = [sums_ref[pl.ds(r, 1), :] + got_ref[a * per + k, offset + j] for j, r in enumerate(rows)]
            for r, value in zip(rows, new):
                sums_ref[pl.ds(r, 1), :] = value
        return 0

    lax.fori_loop(0, total // per, step, 0)


def square_sums(block):
    return jnp.sum(block * block, axis=1, keepdims=True)


def rate(accums):
    return LEARN / (jnp.sqrt(accums) + EPSILON)


def lane_of(columns, k):
    return columns[:, k : k + 1]


def fetch_kernel(list_ref, table_ref, acc_ref, out_ref, old_ref, sems):
    copies = [pltpu.make_async_copy(table_ref.at[list_ref[FROM + k]], out_ref.at[k], sems.at[k]) for k in range(MOVES)]
    for copy in copies:
        copy.start()
    old_ref[...] = jnp.zeros_like(old_ref)
    for k in range(MOVES):
        old_ref[pl.ds(k, 1), :] = acc_ref[pl.ds(list_ref[FROM + k], 1), :]
    for copy in copies:
        copy.wait()


def fetch(lists, table, acc):
    vm = pl.BlockSpec(memory_space=VM)
    hbm = pl.BlockSpec(memory_space=pltpu.HBM)
    return pl.pallas_call(
        fetch_kernel,
        out_shape=(
            jax.ShapeDtypeStruct((MOVES,) + table.shape[1:], jnp.float32),
            jax.ShapeDtypeStruct((LANES, LANES), jnp.float32),
        ),
        in_specs=[pl.BlockSpec(memory_space=SM), hbm, vm],
        out_specs=(vm, vm),
        scratch_shapes=[pltpu.SemaphoreType.DMA((MOVES,))],
        compiler_params=pltpu.CompilerParams(vmem_limit_bytes=ALL_VMEM - ROOM),
        name="fetch",
    )(lists, table, acc)


ROUNDS = ((0, 6), (6, 5), (11, 5))


def message(ref, peer):
    peers, rows, _, feature = ref.shape
    return ref.reshape(peers * rows, feature).at[pl.ds(peer * rows, rows)]


def leave_kernel(list_ref, table_ref, acc_ref, got_ref, names_out, out_hbm, kept_hbm, out_ref, even_ref, odd_ref, old_ref, names_v, names_s, sems, *, cap, rows):
    block, feature = table_ref.shape[1:]
    spans = [pl.ds(pl.multiple_of(list_ref[FROM + k] * block, block), block) for k in range(MOVES)]
    to_scalar = pltpu.make_async_copy(names_v, names_s, sems.at[MOVES])
    keep = pltpu.make_async_copy(got_ref, kept_hbm, sems.at[MOVES + 1])
    keep.start()
    named = read_names(got_ref, names_v, to_scalar, dump=rows)
    names_out[...] = named
    at = iota(named.shape, 1) & (2 * cap - 1)
    goes = jnp.zeros(named.shape, jnp.bool_)
    for k in range(MOVES):
        goes = goes | ((named >> 7) == list_ref[FROM + k])
    needed = jnp.max(jnp.where(goes & (at < cap), at + 1, 0))
    for k in range(MOVES):
        even_ref[spans[k], :] = jnp.zeros((block, feature), jnp.float32)
        odd_ref[spans[k], :] = jnp.zeros((block, feature), jnp.float32)
    to_scalar.wait()

    for offset, count in ROUNDS:

        @pl.when(needed > offset)
        def _():
            add_rows(names_s, got_ref, (even_ref, odd_ref), offset=offset, count=count)

    lane = iota((block, LANES), 1)
    squares = jnp.zeros((block, LANES), jnp.float32)
    for k in range(MOVES):
        gradient = even_ref[spans[k], :] + odd_ref[spans[k], :]
        even_ref[spans[k], :] = gradient
        squares = jnp.where(lane == k, square_sums(gradient), squares)
    fresh = jnp.transpose(acc_ref[...]) + squares * (1.0 / feature)
    rates = rate(jnp.where(lane < MOVES, fresh, 1.0))
    old_ref[...] = jnp.transpose(fresh)
    sends = []
    for k in range(MOVES):
        out_ref[k, pl.ds(block, 1), :] = old_ref[pl.ds(k, 1), :]
        out_ref[k, pl.ds(0, block), :] = table_ref[k] - lane_of(rates, k) * even_ref[spans[k], :]
        sends.append(pltpu.make_async_copy(out_ref.at[k, pl.ds(0, block + 1)], message(out_hbm, list_ref[TO + k]), sems.at[k]))
        sends[-1].start()
    for send in sends:
        send.wait()
    keep.wait()


def leave(lists, table, acc, got, peers, cap, rows):
    block, feature = table.shape[1:]
    vm = pl.BlockSpec(memory_space=VM)
    sm = pl.BlockSpec(memory_space=SM)
    names = (got.shape[0] * 2 * cap // LANES, LANES)
    return pl.pallas_call(
        lambda *refs: leave_kernel(*refs, cap=cap, rows=rows),
        out_shape=(
            jax.ShapeDtypeStruct(names, jnp.int32),
            pltpu.HBM((peers, block + 1, 1, feature), jnp.float32),
            pltpu.HBM(got.shape, jnp.float32),
        ),
        in_specs=[sm, vm, vm, vm],
        out_specs=(vm, pl.BlockSpec(memory_space=pltpu.HBM), pl.BlockSpec(memory_space=pltpu.HBM)),
        scratch_shapes=[
            VM((MOVES, block + 8, feature), jnp.float32),
            VM((rows + 8, feature), jnp.float32),
            VM((rows + 8, feature), jnp.float32),
            VM((LANES, LANES), jnp.float32),
            VM(names, jnp.int32),
            SM(names, jnp.int32),
            pltpu.SemaphoreType.DMA((MOVES + 2,)),
        ],
        compiler_params=pltpu.CompilerParams(vmem_limit_bytes=ALL_VMEM - ROOM),
        name="leave",
    )(lists, table, acc, got)


PIECE = 8


def stay_kernel(list_ref, names_ref, table_hbm, acc_ref, got_ref, out_hbm, accout_ref, arrive_ref, squares_ref, table_ref, one_ref, two_ref, rates_ref, sems):
    blocks, block, feature = table_ref.shape
    pieces = blocks // PIECE
    cap = (got_ref.shape[1] - 1) // 2

    def take(i):
        at = pl.ds(i * PIECE, PIECE)
        return pltpu.make_async_copy(table_hbm.at[at], table_ref.at[at], sems.at[i])

    def give(i):
        at = pl.ds(i * PIECE, PIECE)
        return pltpu.make_async_copy(table_ref.at[at], out_hbm.at[at], sems.at[i])

    for i in range(pieces):
        take(i).start()

    def span(b):
        return pl.ds(pl.multiple_of(b * block, block), block)

    def clear(b, _):
        one_ref[span(b), :] = jnp.zeros((block, feature), jnp.float32)
        two_ref[span(b), :] = jnp.zeros((block, feature), jnp.float32)
        return 0

    lax.fori_loop(0, blocks, clear, 0)
    add_rows(names_ref, got_ref, (one_ref,), offset=0, count=cap)
    add_rows(names_ref, got_ref, (two_ref,), offset=cap, count=cap)
    lane = iota((block, LANES), 1)

    def squares(g, sums):
        sums = list(sums)
        for k in range(4):
            b = g * 4 + k
            for n, ref in enumerate((one_ref, two_ref)):
                sums[n] = jnp.where(lane == b, square_sums(ref[span(b), :]), sums[n])
        return tuple(sums)

    zero = jnp.zeros((block, LANES), jnp.float32)
    first, second = lax.fori_loop(0, blocks // 4, squares, (zero, zero))
    old = jnp.concatenate([acc_ref[...], jnp.ones((LANES - blocks, LANES), jnp.float32)], axis=0)
    fresh = jnp.transpose(old) + first * (1.0 / feature)
    rates_ref[0] = rate(fresh)
    fresh = fresh + second * (1.0 / feature)
    rates_ref[1] = rate(fresh)
    accout_ref[...] = jnp.transpose(fresh)[:blocks, :]
    arriving = zero
    for k in range(MOVES):
        gradient = two_ref[span(list_ref[SLOT + k]), :]
        arrive_ref[k] = gradient
        arriving = jnp.where(lane == k, square_sums(gradient), arriving)
    squares_ref[...] = arriving

    def piece(i, _):
        turn = (LANES - PIECE * i) % LANES
        one_rate = pltpu.roll(rates_ref[0], turn, 1)
        two_rate = pltpu.roll(rates_ref[1], turn, 1)
        take(i).wait()
        for k in range(PIECE):
            b = i * PIECE + k
            weights = table_ref[b] - lane_of(one_rate, k) * one_ref[span(b), :]
            table_ref[b] = weights - lane_of(two_rate, k) * two_ref[span(b), :]
        give(i).start()
        return 0

    lax.fori_loop(0, pieces, piece, 0)
    for i in range(pieces):
        give(i).wait()


def stay(lists, names, table, acc, got):
    blocks, block, feature = table.shape
    vm = pl.BlockSpec(memory_space=VM)
    sm = pl.BlockSpec(memory_space=SM)
    hbm = pl.BlockSpec(memory_space=pltpu.HBM)
    return pl.pallas_call(
        stay_kernel,
        out_shape=(
            jax.ShapeDtypeStruct(table.shape, jnp.float32),
            jax.ShapeDtypeStruct(acc.shape, jnp.float32),
            jax.ShapeDtypeStruct((MOVES, block, feature), jnp.float32),
            jax.ShapeDtypeStruct((LANES, LANES), jnp.float32),
        ),
        in_specs=[sm, sm, hbm, vm, vm],
        out_specs=(hbm, vm, vm, vm),
        scratch_shapes=[
            VM(table.shape, jnp.float32),
            VM((blocks * block + 8, feature), jnp.float32),
            VM((blocks * block + 8, feature), jnp.float32),
            VM((2, LANES, LANES), jnp.float32),
            pltpu.SemaphoreType.DMA((blocks // PIECE,)),
        ],
        compiler_params=pltpu.CompilerParams(vmem_limit_bytes=ALL_VMEM - ROOM),
        name="stay",
    )(lists, names, table, acc, got)


def arrive_kernel(list_ref, got_ref, second_ref, squares_ref, stayed_ref, accstay_ref, out_ref, acc_hbm, acc_ref, buf_ref, old_ref, sems):
    block, feature = stayed_ref.shape[1:]
    stride = got_ref.shape[1]
    rows_ref = got_ref.reshape(got_ref.shape[0] * stride, feature)
    acc_ref[...] = accstay_ref[...]
    lane = iota((block, LANES), 1)
    for k in range(MOVES):
        old_ref[pl.ds(k, 1), :] = got_ref[list_ref[PEER + k], block]
    fresh = jnp.transpose(old_ref[...]) + squares_ref[...] * (1.0 / feature)
    rates = rate(jnp.where(lane < MOVES, fresh, 1.0))
    copies = []
    for k in range(MOVES):
        buf_ref[k] = rows_ref[pl.ds(list_ref[PEER + k] * stride, block), :] - lane_of(rates, k) * second_ref[k]
        copies.append(pltpu.make_async_copy(buf_ref.at[k], out_ref.at[list_ref[SLOT + k]], sems.at[k]))
        copies[-1].start()
    old_ref[...] = jnp.transpose(fresh)
    for k in range(MOVES):
        acc_ref[pl.ds(list_ref[SLOT + k], 1), :] = old_ref[pl.ds(k, 1), :]
    copies.append(pltpu.make_async_copy(acc_ref, acc_hbm, sems.at[MOVES]))
    copies[-1].start()
    for copy in copies:
        copy.wait()


def arrive(lists, got, second, squares, stayed, accstay):
    blocks, block, feature = stayed.shape
    vm = pl.BlockSpec(memory_space=VM)
    sm = pl.BlockSpec(memory_space=SM)
    hbm = pl.BlockSpec(memory_space=pltpu.HBM)
    return pl.pallas_call(
        arrive_kernel,
        out_shape=(
            jax.ShapeDtypeStruct(stayed.shape, jnp.float32),
            jax.ShapeDtypeStruct(accstay.shape, jnp.float32),
        ),
        in_specs=[sm, vm, vm, vm, hbm, vm],
        out_specs=(hbm, hbm),
        scratch_shapes=[
            VM(accstay.shape, jnp.float32),
            VM((MOVES, block, feature), jnp.float32),
            VM((LANES, LANES), jnp.float32),
            pltpu.SemaphoreType.DMA((MOVES + 1,)),
        ],
        input_output_aliases={4: 0},
        compiler_params=pltpu.CompilerParams(vmem_limit_bytes=ALL_VMEM - LAST_ROOM),
        name="arrive",
    )(lists, got, second, squares, stayed, accstay)


def listed(mask, values):
    position = jnp.cumsum(mask.astype(jnp.int32)) - 1
    hit = mask[None, :] & (position[None, :] == jnp.arange(MOVES, dtype=jnp.int32)[:, None])
    return [jnp.sum(jnp.where(hit, v[None, :], 0), axis=1) for v in values]


def on_device(table, accumulator, grads_one, ids_one, grads_two, ids_two, new_slot):
    blocks, block, feature = table.shape
    peers = lax.axis_size("row")
    total = lax.axis_size("table") * peers
    group = lax.axis_index("table")
    mine = lax.axis_index("row")
    device = group * peers + mine
    rows = grads_one.shape[0]
    cap = 2 * rows // total

    slot_table = new_slot.reshape(-1, LANES)
    outgoing = pack(ids_one.reshape(1, rows), ids_two.reshape(1, rows), slot_table, grads_one, grads_two, total, blocks, cap)
    got = lax.all_to_all(outgoing, ("table", "row"), split_axis=0, concat_axis=0, tiled=True)

    here = lax.dynamic_slice_in_dim(new_slot, group * peers * blocks, peers * blocks).reshape(peers, blocks)
    own = lax.dynamic_slice_in_dim(new_slot, device * blocks, blocks)
    going = listed(own // blocks != device, (jnp.arange(blocks, dtype=jnp.int32), own // blocks % peers))
    peer = jnp.arange(peers, dtype=jnp.int32)
    to_me = (here // blocks == device) & (peer != mine)[:, None]
    slots = jnp.sum(jnp.where(to_me, here - device * blocks + 1, 0), axis=1)
    coming = listed(slots > 0, (slots - 1, peer))
    lists = jnp.concatenate(going + coming)

    gone, old = fetch(lists, table, accumulator)
    names, moving, kept = leave(lists, gone, old, got, peers, cap, blocks * block)
    moved = lax.all_to_all(moving, "row", split_axis=0, concat_axis=0, tiled=True)
    stayed, accstay, second, squares = stay(lists, names, table, accumulator, kept)
    return arrive(lists, moved, second, squares, stayed, accstay)


def solution(mesh):
    in_specs = (
        P(("table", "row"), None, None),
        P(("table", "row"), None),
        P(("table", "row"), None),
        P(("table", "row")),
        P(("table", "row"), None),
        P(("table", "row")),
        P(),
    )
    out_specs = (P(("table", "row"), None, None), P(("table", "row"), None))
    return jax.shard_map(
        on_device, mesh=mesh, in_specs=in_specs, out_specs=out_specs, check_vma=False
    )
```

```python
import jax
import jax.numpy as jnp
from jax import lax
from jax.experimental import pallas as pl
from jax.experimental.pallas import tpu as pltpu
from jax.sharding import PartitionSpec as P

LEARN = 0.5
EPSILON = 1e-08
LANES = 128
MOVES = 12
FROM, TO, SLOT, PEER = 0, MOVES, 2 * MOVES, 3 * MOVES
VM = pltpu.VMEM
SM = pltpu.SMEM
GRANT = 67043328
ROOM = 14000000
LAST_ROOM = 14000000


def iota(shape, dim):
    return lax.broadcasted_iota(jnp.int32, shape, dim)


def dot(a, b, contract):
    return lax.dot_general(a, b, ((contract[:1], contract[1:]), ((), ())), preferred_element_type=jnp.float32)


def lookup(which_ref, indices):
    high, low = which_ref.shape
    pick = (iota((high, indices.shape[1]), 0) == (indices >> 7)).astype(jnp.bfloat16)
    table = jnp.concatenate([which_ref[...].astype(jnp.float32), jnp.zeros((low - high, low), jnp.float32)], axis=0)
    table = jnp.transpose(table)[:, :high].astype(jnp.int32)
    halves = jnp.concatenate([(table >> 7).astype(jnp.float32), (table & 127).astype(jnp.float32)], axis=0)
    found = dot(halves.astype(jnp.bfloat16), pick, (1, 0))
    found = found[:low] * 128.0 + found[low:]
    here = iota(found.shape, 0) == (indices & 127)
    return jnp.sum(jnp.where(here, found, 0.0), axis=0, keepdims=True).astype(jnp.int32)


def leaves(which_ref, indices):
    high, low = which_ref.shape
    pick = (iota((high, indices.shape[1]), 0) == (indices >> 7)).astype(jnp.bfloat16)
    moves = jnp.where(which_ref[...] != iota((high, low), 0) * low + iota((high, low), 1), 1.0, 0.0)
    moves = jnp.concatenate([moves, jnp.zeros((low - high, low), jnp.float32)], axis=0)
    found = dot(jnp.transpose(moves)[:, :high].astype(jnp.bfloat16), pick, (1, 0))
    here = iota(found.shape, 0) == (indices & 127)
    return jnp.sum(jnp.where(here, found, 0.0), axis=0, keepdims=True) > 0.5


def pack_kernel(one_ids, two_ids, slot_hbm, one_hbm, two_hbm, out_hbm, one_ref, two_ref, ids_ref, ids2_ref, slot_ref, place_v, place2_v, place_s, place2_s, names_v, halves_ref, spots_ref, out_ref, sems, *, blocks, cap):
    total, stride = out_ref.shape[:2]
    rows = one_ref.shape[0]
    chunks = rows // LANES
    pairs = ((one_ids, ids_ref), (two_ids, ids2_ref), (slot_hbm, slot_ref), (one_hbm, one_ref), (two_hbm, two_ref))
    copies = [pltpu.make_async_copy(src, dst, sems.at[n]) for n, (src, dst) in enumerate(pairs)]
    for copy in copies:
        copy.start()
    for copy in copies[:3]:
        copy.wait()
    ids = ids_ref[...]
    ids2 = ids2_ref[...]
    held = ids >> 7
    leaving = leaves(slot_ref, held)
    block_slots = (held, lookup(slot_ref, ids2 >> 7))
    inner = (ids & 127, ids2 & 127)
    upper = jnp.where(iota((LANES, 2 * LANES), 0) < iota((LANES, 2 * LANES), 1), 1.0, 0.0).astype(jnp.bfloat16)
    everywhere = jnp.ones((LANES, LANES), jnp.bfloat16)
    lane_slot = iota((LANES, LANES), 0) & (2 * cap - 1)
    places = ((place_v, place_s), (place2_v, place2_s))
    to_scalar = [pltpu.make_async_copy(v, s, sems.at[5 + n]) for n, (v, s) in enumerate(places)]
    for step in range(2):
        slot = block_slots[step]
        owner = (slot * 43691) >> 22
        named = (slot - owner * blocks) * LANES + inner[step] + 1
        carry = jnp.zeros((total, LANES), jnp.float32)
        carry_first = jnp.zeros((total, LANES), jnp.float32)
        spots = [slice(c * LANES, (c + 1) * LANES) for c in range(chunks)]
        if step == 0:
            firsts = jnp.zeros((total, LANES), jnp.float32)
            for at in spots:
                mine = (iota((total, LANES), 0) == owner[:, at]) & leaving[:, at]
                firsts += dot(jnp.where(mine, 1.0, 0.0).astype(jnp.bfloat16), everywhere, (1, 0))
        for c, at in enumerate(spots):
            own = owner[:, at]
            name = named[:, at]
            mine = iota((total, LANES), 0) == own
            counted = dot(jnp.where(mine, 1.0, 0.0).astype(jnp.bfloat16), upper, (1, 0))
            before = counted[:, :LANES] + carry
            carry = carry + counted[:, LANES:]
            if step == 0:
                early = leaving[:, at]
                counted = dot(jnp.where(mine & early, 1.0, 0.0).astype(jnp.bfloat16), upper, (1, 0))
                before_first = counted[:, :LANES] + carry_first
                carry_first = carry_first + counted[:, LANES:]
                before = jnp.where(early, before_first, firsts + before - before_first)
            within = jnp.sum(jnp.where(mine, before, 0.0), axis=0, keepdims=True).astype(jnp.int32) + step * cap
            places[step][0][pl.ds(c, 1), :] = own * stride + within
            here = slice(step * rows + c * LANES, step * rows + (c + 1) * LANES)
            spots_ref[:, here] = jnp.where(lane_slot == within, 1.0, 0.0).astype(jnp.bfloat16)
            halves_ref[:total, here] = jnp.where(mine, (name >> 7).astype(jnp.float32), 0.0).astype(jnp.bfloat16)
            halves_ref[total:, here] = jnp.where(mine, (name & 127).astype(jnp.float32), 0.0).astype(jnp.bfloat16)
        to_scalar[step].start()
    halves = dot(halves_ref[...], spots_ref[...], (1, 1))
    names_v[...] = halves[:total] * 128.0 + halves[total:]
    flat = out_ref.reshape(total * stride, 1, LANES)

    def move(src, place):
        def chunk(c, _):
            for g in range(LANES // 8):
                tile = src[pl.ds(c * LANES + g * 8, 8), :]
                for j in range(8):
                    flat[place[c, g * 8 + j]] = tile[j : j + 1, :]
            return 0

        lax.fori_loop(0, chunks, chunk, 0)

    to_scalar[0].wait()
    copies[3].wait()
    move(one_ref, place_s)
    first = pltpu.make_async_copy(out_ref.at[:, pl.ds(0, cap)], out_hbm.at[:, pl.ds(0, cap)], sems.at[7])
    first.start()

    def names(d, _):
        base = d * 8
        tile = names_v[pl.ds(base, 8), :]
        for j in range(8):
            out_ref[base + j, stride - 1] = tile[j : j + 1, :]
        return 0

    lax.fori_loop(0, total // 8, names, 0, unroll=2)
    to_scalar[1].wait()
    copies[4].wait()
    move(two_ref, place2_s)
    second = pltpu.make_async_copy(out_ref.at[:, pl.ds(cap, cap + 1)], out_hbm.at[:, pl.ds(cap, cap + 1)], sems.at[8])
    second.start()
    first.wait()
    second.wait()


def pack(one_ids, two_ids, slots, one, two, total, blocks, cap):
    rows, feature = one.shape
    hbm = pl.BlockSpec(memory_space=pltpu.HBM)
    message = (total, 2 * cap + 1, 1, feature)
    place = (rows // LANES, LANES)
    return pl.pallas_call(
        lambda *refs: pack_kernel(*refs, blocks=blocks, cap=cap),
        out_shape=jax.ShapeDtypeStruct(message, jnp.float32),
        in_specs=[hbm] * 5,
        out_specs=hbm,
        scratch_shapes=[
            VM((rows, feature), jnp.float32),
            VM((rows, feature), jnp.float32),
            VM((1, rows), jnp.int32),
            VM((1, rows), jnp.int32),
            VM(slots.shape, jnp.int32),
            VM(place, jnp.int32),
            VM(place, jnp.int32),
            SM(place, jnp.int32),
            SM(place, jnp.int32),
            VM((total, LANES), jnp.float32),
            VM((2 * total, 2 * rows), jnp.bfloat16),
            VM((LANES, 2 * rows), jnp.bfloat16),
            VM(message, jnp.float32),
            pltpu.SemaphoreType.DMA((9,)),
        ],
        compiler_params=pltpu.CompilerParams(vmem_limit_bytes=GRANT),
        name="pack",
    )(one_ids, two_ids, slots, one, two)


def read_names(got_ref, names_v, copy, *, dump):
    total, stride = got_ref.shape[:2]
    width = stride - 1
    per = LANES // width
    group = iota((1, LANES), 1) // width
    for a in range(total // per):
        row = got_ref[a * per, width]
        for k in range(1, per):
            row = jnp.where(group == k, got_ref[a * per + k, width], row)
        names_v[pl.ds(a, 1), :] = row.astype(jnp.int32)
    named = names_v[...]
    named = jnp.where(named > 0, named - 1, dump)
    names_v[...] = named
    copy.start()
    return named


def add_rows(names_s, got_ref, sums_refs, *, offset, count):
    total, stride = got_ref.shape[:2]
    width = stride - 1
    per = LANES // width

    def step(a, _):
        for k in range(per):
            sums_ref = sums_refs[k % len(sums_refs)]
            rows = [names_s[a, k * width + offset + j] for j in range(count)]
            new = [sums_ref[pl.ds(r, 1), :] + got_ref[a * per + k, offset + j] for j, r in enumerate(rows)]
            for r, value in zip(rows, new):
                sums_ref[pl.ds(r, 1), :] = value
        return 0

    lax.fori_loop(0, total // per, step, 0)


def square_sums(block):
    return jnp.sum(block * block, axis=1, keepdims=True)


def rate(accums):
    return LEARN / (jnp.sqrt(accums) + EPSILON)


def lane_of(columns, k):
    return columns[:, k : k + 1]


def fetch_kernel(list_ref, table_ref, acc_ref, out_ref, columns_ref, old_ref, sems):
    copies = [pltpu.make_async_copy(table_ref.at[list_ref[0, FROM + k]], out_ref.at[k], sems.at[k]) for k in range(MOVES)]
    for copy in copies:
        copy.start()
    old_ref[...] = jnp.zeros_like(old_ref)
    for k in range(MOVES):
        old_ref[pl.ds(k, 1), :] = acc_ref[pl.ds(list_ref[0, FROM + k], 1), :]
    columns_ref[...] = jnp.transpose(old_ref[...])
    for copy in copies:
        copy.wait()


def fetch(lists, table, acc):
    vm = pl.BlockSpec(memory_space=VM)
    hbm = pl.BlockSpec(memory_space=pltpu.HBM)
    return pl.pallas_call(
        fetch_kernel,
        out_shape=(
            jax.ShapeDtypeStruct((MOVES,) + table.shape[1:], jnp.float32),
            jax.ShapeDtypeStruct((LANES, LANES), jnp.float32),
        ),
        in_specs=[pl.BlockSpec(memory_space=SM), hbm, vm],
        out_specs=(vm, vm),
        scratch_shapes=[VM((LANES, LANES), jnp.float32), pltpu.SemaphoreType.DMA((MOVES,))],
        compiler_params=pltpu.CompilerParams(vmem_limit_bytes=GRANT - ROOM),
        name="fetch",
    )(lists, table, acc)


ROUNDS = ((0, 6), (6, 5), (11, 5))


def message(ref, peer):
    peers, rows, _, feature = ref.shape
    return ref.reshape(peers * rows, feature).at[pl.ds(peer * rows, rows)]


def leave_kernel(list_hbm, table_ref, acc_ref, got_ref, names_out, out_hbm, kept_hbm, out_ref, even_ref, odd_ref, old_ref, names_v, names_s, list_ref, sems, *, cap, rows):
    block, feature = table_ref.shape[1:]
    scalars = pltpu.make_async_copy(list_hbm, list_ref, sems.at[MOVES + 2])
    scalars.start()
    to_scalar = pltpu.make_async_copy(names_v, names_s, sems.at[MOVES])
    keep = pltpu.make_async_copy(got_ref, kept_hbm, sems.at[MOVES + 1])
    keep.start()
    named = read_names(got_ref, names_v, to_scalar, dump=rows)
    names_out[...] = named
    scalars.wait()
    spans = [pl.ds(pl.multiple_of(list_ref[0, FROM + k] * block, block), block) for k in range(MOVES)]
    at = iota(named.shape, 1) & (2 * cap - 1)
    goes = jnp.zeros(named.shape, jnp.bool_)
    for k in range(MOVES):
        goes = goes | ((named >> 7) == list_ref[0, FROM + k])
    needed = jnp.max(jnp.where(goes & (at < cap), at + 1, 0))
    for k in range(MOVES):
        even_ref[spans[k], :] = jnp.zeros((block, feature), jnp.float32)
        odd_ref[spans[k], :] = jnp.zeros((block, feature), jnp.float32)
    to_scalar.wait()

    for offset, count in ROUNDS:

        @pl.when(needed > offset)
        def _():
            add_rows(names_s, got_ref, (even_ref, odd_ref), offset=offset, count=count)

    lane = iota((block, LANES), 1)
    squares = jnp.zeros((block, LANES), jnp.float32)
    for k in range(MOVES):
        gradient = even_ref[spans[k], :] + odd_ref[spans[k], :]
        even_ref[spans[k], :] = gradient
        squares = jnp.where(lane == k, square_sums(gradient), squares)
    fresh = acc_ref[...] + squares * (1.0 / feature)
    rates = rate(jnp.where(lane < MOVES, fresh, 1.0))
    old_ref[...] = jnp.transpose(fresh)
    sends = []
    for k in range(MOVES):
        out_ref[k, pl.ds(block, 1), :] = old_ref[pl.ds(k, 1), :]
        out_ref[k, pl.ds(0, block), :] = table_ref[k] - lane_of(rates, k) * even_ref[spans[k], :]
        sends.append(pltpu.make_async_copy(out_ref.at[k, pl.ds(0, block + 1)], message(out_hbm, list_ref[0, TO + k]), sems.at[k]))
        sends[-1].start()
    for send in sends:
        send.wait()
    keep.wait()


def leave(lists, table, acc, got, peers, cap, rows):
    block, feature = table.shape[1:]
    vm = pl.BlockSpec(memory_space=VM)
    names = (got.shape[0] * 2 * cap // LANES, LANES)
    return pl.pallas_call(
        lambda *refs: leave_kernel(*refs, cap=cap, rows=rows),
        out_shape=(
            jax.ShapeDtypeStruct(names, jnp.int32),
            pltpu.HBM((peers, block + 1, 1, feature), jnp.float32),
            pltpu.HBM(got.shape, jnp.float32),
        ),
        in_specs=[pl.BlockSpec(memory_space=pltpu.HBM), vm, vm, vm],
        out_specs=(vm, pl.BlockSpec(memory_space=pltpu.HBM), pl.BlockSpec(memory_space=pltpu.HBM)),
        scratch_shapes=[
            VM((MOVES, block + 8, feature), jnp.float32),
            VM((rows + 8, feature), jnp.float32),
            VM((rows + 8, feature), jnp.float32),
            VM((LANES, LANES), jnp.float32),
            VM(names, jnp.int32),
            SM(names, jnp.int32),
            SM(lists.shape, jnp.int32),
            pltpu.SemaphoreType.DMA((MOVES + 3,)),
        ],
        compiler_params=pltpu.CompilerParams(vmem_limit_bytes=GRANT - ROOM),
        name="leave",
    )(lists, table, acc, got)


PIECE = 8


def stay_kernel(list_ref, names_ref, table_hbm, acc_ref, got_ref, out_hbm, accout_ref, arrive_ref, squares_ref, table_ref, one_ref, two_ref, rates_ref, sems):
    blocks, block, feature = table_ref.shape
    pieces = blocks // PIECE
    cap = (got_ref.shape[1] - 1) // 2

    def take(i):
        at = pl.ds(i * PIECE, PIECE)
        return pltpu.make_async_copy(table_hbm.at[at], table_ref.at[at], sems.at[i])

    def give(i):
        at = pl.ds(i * PIECE, PIECE)
        return pltpu.make_async_copy(table_ref.at[at], out_hbm.at[at], sems.at[i])

    for i in range(pieces):
        take(i).start()

    def span(b):
        return pl.ds(pl.multiple_of(b * block, block), block)

    def clear(b, _):
        one_ref[span(b), :] = jnp.zeros((block, feature), jnp.float32)
        two_ref[span(b), :] = jnp.zeros((block, feature), jnp.float32)
        return 0

    lax.fori_loop(0, blocks, clear, 0)
    add_rows(names_ref, got_ref, (one_ref,), offset=0, count=cap)
    add_rows(names_ref, got_ref, (two_ref,), offset=cap, count=cap)
    lane = iota((block, LANES), 1)

    def squares(g, sums):
        sums = list(sums)
        for k in range(4):
            b = g * 4 + k
            for n, ref in enumerate((one_ref, two_ref)):
                sums[n] = jnp.where(lane == b, square_sums(ref[span(b), :]), sums[n])
        return tuple(sums)

    zero = jnp.zeros((block, LANES), jnp.float32)
    first, second = lax.fori_loop(0, blocks // 4, squares, (zero, zero))
    old = jnp.concatenate([acc_ref[...], jnp.ones((LANES - blocks, LANES), jnp.float32)], axis=0)
    fresh = jnp.transpose(old) + first * (1.0 / feature)
    rates_ref[0] = rate(fresh)
    fresh = fresh + second * (1.0 / feature)
    rates_ref[1] = rate(fresh)
    accout_ref[...] = jnp.transpose(fresh)[:blocks, :]
    arriving = zero
    for k in range(MOVES):
        gradient = two_ref[span(list_ref[0, SLOT + k]), :]
        arrive_ref[k] = gradient
        arriving = jnp.where(lane == k, square_sums(gradient), arriving)
    squares_ref[...] = arriving

    def piece(i, _):
        turn = (LANES - PIECE * i) % LANES
        one_rate = pltpu.roll(rates_ref[0], turn, 1)
        two_rate = pltpu.roll(rates_ref[1], turn, 1)
        take(i).wait()
        for k in range(PIECE):
            b = i * PIECE + k
            weights = table_ref[b] - lane_of(one_rate, k) * one_ref[span(b), :]
            table_ref[b] = weights - lane_of(two_rate, k) * two_ref[span(b), :]
        give(i).start()
        return 0

    lax.fori_loop(0, pieces, piece, 0)
    for i in range(pieces):
        give(i).wait()


def stay(lists, names, table, acc, got):
    blocks, block, feature = table.shape
    vm = pl.BlockSpec(memory_space=VM)
    sm = pl.BlockSpec(memory_space=SM)
    hbm = pl.BlockSpec(memory_space=pltpu.HBM)
    return pl.pallas_call(
        stay_kernel,
        out_shape=(
            jax.ShapeDtypeStruct(table.shape, jnp.float32),
            jax.ShapeDtypeStruct(acc.shape, jnp.float32),
            jax.ShapeDtypeStruct((MOVES, block, feature), jnp.float32),
            jax.ShapeDtypeStruct((LANES, LANES), jnp.float32),
        ),
        in_specs=[sm, sm, hbm, vm, vm],
        out_specs=(hbm, vm, vm, vm),
        scratch_shapes=[
            VM(table.shape, jnp.float32),
            VM((blocks * block + 8, feature), jnp.float32),
            VM((blocks * block + 8, feature), jnp.float32),
            VM((2, LANES, LANES), jnp.float32),
            pltpu.SemaphoreType.DMA((blocks // PIECE,)),
        ],
        compiler_params=pltpu.CompilerParams(vmem_limit_bytes=GRANT - ROOM),
        name="stay",
    )(lists, names, table, acc, got)


def arrive_kernel(list_ref, got_ref, second_ref, squares_ref, stayed_ref, accstay_ref, out_ref, acc_hbm, acc_ref, buf_ref, old_ref, sems):
    block, feature = stayed_ref.shape[1:]
    stride = got_ref.shape[1]
    rows_ref = got_ref.reshape(got_ref.shape[0] * stride, feature)
    acc_ref[...] = accstay_ref[...]
    lane = iota((block, LANES), 1)
    for k in range(MOVES):
        old_ref[pl.ds(k, 1), :] = got_ref[list_ref[0, PEER + k], block]
    fresh = jnp.transpose(old_ref[...]) + squares_ref[...] * (1.0 / feature)
    rates = rate(jnp.where(lane < MOVES, fresh, 1.0))
    copies = []
    for k in range(MOVES):
        buf_ref[k] = rows_ref[pl.ds(list_ref[0, PEER + k] * stride, block), :] - lane_of(rates, k) * second_ref[k]
        copies.append(pltpu.make_async_copy(buf_ref.at[k], out_ref.at[list_ref[0, SLOT + k]], sems.at[k]))
        copies[-1].start()
    old_ref[...] = jnp.transpose(fresh)
    for k in range(MOVES):
        acc_ref[pl.ds(list_ref[0, SLOT + k], 1), :] = old_ref[pl.ds(k, 1), :]
    copies.append(pltpu.make_async_copy(acc_ref, acc_hbm, sems.at[MOVES]))
    copies[-1].start()
    for copy in copies:
        copy.wait()


def arrive(lists, got, second, squares, stayed, accstay):
    blocks, block, feature = stayed.shape
    vm = pl.BlockSpec(memory_space=VM)
    sm = pl.BlockSpec(memory_space=SM)
    hbm = pl.BlockSpec(memory_space=pltpu.HBM)
    return pl.pallas_call(
        arrive_kernel,
        out_shape=(
            jax.ShapeDtypeStruct(stayed.shape, jnp.float32),
            jax.ShapeDtypeStruct(accstay.shape, jnp.float32),
        ),
        in_specs=[sm, vm, vm, vm, hbm, vm],
        out_specs=(hbm, hbm),
        scratch_shapes=[
            VM(accstay.shape, jnp.float32),
            VM((MOVES, block, feature), jnp.float32),
            VM((LANES, LANES), jnp.float32),
            pltpu.SemaphoreType.DMA((MOVES + 1,)),
        ],
        input_output_aliases={4: 0},
        compiler_params=pltpu.CompilerParams(vmem_limit_bytes=GRANT - LAST_ROOM),
        name="arrive",
    )(lists, got, second, squares, stayed, accstay)


def listed(mask, values):
    position = jnp.cumsum(mask.astype(jnp.int32)) - 1
    hit = mask[None, :] & (position[None, :] == jnp.arange(MOVES, dtype=jnp.int32)[:, None])
    return [jnp.sum(jnp.where(hit, v[None, :], 0), axis=1) for v in values]


def on_device(table, accumulator, grads_one, ids_one, grads_two, ids_two, new_slot):
    blocks, block, feature = table.shape
    peers = lax.axis_size("row")
    total = lax.axis_size("table") * peers
    group = lax.axis_index("table")
    mine = lax.axis_index("row")
    device = group * peers + mine
    rows = grads_one.shape[0]
    cap = 2 * rows // total

    slot_table = new_slot.reshape(-1, LANES)
    outgoing = pack(ids_one.reshape(1, rows), ids_two.reshape(1, rows), slot_table, grads_one, grads_two, total, blocks, cap)
    got = lax.all_to_all(outgoing, ("table", "row"), split_axis=0, concat_axis=0, tiled=True)

    here = lax.dynamic_slice_in_dim(new_slot, group * peers * blocks, peers * blocks).reshape(peers, blocks)
    own = lax.dynamic_slice_in_dim(new_slot, device * blocks, blocks)
    going = listed(own // blocks != device, (jnp.arange(blocks, dtype=jnp.int32), own // blocks % peers))
    peer = jnp.arange(peers, dtype=jnp.int32)
    to_me = (here // blocks == device) & (peer != mine)[:, None]
    slots = jnp.sum(jnp.where(to_me, here - device * blocks + 1, 0), axis=1)
    coming = listed(slots > 0, (slots - 1, peer))
    lists = jnp.concatenate(going + coming)
    lists = jnp.pad(lists, (0, LANES - lists.shape[0]))[None, :]

    gone, old = fetch(lists, table, accumulator)
    names, moving, kept = leave(lists, gone, old, got, peers, cap, blocks * block)
    moved = lax.all_to_all(moving, "row", split_axis=0, concat_axis=0, tiled=True)
    stayed, accstay, second, squares = stay(lists, names, table, accumulator, kept)
    return arrive(lists, moved, second, squares, stayed, accstay)


def solution(mesh):
    in_specs = (
        P(("table", "row"), None, None),
        P(("table", "row"), None),
        P(("table", "row"), None),
        P(("table", "row")),
        P(("table", "row"), None),
        P(("table", "row")),
        P(),
    )
    out_specs = (P(("table", "row"), None, None), P(("table", "row"), None))
    return jax.shard_map(
        on_device, mesh=mesh, in_specs=in_specs, out_specs=out_specs, check_vma=False
    )
```

```python
import jax
import jax.numpy as jnp
from jax import lax
from jax.experimental import pallas as pl
from jax.experimental.pallas import tpu as pltpu
from jax.sharding import PartitionSpec as P

LEARN = 0.5
EPSILON = 1e-08
LANES = 128
MOVES = 12
FROM, TO, SLOT, PEER = 0, MOVES, 2 * MOVES, 3 * MOVES
VM = pltpu.VMEM
SM = pltpu.SMEM
GRANT = 67043328
ROOM = 14000000
LAST_ROOM = 14000000


def iota(shape, dim):
    return lax.broadcasted_iota(jnp.int32, shape, dim)


def dot(a, b, contract):
    return lax.dot_general(a, b, ((contract[:1], contract[1:]), ((), ())), preferred_element_type=jnp.float32)


def lookup(which_ref, indices):
    high, low = which_ref.shape
    pick = (iota((high, indices.shape[1]), 0) == (indices >> 7)).astype(jnp.bfloat16)
    table = jnp.concatenate([which_ref[...].astype(jnp.float32), jnp.zeros((low - high, low), jnp.float32)], axis=0)
    table = jnp.transpose(table)[:, :high].astype(jnp.int32)
    halves = jnp.concatenate([(table >> 7).astype(jnp.float32), (table & 127).astype(jnp.float32)], axis=0)
    found = dot(halves.astype(jnp.bfloat16), pick, (1, 0))
    found = found[:low] * 128.0 + found[low:]
    here = iota(found.shape, 0) == (indices & 127)
    return jnp.sum(jnp.where(here, found, 0.0), axis=0, keepdims=True).astype(jnp.int32)


def leaves(which_ref, indices):
    high, low = which_ref.shape
    pick = (iota((high, indices.shape[1]), 0) == (indices >> 7)).astype(jnp.bfloat16)
    moves = jnp.where(which_ref[...] != iota((high, low), 0) * low + iota((high, low), 1), 1.0, 0.0)
    moves = jnp.concatenate([moves, jnp.zeros((low - high, low), jnp.float32)], axis=0)
    found = dot(jnp.transpose(moves)[:, :high].astype(jnp.bfloat16), pick, (1, 0))
    here = iota(found.shape, 0) == (indices & 127)
    return jnp.sum(jnp.where(here, found, 0.0), axis=0, keepdims=True) > 0.5


def pack_kernel(one_ids, two_ids, slot_hbm, one_hbm, two_hbm, out_hbm, one_ref, two_ref, ids_ref, ids2_ref, slot_ref, place_v, place2_v, place_s, place2_s, names_v, halves_ref, spots_ref, out_ref, sems, *, blocks, cap):
    total, stride = out_ref.shape[:2]
    rows = one_ref.shape[0]
    chunks = rows // LANES
    pairs = ((one_ids, ids_ref), (two_ids, ids2_ref), (slot_hbm, slot_ref), (one_hbm, one_ref), (two_hbm, two_ref))
    copies = [pltpu.make_async_copy(src, dst, sems.at[n]) for n, (src, dst) in enumerate(pairs)]
    for copy in copies:
        copy.start()
    for copy in copies[:3]:
        copy.wait()
    ids = ids_ref[...]
    ids2 = ids2_ref[...]
    held = ids >> 7
    leaving = leaves(slot_ref, held)
    block_slots = (held, lookup(slot_ref, ids2 >> 7))
    inner = (ids & 127, ids2 & 127)
    upper = jnp.where(iota((LANES, 2 * LANES), 0) < iota((LANES, 2 * LANES), 1), 1.0, 0.0).astype(jnp.bfloat16)
    everywhere = jnp.ones((LANES, LANES), jnp.bfloat16)
    lane_slot = iota((LANES, LANES), 0) & (2 * cap - 1)
    places = ((place_v, place_s), (place2_v, place2_s))
    to_scalar = [pltpu.make_async_copy(v, s, sems.at[5 + n]) for n, (v, s) in enumerate(places)]
    for step in range(2):
        slot = block_slots[step]
        owner = (slot * 43691) >> 22
        named = (slot - owner * blocks) * LANES + inner[step] + 1
        carry = jnp.zeros((total, LANES), jnp.float32)
        carry_first = jnp.zeros((total, LANES), jnp.float32)
        spots = [slice(c * LANES, (c + 1) * LANES) for c in range(chunks)]
        if step == 0:
            firsts = jnp.zeros((total, LANES), jnp.float32)
            for at in spots:
                mine = (iota((total, LANES), 0) == owner[:, at]) & leaving[:, at]
                firsts += dot(jnp.where(mine, 1.0, 0.0).astype(jnp.bfloat16), everywhere, (1, 0))
        for c, at in enumerate(spots):
            own = owner[:, at]
            name = named[:, at]
            mine = iota((total, LANES), 0) == own
            counted = dot(jnp.where(mine, 1.0, 0.0).astype(jnp.bfloat16), upper, (1, 0))
            before = counted[:, :LANES] + carry
            carry = carry + counted[:, LANES:]
            if step == 0:
                early = leaving[:, at]
                counted = dot(jnp.where(mine & early, 1.0, 0.0).astype(jnp.bfloat16), upper, (1, 0))
                before_first = counted[:, :LANES] + carry_first
                carry_first = carry_first + counted[:, LANES:]
                before = jnp.where(early, before_first, firsts + before - before_first)
            within = jnp.sum(jnp.where(mine, before, 0.0), axis=0, keepdims=True).astype(jnp.int32) + step * cap
            places[step][0][pl.ds(c, 1), :] = own * stride + within
            here = slice(step * rows + c * LANES, step * rows + (c + 1) * LANES)
            spots_ref[:, here] = jnp.where(lane_slot == within, 1.0, 0.0).astype(jnp.bfloat16)
            halves_ref[:total, here] = jnp.where(mine, (name >> 7).astype(jnp.float32), 0.0).astype(jnp.bfloat16)
            halves_ref[total:, here] = jnp.where(mine, (name & 127).astype(jnp.float32), 0.0).astype(jnp.bfloat16)
        to_scalar[step].start()
    halves = dot(halves_ref[...], spots_ref[...], (1, 1))
    names_v[...] = halves[:total] * 128.0 + halves[total:]
    flat = out_ref.reshape(total * stride, 1, LANES)

    def move(src, place):
        def chunk(c, _):
            for g in range(LANES // 8):
                tile = src[pl.ds(c * LANES + g * 8, 8), :]
                for j in range(8):
                    flat[place[c, g * 8 + j]] = tile[j : j + 1, :]
            return 0

        lax.fori_loop(0, chunks, chunk, 0)

    to_scalar[0].wait()
    copies[3].wait()
    move(one_ref, place_s)
    first = pltpu.make_async_copy(out_ref.at[:, pl.ds(0, cap)], out_hbm.at[:, pl.ds(0, cap)], sems.at[7])
    first.start()

    def names(d, _):
        base = d * 8
        tile = names_v[pl.ds(base, 8), :]
        for j in range(8):
            out_ref[base + j, stride - 1] = tile[j : j + 1, :]
        return 0

    lax.fori_loop(0, total // 8, names, 0, unroll=2)
    to_scalar[1].wait()
    copies[4].wait()
    move(two_ref, place2_s)
    second = pltpu.make_async_copy(out_ref.at[:, pl.ds(cap, cap + 1)], out_hbm.at[:, pl.ds(cap, cap + 1)], sems.at[8])
    second.start()
    first.wait()
    second.wait()


def pack(one_ids, two_ids, slots, one, two, total, blocks, cap):
    rows, feature = one.shape
    hbm = pl.BlockSpec(memory_space=pltpu.HBM)
    message = (total, 2 * cap + 1, 1, feature)
    place = (rows // LANES, LANES)
    return pl.pallas_call(
        lambda *refs: pack_kernel(*refs, blocks=blocks, cap=cap),
        out_shape=jax.ShapeDtypeStruct(message, jnp.float32),
        in_specs=[hbm] * 5,
        out_specs=hbm,
        scratch_shapes=[
            VM((rows, feature), jnp.float32),
            VM((rows, feature), jnp.float32),
            VM((1, rows), jnp.int32),
            VM((1, rows), jnp.int32),
            VM(slots.shape, jnp.int32),
            VM(place, jnp.int32),
            VM(place, jnp.int32),
            SM(place, jnp.int32),
            SM(place, jnp.int32),
            VM((total, LANES), jnp.float32),
            VM((2 * total, 2 * rows), jnp.bfloat16),
            VM((LANES, 2 * rows), jnp.bfloat16),
            VM(message, jnp.float32),
            pltpu.SemaphoreType.DMA((9,)),
        ],
        compiler_params=pltpu.CompilerParams(vmem_limit_bytes=GRANT),
        name="pack",
    )(one_ids, two_ids, slots, one, two)


def read_names(got_ref, names_v, copy, *, dump):
    total, stride = got_ref.shape[:2]
    width = stride - 1
    per = LANES // width
    group = iota((1, LANES), 1) // width
    for a in range(total // per):
        row = got_ref[a * per, width]
        for k in range(1, per):
            row = jnp.where(group == k, got_ref[a * per + k, width], row)
        names_v[pl.ds(a, 1), :] = row.astype(jnp.int32)
    named = names_v[...]
    named = jnp.where(named > 0, named - 1, dump)
    names_v[...] = named
    copy.start()
    return named


def add_rows(names_s, got_ref, sums_refs, *, offset, count):
    total, stride = got_ref.shape[:2]
    width = stride - 1
    per = LANES // width

    def step(a, _):
        for k in range(per):
            sums_ref = sums_refs[k % len(sums_refs)]
            rows = [names_s[a, k * width + offset + j] for j in range(count)]
            new = [sums_ref[pl.ds(r, 1), :] + got_ref[a * per + k, offset + j] for j, r in enumerate(rows)]
            for r, value in zip(rows, new):
                sums_ref[pl.ds(r, 1), :] = value
        return 0

    lax.fori_loop(0, total // per, step, 0)


def square_sums(block):
    return jnp.sum(block * block, axis=1, keepdims=True)


def rate(accums):
    return LEARN / (jnp.sqrt(accums) + EPSILON)


def lane_of(columns, k):
    return columns[:, k : k + 1]


def fetch_kernel(list_ref, table_ref, acc_ref, out_ref, columns_ref, old_ref, sems):
    copies = [pltpu.make_async_copy(table_ref.at[list_ref[0, FROM + k]], out_ref.at[k], sems.at[k]) for k in range(MOVES)]
    for copy in copies:
        copy.start()
    old_ref[...] = jnp.zeros_like(old_ref)
    for k in range(MOVES):
        old_ref[pl.ds(k, 1), :] = acc_ref[pl.ds(list_ref[0, FROM + k], 1), :]
    columns_ref[...] = jnp.transpose(old_ref[...])
    for copy in copies:
        copy.wait()


def fetch(lists, table, acc):
    vm = pl.BlockSpec(memory_space=VM)
    hbm = pl.BlockSpec(memory_space=pltpu.HBM)
    return pl.pallas_call(
        fetch_kernel,
        out_shape=(
            jax.ShapeDtypeStruct((MOVES,) + table.shape[1:], jnp.float32),
            jax.ShapeDtypeStruct((LANES, LANES), jnp.float32),
        ),
        in_specs=[pl.BlockSpec(memory_space=SM), hbm, vm],
        out_specs=(vm, vm),
        scratch_shapes=[VM((LANES, LANES), jnp.float32), pltpu.SemaphoreType.DMA((MOVES,))],
        compiler_params=pltpu.CompilerParams(vmem_limit_bytes=GRANT - ROOM),
        name="fetch",
    )(lists, table, acc)


ROUNDS = ((0, 6), (6, 5), (11, 5))


def message(ref, peer):
    peers, rows, _, feature = ref.shape
    return ref.reshape(peers * rows, feature).at[pl.ds(peer * rows, rows)]


def leave_kernel(list_hbm, table_ref, acc_ref, got_ref, names_out, out_hbm, kept_hbm, out_ref, even_ref, odd_ref, old_ref, names_v, names_s, list_ref, sems, *, cap, rows):
    block, feature = table_ref.shape[1:]
    scalars = pltpu.make_async_copy(list_hbm, list_ref, sems.at[MOVES + 2])
    scalars.start()
    to_scalar = pltpu.make_async_copy(names_v, names_s, sems.at[MOVES])
    keep = pltpu.make_async_copy(got_ref, kept_hbm, sems.at[MOVES + 1])
    keep.start()
    named = read_names(got_ref, names_v, to_scalar, dump=rows)
    names_out[...] = named
    scalars.wait()
    spans = [pl.ds(pl.multiple_of(list_ref[0, FROM + k] * block, block), block) for k in range(MOVES)]
    at = iota(named.shape, 1) & (2 * cap - 1)
    goes = jnp.zeros(named.shape, jnp.bool_)
    for k in range(MOVES):
        goes = goes | ((named >> 7) == list_ref[0, FROM + k])
    needed = jnp.max(jnp.where(goes & (at < cap), at + 1, 0))
    for k in range(MOVES):
        even_ref[spans[k], :] = jnp.zeros((block, feature), jnp.float32)
        odd_ref[spans[k], :] = jnp.zeros((block, feature), jnp.float32)
    to_scalar.wait()

    for offset, count in ROUNDS:

        @pl.when(needed > offset)
        def _():
            add_rows(names_s, got_ref, (even_ref, odd_ref), offset=offset, count=count)

    lane = iota((block, LANES), 1)
    squares = jnp.zeros((block, LANES), jnp.float32)
    for k in range(MOVES):
        gradient = even_ref[spans[k], :] + odd_ref[spans[k], :]
        even_ref[spans[k], :] = gradient
        squares = jnp.where(lane == k, square_sums(gradient), squares)
    fresh = acc_ref[...] + squares * (1.0 / feature)
    rates = rate(jnp.where(lane < MOVES, fresh, 1.0))
    old_ref[...] = jnp.transpose(fresh)
    sends = []
    for k in range(MOVES):
        out_ref[k, pl.ds(block, 1), :] = old_ref[pl.ds(k, 1), :]
        out_ref[k, pl.ds(0, block), :] = table_ref[k] - lane_of(rates, k) * even_ref[spans[k], :]
        sends.append(pltpu.make_async_copy(out_ref.at[k, pl.ds(0, block + 1)], message(out_hbm, list_ref[0, TO + k]), sems.at[k]))
        sends[-1].start()
    for send in sends:
        send.wait()
    keep.wait()


def leave(lists, table, acc, got, peers, cap, rows):
    block, feature = table.shape[1:]
    vm = pl.BlockSpec(memory_space=VM)
    names = (got.shape[0] * 2 * cap // LANES, LANES)
    return pl.pallas_call(
        lambda *refs: leave_kernel(*refs, cap=cap, rows=rows),
        out_shape=(
            jax.ShapeDtypeStruct(names, jnp.int32),
            pltpu.HBM((peers, block + 1, 1, feature), jnp.float32),
            pltpu.HBM(got.shape, jnp.float32),
        ),
        in_specs=[pl.BlockSpec(memory_space=pltpu.HBM), vm, vm, vm],
        out_specs=(vm, pl.BlockSpec(memory_space=pltpu.HBM), pl.BlockSpec(memory_space=pltpu.HBM)),
        scratch_shapes=[
            VM((MOVES, block + 8, feature), jnp.float32),
            VM((rows + 8, feature), jnp.float32),
            VM((rows + 8, feature), jnp.float32),
            VM((LANES, LANES), jnp.float32),
            VM(names, jnp.int32),
            SM(names, jnp.int32),
            SM(lists.shape, jnp.int32),
            pltpu.SemaphoreType.DMA((MOVES + 3,)),
        ],
        compiler_params=pltpu.CompilerParams(vmem_limit_bytes=GRANT - ROOM),
        name="leave",
    )(lists, table, acc, got)


PIECE = 8


def stay_kernel(list_ref, names_ref, table_hbm, acc_ref, got_ref, out_hbm, accout_ref, arrive_ref, squares_ref, table_ref, one_ref, two_ref, rates_ref, sems):
    blocks, block, feature = table_ref.shape
    pieces = blocks // PIECE
    cap = (got_ref.shape[1] - 1) // 2

    def take(i):
        at = pl.ds(i * PIECE, PIECE)
        return pltpu.make_async_copy(table_hbm.at[at], table_ref.at[at], sems.at[i])

    def give(i):
        at = pl.ds(i * PIECE, PIECE)
        return pltpu.make_async_copy(table_ref.at[at], out_hbm.at[at], sems.at[i])

    for i in range(pieces):
        take(i).start()

    def span(b):
        return pl.ds(pl.multiple_of(b * block, block), block)

    def clear(b, _):
        one_ref[span(b), :] = jnp.zeros((block, feature), jnp.float32)
        two_ref[span(b), :] = jnp.zeros((block, feature), jnp.float32)
        return 0

    lax.fori_loop(0, blocks, clear, 0)
    add_rows(names_ref, got_ref, (one_ref,), offset=0, count=cap)
    add_rows(names_ref, got_ref, (two_ref,), offset=cap, count=cap)
    lane = iota((block, LANES), 1)

    def squares(g, sums):
        sums = list(sums)
        for k in range(4):
            b = g * 4 + k
            for n, ref in enumerate((one_ref, two_ref)):
                sums[n] = jnp.where(lane == b, square_sums(ref[span(b), :]), sums[n])
        return tuple(sums)

    zero = jnp.zeros((block, LANES), jnp.float32)
    first, second = lax.fori_loop(0, blocks // 4, squares, (zero, zero))
    old = jnp.concatenate([acc_ref[...], jnp.ones((LANES - blocks, LANES), jnp.float32)], axis=0)
    fresh = jnp.transpose(old) + first * (1.0 / feature)
    rates_ref[0] = rate(fresh)
    fresh = fresh + second * (1.0 / feature)
    rates_ref[1] = rate(fresh)
    accout_ref[...] = jnp.transpose(fresh)[:blocks, :]
    arriving = zero
    for k in range(MOVES):
        gradient = two_ref[span(list_ref[0, SLOT + k]), :]
        arrive_ref[k] = gradient
        arriving = jnp.where(lane == list_ref[0, PEER + k], square_sums(gradient), arriving)
    squares_ref[...] = arriving

    def piece(i, _):
        turn = (LANES - PIECE * i) % LANES
        one_rate = pltpu.roll(rates_ref[0], turn, 1)
        two_rate = pltpu.roll(rates_ref[1], turn, 1)
        take(i).wait()
        for k in range(PIECE):
            b = i * PIECE + k
            weights = table_ref[b] - lane_of(one_rate, k) * one_ref[span(b), :]
            table_ref[b] = weights - lane_of(two_rate, k) * two_ref[span(b), :]
        give(i).start()
        return 0

    lax.fori_loop(0, pieces, piece, 0)
    for i in range(pieces):
        give(i).wait()


def stay(lists, names, table, acc, got):
    blocks, block, feature = table.shape
    vm = pl.BlockSpec(memory_space=VM)
    sm = pl.BlockSpec(memory_space=SM)
    hbm = pl.BlockSpec(memory_space=pltpu.HBM)
    return pl.pallas_call(
        stay_kernel,
        out_shape=(
            jax.ShapeDtypeStruct(table.shape, jnp.float32),
            jax.ShapeDtypeStruct(acc.shape, jnp.float32),
            jax.ShapeDtypeStruct((MOVES, block, feature), jnp.float32),
            jax.ShapeDtypeStruct((LANES, LANES), jnp.float32),
        ),
        in_specs=[sm, sm, hbm, vm, vm],
        out_specs=(hbm, vm, vm, vm),
        scratch_shapes=[
            VM(table.shape, jnp.float32),
            VM((blocks * block + 8, feature), jnp.float32),
            VM((blocks * block + 8, feature), jnp.float32),
            VM((2, LANES, LANES), jnp.float32),
            pltpu.SemaphoreType.DMA((blocks // PIECE,)),
        ],
        compiler_params=pltpu.CompilerParams(vmem_limit_bytes=GRANT - ROOM),
        name="stay",
    )(lists, names, table, acc, got)


def arrive_kernel(list_hbm, got_ref, second_ref, squares_ref, stayed_ref, accstay_ref, out_ref, acc_hbm, acc_ref, buf_ref, old_ref, list_ref, sems):
    block, feature = stayed_ref.shape[1:]
    stride = got_ref.shape[1]
    rows_ref = got_ref.reshape(got_ref.shape[0] * stride, feature)
    scalars = pltpu.make_async_copy(list_hbm, list_ref, sems.at[MOVES + 1])
    scalars.start()
    acc_ref[...] = accstay_ref[...]
    lane = iota((block, LANES), 1)
    peers = got_ref.shape[0]
    for p in range(peers):
        old_ref[pl.ds(p, 1), :] = got_ref[p, block]
    fresh = jnp.transpose(old_ref[...]) + squares_ref[...] * (1.0 / feature)
    rates = rate(jnp.where(lane < peers, fresh, 1.0))
    scalars.wait()
    copies = []
    for k in range(MOVES):
        rates_of = jnp.sum(jnp.where(lane == list_ref[0, PEER + k], rates, 0.0), axis=1, keepdims=True)
        buf_ref[k] = rows_ref[pl.ds(list_ref[0, PEER + k] * stride, block), :] - rates_of * second_ref[k]
        copies.append(pltpu.make_async_copy(buf_ref.at[k], out_ref.at[list_ref[0, SLOT + k]], sems.at[k]))
        copies[-1].start()
    old_ref[...] = jnp.transpose(fresh)
    for k in range(MOVES):
        acc_ref[pl.ds(list_ref[0, SLOT + k], 1), :] = old_ref[pl.ds(list_ref[0, PEER + k], 1), :]
    copies.append(pltpu.make_async_copy(acc_ref, acc_hbm, sems.at[MOVES]))
    copies[-1].start()
    for copy in copies:
        copy.wait()


def arrive(lists, got, second, squares, stayed, accstay):
    blocks, block, feature = stayed.shape
    vm = pl.BlockSpec(memory_space=VM)
    hbm = pl.BlockSpec(memory_space=pltpu.HBM)
    return pl.pallas_call(
        arrive_kernel,
        out_shape=(
            jax.ShapeDtypeStruct(stayed.shape, jnp.float32),
            jax.ShapeDtypeStruct(accstay.shape, jnp.float32),
        ),
        in_specs=[hbm, vm, vm, vm, hbm, vm],
        out_specs=(hbm, hbm),
        scratch_shapes=[
            VM(accstay.shape, jnp.float32),
            VM((MOVES, block, feature), jnp.float32),
            VM((LANES, LANES), jnp.float32),
            SM(lists.shape, jnp.int32),
            pltpu.SemaphoreType.DMA((MOVES + 2,)),
        ],
        input_output_aliases={4: 0},
        compiler_params=pltpu.CompilerParams(vmem_limit_bytes=GRANT - LAST_ROOM),
        name="arrive",
    )(lists, got, second, squares, stayed, accstay)


def listed(mask, values):
    position = jnp.cumsum(mask.astype(jnp.int32)) - 1
    hit = mask[None, :] & (position[None, :] == jnp.arange(MOVES, dtype=jnp.int32)[:, None])
    return [jnp.sum(jnp.where(hit, v[None, :], 0), axis=1) for v in values]


def on_device(table, accumulator, grads_one, ids_one, grads_two, ids_two, new_slot):
    blocks, block, feature = table.shape
    peers = lax.axis_size("row")
    total = lax.axis_size("table") * peers
    group = lax.axis_index("table")
    mine = lax.axis_index("row")
    device = group * peers + mine
    rows = grads_one.shape[0]
    cap = 2 * rows // total

    slot_table = new_slot.reshape(-1, LANES)
    outgoing = pack(ids_one.reshape(1, rows), ids_two.reshape(1, rows), slot_table, grads_one, grads_two, total, blocks, cap)
    got = lax.all_to_all(outgoing, ("table", "row"), split_axis=0, concat_axis=0, tiled=True)

    here = lax.dynamic_slice_in_dim(new_slot, group * peers * blocks, peers * blocks).reshape(peers, blocks)
    own = lax.dynamic_slice_in_dim(new_slot, device * blocks, blocks)
    going = listed(own // blocks != device, (jnp.arange(blocks, dtype=jnp.int32), own // blocks % peers))
    peer = jnp.arange(peers, dtype=jnp.int32)
    to_me = (here // blocks == device) & (peer != mine)[:, None]
    slots = jnp.sum(jnp.where(to_me, here - device * blocks + 1, 0), axis=1)
    coming = listed(slots > 0, (slots - 1, peer))
    lists = jnp.concatenate(going + coming)
    lists = jnp.pad(lists, (0, LANES - lists.shape[0]))[None, :]

    gone, old = fetch(lists, table, accumulator)
    names, moving, kept = leave(lists, gone, old, got, peers, cap, blocks * block)
    moved = lax.all_to_all(moving, "row", split_axis=0, concat_axis=0, tiled=True)
    stayed, accstay, second, squares = stay(lists, names, table, accumulator, kept)
    return arrive(lists, moved, second, squares, stayed, accstay)


def solution(mesh):
    in_specs = (
        P(("table", "row"), None, None),
        P(("table", "row"), None),
        P(("table", "row"), None),
        P(("table", "row")),
        P(("table", "row"), None),
        P(("table", "row")),
        P(),
    )
    out_specs = (P(("table", "row"), None, None), P(("table", "row"), None))
    return jax.shard_map(
        on_device, mesh=mesh, in_specs=in_specs, out_specs=out_specs, check_vma=False
    )
```
